32 devices in a mesh: fsdp: 4 (over y, x), ctx: 4 (over z), tp: 2 (over core).
Axes of the slice: x: 2, y: 2, z: 4, core: 2. Of those that a mesh axis runs over, the one named last changes fastest.
Arguments:
- tokens: bfloat16 [8, 1024, 768], P('fsdp', 'ctx'), may hold values from -6 to 6
- lengths: int32 [8], P('fsdp'), may hold values from 256 to 1024, as said below
- cotangent: bfloat16 [8, 1024, 768], P('fsdp', 'ctx'), may hold values from -6 to 6
- ln1_gain: float32 [768], replicated, may hold values from 0.5 to 1.5
- ln1_bias: float32 [768], replicated, may hold values from -1.8 to 1.8
- qkv_weight: bfloat16 [768, 3, 768], P('fsdp', None, 'tp'), may hold values from -0.21875 to 0.21875
- conv_kernel: float32 [3, 3, 768], P(None, None, 'tp'), may hold values from -3.5 to 3.5
- conv_bias: float32 [3, 768], P(None, 'tp'), may hold values from -1.8 to 1.8
- out_weight: bfloat16 [768, 768], P('tp', 'fsdp'), may hold values from -1.75 to 1.75
- ln2_gain: float32 [768], replicated, may hold values from 0.5 to 1.5
- ln2_bias: float32 [768], replicated, may hold values from -1.8 to 1.8
- up_weight: bfloat16 [768, 3072], P('fsdp', 'tp'), may hold values from -0.21875 to 0.21875
- down_weight: bfloat16 [3072, 768], P('tp', 'fsdp'), may hold values from -0.109375 to 0.109375
Outputs:
- result: bfloat16 [8, 1024, 768], P('fsdp', 'ctx')
- input_grad: float32 [8, 1024, 768], P('fsdp', 'ctx')
- ln1_gain_grad: float32 [768], replicated
- ln1_bias_grad: float32 [768], replicated
- qkv_weight_grad: float32 [768, 3, 768], P('fsdp', None, 'tp')
- conv_kernel_grad: float32 [3, 3, 768], P(None, None, 'tp')
- conv_bias_grad: float32 [3, 768], P(None, 'tp')
- out_weight_grad: float32 [768, 768], P('tp', 'fsdp')
- ln2_gain_grad: float32 [768], replicated
- ln2_bias_grad: float32 [768], replicated
- up_weight_grad: float32 [768, 3072], P('fsdp', 'tp')
- down_weight_grad: float32 [3072, 768], P('tp', 'fsdp')
The draws below stay inside these ranges and needn't reach their ends.
Inputs may be any that keep to these rules, and one draw needn't show every extreme that they name: `lengths`: some slot holds 1024 tokens and some other slot 256.
All inputs are finite; a program needn't handle non-finite values.
Results may differ from the reference program's by a relative error of at most 0.014.
The reference program's roundings to bfloat16 on the way count: a program that leaves them out, or rounds other values in their place, can miss the bound.
Values may be sent and summed in bfloat16 or wider, within the bound.
A program may use at most 256 MiB of HBM per device.

```python
import jax
import jax.numpy as jnp
from jax import lax

D = 768
H = 12
HD = 64
FF = 3072
HH = 768
S = 1024
SLOTS = 8


def draw_lengths(key, part):
    drawn = jax.random.randint(jax.random.fold_in(key, 11), (SLOTS,), S // 4, S + 1)
    chosen = jax.random.permutation(jax.random.fold_in(key, 12), SLOTS)
    drawn = drawn.at[chosen[0]].set(S)
    drawn = drawn.at[chosen[1]].set(S // 4)
    return drawn.astype(jnp.int32)


def block_levels(key, shape, split, low, high):
    level = 1.0
    for axis_at, parts in split:
        heights = jax.random.uniform(jax.random.fold_in(jax.random.fold_in(key, 6), axis_at), (parts,), jnp.float32, low / len(split), high / len(split))
        level = level * jnp.repeat(jnp.exp(heights), shape[axis_at] // parts).reshape((-1,) + (1,) * (len(shape) - 1 - axis_at))
    return level


def normal_values(stream_key, shape, deviation, most, cuts=(), kind=jnp.bfloat16):
    array = deviation * jax.random.normal(stream_key, shape, jnp.float32)
    if cuts:
        array = array * block_levels(stream_key, shape, cuts, -0.22, 0.18)
    return jnp.clip(array, -most, most).astype(kind)


def setup_inputs(seed: int = 0) -> dict:
    keys = jax.random.split(jax.random.key(seed), 14)
    return {
        "tokens": normal_values(keys[0], (SLOTS, S, D), 1.0, 6.0, ((0, 4), (1, 4))),
        "lengths": draw_lengths(jax.random.fold_in(keys[13], 71), 0),
        "cotangent": normal_values(keys[2], (SLOTS, S, D), 1.0, 6.0, ((0, 4), (1, 4))),
        "ln1_gain": jnp.clip(1.0 + 0.1 * jax.random.normal(keys[3], (D,), jnp.float32), 0.5, 1.5),
        "ln1_bias": normal_values(keys[4], (D,), 0.3, 1.8, (), jnp.float32),
        "qkv_weight": normal_values(keys[5], (D, 3, HH), D ** -0.5, 0.21875, ((0, 4), (2, 2))),
        "conv_kernel": normal_values(keys[6], (3, 3, HH), 3 ** -0.5, 3.5, ((2, 2),), jnp.float32),
        "conv_bias": normal_values(keys[7], (3, HH), 0.3, 1.8, ((1, 2),), jnp.float32),
        "out_weight": normal_values(keys[8], (HH, D), (max(HH // 64, 1)) ** -0.5, 1.75, ((0, 2), (1, 4))),
        "ln2_gain": jnp.clip(1.0 + 0.1 * jax.random.normal(keys[9], (D,), jnp.float32), 0.5, 1.5),
        "ln2_bias": normal_values(keys[10], (D,), 0.3, 1.8, (), jnp.float32),
        "up_weight": normal_values(keys[11], (D, FF), D ** -0.5, 0.21875, ((0, 4), (1, 2))),
        "down_weight": normal_values(keys[12], (FF, D), FF ** -0.5, 0.109375, ((0, 2), (1, 4))),
    }


@jax.custom_vjp
def low(v):
    return lax.optimization_barrier(v.astype(jnp.bfloat16)).astype(jnp.float32)

@jax.custom_vjp
def low_back(v):
    return v

def low_keep(v):
    return (low(v), None)

def low_pass(kept, grad):
    return (grad,)

def back_keep(v):
    return (v, None)

def back_low(kept, grad):
    return (low(grad),)
low.defvjp(low_keep, low_pass)
low_back.defvjp(back_keep, back_low)
EPSILON = 1e-05
SCALING = 0.125
MASKED = -1e+30
PRECISE = lax.Precision.HIGHEST

def layer_norm(row_data, norm_gain, shift_bias):
    centred = row_data - lax.optimization_barrier(jnp.mean(row_data, axis=-1, keepdims=True))
    recip = lax.rsqrt(lax.optimization_barrier(jnp.mean(centred * centred, axis=-1, keepdims=True)) + EPSILON)
    return centred * recip * norm_gain + shift_bias

def slot_forward(params, slot_tokens, slot_length):
    gain_one, bias_one, qkv_full, kernel, conv_shift, out_full, gain_two, bias_two, up_weights, down_weights = params
    positions = jnp.arange(S, dtype=jnp.int32)
    first_out = low(layer_norm(slot_tokens, gain_one, bias_one))
    pre_low = low_back(low(jnp.einsum('td,dcn->tcn', first_out, qkv_full, precision=PRECISE)))
    padded = jnp.pad(pre_low, ((2, 0), (0, 0), (0, 0)))
    conv_out = low(conv_shift + kernel[0] * padded[2:] + kernel[1] * padded[1:-1] + kernel[2] * padded[:-2])
    query_heads = conv_out[:, 0].reshape(S, H, HD)
    key_heads = conv_out[:, 1].reshape(S, H, HD)
    value_heads = conv_out[:, 2].reshape(S, H, HD)
    scores = low_back(jnp.einsum('qhd,khd->hqk', query_heads, key_heads, precision=PRECISE) * SCALING)
    allowed = (positions[None, :] <= positions[:, None]) & (positions[None, :] < slot_length)
    scores = jnp.where(allowed[None], scores, MASKED)
    row_max = lax.optimization_barrier(jnp.max(scores, axis=-1, keepdims=True))
    log_total = row_max + jnp.log(lax.optimization_barrier(jnp.sum(jnp.exp(scores - row_max), axis=-1, keepdims=True)))
    probs_low = low(jnp.exp(scores - log_total))
    attn_full = jnp.einsum('hqk,khd->qhd', probs_low, value_heads, precision=PRECISE).reshape(S, HH)
    attn_low = low_back(low(attn_full))
    middle = slot_tokens + low_back(jnp.dot(attn_low, out_full, precision=PRECISE))
    second_out = low(layer_norm(middle, gain_two, bias_two))
    up_full = low_back(jnp.dot(second_out, up_weights, precision=PRECISE))
    act_low = low(jnp.square(jnp.maximum(up_full, 0.0)))
    return middle + low_back(jnp.dot(act_low, down_weights, precision=PRECISE))

def reference(tokens, lengths, cotangent, ln1_gain, ln1_bias, qkv_weight, conv_kernel, conv_bias, out_weight, ln2_gain, ln2_bias, up_weight, down_weight):
    params = (ln1_gain, ln1_bias, qkv_weight.astype(jnp.float32), conv_kernel, conv_bias, out_weight.astype(jnp.float32), ln2_gain, ln2_bias, up_weight.astype(jnp.float32), down_weight.astype(jnp.float32))
    inputs = tokens.astype(jnp.float32)

    def forward(weights_all, inputs_all):
        checked = jax.checkpoint(slot_forward)
        return lax.map(lambda slot_pair: checked(weights_all, slot_pair[0], slot_pair[1]), (inputs_all, lengths))
    outputs, pullback = jax.vjp(forward, params, inputs)
    token_valid = (jnp.arange(S, dtype=jnp.int32)[None, :] < lengths[:, None]).astype(jnp.float32)
    grads, input_grad = pullback(cotangent.astype(jnp.float32) * token_valid[:, :, None])
    g_gain_one, g_bias_one, g_qkv, g_kernel, g_conv_shift, g_out, g_gain_two, g_bias_two, g_up, g_down = grads
    return (outputs.astype(jnp.bfloat16), input_grad, g_gain_one, g_bias_one, g_qkv, g_kernel, g_conv_shift, g_out, g_gain_two, g_bias_two, g_up, g_down)
```

```python
import jax
import jax.numpy as jnp
from jax import lax
from jax.experimental import pallas as pl
from jax.experimental.pallas import tpu as pltpu
from jax.sharding import PartitionSpec as P

HD = 64


EPSILON = 1e-05
SCALING = 0.125
MASKED = -1e30


BF = jnp.bfloat16
F32 = jnp.float32
MESH = pl.DeviceIdType.MESH
ANY = pl.BlockSpec(memory_space=pl.ANY)
VMEM = pl.BlockSpec(memory_space=pltpu.VMEM)
SMEM = pl.BlockSpec(memory_space=pltpu.SMEM)


def mm(left, right, left_dim, right_dim):
    return lax.dot_general(
        left, right, (((left_dim,), (right_dim,)), ((), ())), preferred_element_type=F32
    )


def remote(source, target, send_sem, recv_sem, device):
    return pltpu.make_async_remote_copy(
        src_ref=source,
        dst_ref=target,
        send_sem=send_sem,
        recv_sem=recv_sem,
        device_id=device,
        device_id_type=MESH,
    )


def place():
    f, c, t = lax.axis_index("fsdp"), lax.axis_index("ctx"), lax.axis_index("tp")
    fx = f + 1 - 2 * lax.rem(f, 2)
    fy = lax.rem(f + 2, 4)
    fd = lax.rem(fx + 2, 4)
    return f, c, t, fx, fy, fd


def greet(peers):
    barrier = pltpu.get_barrier_semaphore()
    for peer in peers:
        pl.semaphore_signal(barrier, inc=1, device_id=peer, device_id_type=MESH)
    pl.semaphore_wait(barrier, len(peers))


def norm_rows(x, gain, bias):
    centred = x - jnp.mean(x, axis=-1, keepdims=True)
    recip = lax.rsqrt(jnp.mean(centred * centred, axis=-1, keepdims=True) + EPSILON)
    normed = centred * recip
    return normed * gain + bias, normed, recip


def forward_kernel(
    lens, tok, wq3, wo, wu, wd, gain, bias, taps3, shift3,
    wq_all, wo_all, wu_all, wd_all, attn, heads, pre_all, first_all,
    tok_buf, wq_buf, wq, taps, shift, att, prev,
    own_sem, tok_send, tok_recv, pass_send, pass_recv, w_send, w_recv, att_send, att_recv,
):
    f, c, t, fx, fy, fd = place()
    slot = lax.div(c, 2)
    other = 1 - t
    ctx_peers = [lax.rem(c + d, 4) for d in (1, 2, 3)]
    greet(
        [(fx, c, t), (fy, c, t), (f, c, other)] + [(f, p, t) for p in ctx_peers]
    )
    half_rows = tok.shape[1] // 2
    mine = pl.ds(pl.multiple_of(t * half_rows, half_rows), half_rows)
    theirs = pl.ds(pl.multiple_of(other * half_rows, half_rows), half_rows)

    shards = [wq, wo, wu, wd]
    wholes = [wq_all, wo_all, wu_all, wd_all]

    def direct(w, kind):
        target = (fx, c, t) if kind == 0 else (fy, c, t)
        return remote(shards[w], wholes[w].at[f], w_send.at[w, kind], w_recv.at[w, kind], target)

    def part(w, kind):
        rows = wholes[w].shape[1] // 2
        return pl.ds(0, rows) if kind == 2 else pl.ds(rows, rows)

    def relay(w, kind):
        origin, target = (fx, (fy, c, t)) if kind == 2 else (fy, (fx, c, t))
        view = wholes[w].at[origin, part(w, kind)]
        return remote(view, view, w_send.at[w, kind], w_recv.at[w, kind], target)

    def landed(w, kind):
        if kind < 2:
            view = wholes[w].at[fx if kind == 0 else fy]
        else:
            view = wholes[w].at[fd, part(w, kind)]
        remote(view, view, w_send.at[w, kind], w_recv.at[w, kind], (f, c, other)).wait_recv()

    def send_direct(w):
        direct(w, 0).start()
        direct(w, 1).start()

    def pass_on(w):
        landed(w, 0)
        relay(w, 2).start()
        landed(w, 1)
        relay(w, 3).start()

    def tok_copy(d):
        target = lax.rem(c + d, 4)
        return remote(
            tok.at[lax.div(target, 2), mine],
            tok_buf.at[c, mine],
            tok_send.at[d],
            tok_recv.at[d],
            (f, target, t),
        )

    def tok_pass(source, d):
        view = tok_buf.at[source, mine]
        return remote(view, view, pass_send.at[d], pass_recv.at[d], (f, c, other))

    for d in (1, 2, 3):
        tok_copy(d).start()
    load_wq = pltpu.make_async_copy(wq3, wq_buf, own_sem.at[0])
    load_wq.start()
    load_tok = pltpu.make_async_copy(tok.at[slot], tok_buf.at[c], own_sem.at[1])
    load_tok.start()
    keep = [
        pltpu.make_async_copy(shards[w], wholes[w].at[f], own_sem.at[2 + w]) for w in range(4)
    ]
    for w in range(1, 4):
        keep[w].start()
    load_wq.wait()
    part_width = wq_buf.shape[2] // 2
    for half in (0, 1):

        @pl.when(lax.rem(c, 2) == half)
        def _():
            lanes = slice(half * part_width, (half + 1) * part_width)
            for kind in range(3):
                target = slice(kind * part_width, (kind + 1) * part_width)
                wq[:, target] = wq_buf[kind, :, lanes]
                shift[0:1, target] = shift3[kind : kind + 1, lanes]
                for tap in range(3):
                    taps[tap : tap + 1, target] = taps3[tap, kind : kind + 1, lanes]

    send_direct(0)
    send_direct(1)
    keep[0].start()

    def first_norm(block):
        out, _, _ = norm_rows(tok_buf[block].astype(F32), gain[...], bias[...])
        first_all[block] = out.astype(BF)

    load_tok.wait()
    first_norm(c)

    pass_on(0)
    send_direct(2)

    end = lax.div(c, 3)
    start = lax.div(3 - c, 3)
    d_near = 1 + 2 * start
    d_mid = 3 - start - end
    d_far = 2 - start + end
    for d in (d_near, d_mid, d_far):
        source = lax.rem(c - d + 4, 4)
        view = tok_buf.at[source, mine]
        remote(view, view, tok_send.at[d], tok_recv.at[d], (f, c, other)).wait_recv()
        tok_pass(source, d).start()
        view = tok_buf.at[source, theirs]
        remote(view, view, pass_send.at[d], pass_recv.at[d], (f, c, other)).wait_recv()
        first_norm(source)

    keep[0].wait()
    landed(0, 2)
    landed(0, 3)
    prev[...] = jnp.zeros_like(prev)
    width = wq_all.shape[2]

    def project(block, carry):
        weights = wq_all[...].reshape(-1, width)
        pre = mm(first_all[block], weights, 1, 0).astype(BF)
        pre_all[block] = pre
        pre = pre.astype(F32)
        joined = jnp.concatenate([prev[...], pre], axis=0)
        prev[...] = pre[-8:]
        out = (
            shift[0:1]
            + taps[0:1] * pre
            + taps[1:2] * pltpu.roll(joined, 1, 0)[8:]
            + taps[2:3] * pltpu.roll(joined, 2, 0)[8:]
        ).astype(BF)
        rows = pre.shape[0]
        at = pl.ds(pl.multiple_of(block * rows, rows), rows)
        for head in range(width // HD):
            piece = out[:, head * HD : (head + 1) * HD]
            if head < width // HD // 3:
                piece = (piece.astype(F32) * SCALING).astype(BF)
            heads[head, at, :] = piece
        return carry

    blocks = tok_buf.shape[0]
    block_rows = tok_buf.shape[1]
    lax.fori_loop(0, blocks, project, 0)
    pass_on(1)
    send_direct(3)

    count = width // HD // 3
    length = lens[slot]
    tile = 128
    tiles = block_rows // tile

    def att_copy(block):
        return remote(
            att.at[block],
            attn.at[c],
            att_send.at[block],
            att_recv.at[lax.rem(block - c + 4, 4)],
            (f, block, t),
        )

    for block in reversed(range(blocks)):
        keys = (block + 1) * block_rows

        def attend(n, carry, block=block, keys=keys):
            head, piece = lax.div(n, tiles), lax.rem(n, tiles)
            at = pl.multiple_of(block * block_rows + piece * tile, tile)
            scores = mm(heads[head, pl.ds(at, tile), :], heads[count + head, 0:keys, :], 1, 1)
            col = lax.broadcasted_iota(jnp.int32, scores.shape, 1)
            row = at + lax.broadcasted_iota(jnp.int32, (tile, 1), 0)
            scores = jnp.where(col < jnp.minimum(row + 1, length), scores, MASKED)
            powers = jnp.exp(scores - jnp.max(scores, axis=-1, keepdims=True))
            probs = powers * (1.0 / jnp.sum(powers, axis=-1, keepdims=True))
            out = mm(probs.astype(BF), heads[2 * count + head, 0:keys, :], 1, 0)
            att[
                block,
                pl.ds(pl.multiple_of(head * HD, HD), HD),
                pl.ds(pl.multiple_of(piece * tile, tile), tile),
            ] = out.T.astype(BF)
            return carry

        lax.fori_loop(0, count * tiles, attend, 0)

        @pl.when(block != c)
        def _():
            att_copy(block).start()

        if block == blocks - 1:
            pass_on(2)

    pass_on(3)
    own = pltpu.make_async_copy(att.at[c], attn.at[c], own_sem.at[6])
    own.start()
    own.wait()
    for d in (1, 2, 3):
        source = lax.rem(c - d + 4, 4)
        remote(
            attn.at[source], attn.at[source], att_send.at[0], att_recv.at[d], (f, c, other)
        ).wait_recv()
        tok_copy(d).wait_send()
        tok_pass(lax.rem(c - d + 4, 4), d).wait_send()
    for block in range(blocks):

        @pl.when(block != c)
        def _():
            att_copy(block).wait_send()

    for w in range(4):
        if w:
            landed(w, 2)
            landed(w, 3)
            keep[w].wait()
        direct(w, 0).wait_send()
        direct(w, 1).wait_send()
        relay(w, 2).wait_send()
        relay(w, 3).wait_send()


def forward_call(lens, tok, wq3, wo, wu, wd, gain, bias, taps3, shift3):
    slots, block_rows, model = tok.shape
    blocks = 4
    rows, width = wq3.shape[1], 3 * (wq3.shape[2] // 2)
    dma = pltpu.SemaphoreType.DMA

    def whole(shard):
        return jax.ShapeDtypeStruct((4,) + shard, BF)

    attn_width = width // 3
    return pl.pallas_call(
        forward_kernel,
        name="forward",
        out_shape=[
            whole((rows, width)),
            whole(wo.shape),
            whole(wu.shape),
            whole(wd.shape),
            whole((attn_width, block_rows)),
            jax.ShapeDtypeStruct((width // HD, blocks * block_rows, HD), BF),
            whole((block_rows, width)),
            whole((block_rows, model)),
        ],
        in_specs=[SMEM, ANY, ANY, ANY, ANY, ANY, VMEM, VMEM, VMEM, VMEM],
        out_specs=[VMEM, ANY, ANY, ANY, ANY, VMEM, VMEM, VMEM],
        scratch_shapes=[
            pltpu.VMEM((blocks, block_rows, model), BF),
            pltpu.VMEM(wq3.shape, BF),
            pltpu.VMEM((rows, width), BF),
            pltpu.VMEM((8, width), F32),
            pltpu.VMEM((8, width), F32),
            pltpu.VMEM((blocks, attn_width, block_rows), BF),
            pltpu.VMEM((8, width), F32),
            dma((7,)),
            dma((4,)),
            dma((4,)),
            dma((4,)),
            dma((4,)),
            dma((4, 4)),
            dma((4, 4)),
            dma((4,)),
            dma((4,)),
        ],
        compiler_params=pltpu.CompilerParams(collective_id=0, has_side_effects=True),
    )(lens, tok, wq3, wo, wu, wd, gain, bias, taps3, shift3)


def shifted(block, axis, distance):
    devices = range(lax.axis_size(axis))
    route = [(i - distance, i) for i in devices if i - distance in devices]
    return lax.ppermute(block, axis, route)


def layer_norm(row_data, norm_gain, shift_bias):
    centred = row_data - jnp.mean(row_data, axis=-1, keepdims=True)
    recip = lax.rsqrt(jnp.mean(centred * centred, axis=-1, keepdims=True) + EPSILON)
    normed = centred * recip
    return (normed * norm_gain + shift_bias, normed, recip)


def norm_back(grad_in, normed, recip, norm_gain):
    scaled = grad_in * norm_gain
    return recip * (
        scaled
        - jnp.mean(scaled, axis=-1, keepdims=True)
        - normed * jnp.mean(scaled * normed, axis=-1, keepdims=True)
    )


def tile_scores(query_part, key_part, query_pos, key_pos, lengths):
    scores = (
        jnp.einsum("mqhd,mkhd->mhqk", query_part, key_part, preferred_element_type=jnp.float32)
        * SCALING
    )
    allowed = (key_pos[None, None, :] <= query_pos[None, :, None]) & (
        key_pos[None, None, :] < lengths[:, None, None]
    )
    return jnp.where(allowed[:, None], scores, MASKED)


def tile_grads(
    query_part, key_part, value_part, grad_part, log_part, delta_part, query_pos, key_pos, lengths
):
    probs_full = jnp.exp(tile_scores(query_part, key_part, query_pos, key_pos, lengths) - log_part)
    prob_grad = jnp.einsum(
        "mqhd,mkhd->mhqk", grad_part, value_part, preferred_element_type=jnp.float32
    )
    score_grad = (probs_full * (prob_grad - delta_part)).astype(jnp.bfloat16)
    return (probs_full, prob_grad, score_grad)


def local(
    tokens,
    lengths,
    cotangent,
    ln1_gain,
    ln1_bias,
    qkv_weight,
    conv_kernel,
    conv_bias,
    out_weight,
    ln2_gain,
    ln2_bias,
    up_weight,
    down_weight,
):
    batches, block_rows, model_width = tokens.shape
    all_rows = batches * block_rows
    qkv_full, out_full, up_full_w, down_full_w = (
        lax.all_gather(qkv_weight, "fsdp", axis=0, tiled=True),
        lax.all_gather(out_weight, "fsdp", axis=1, tiled=True),
        lax.all_gather(up_weight, "fsdp", axis=0, tiled=True),
        lax.all_gather(down_weight, "fsdp", axis=1, tiled=True),
    )
    local_width = qkv_full.shape[2]
    local_heads = local_width // HD
    ctx_count = lax.axis_size("ctx")
    slot_span = block_rows * ctx_count
    group_blocks = 4
    key_span = block_rows * group_blocks
    ctx_index = lax.axis_index("ctx")
    positions = ctx_index * block_rows + jnp.arange(block_rows, dtype=jnp.int32)
    span_iota = jnp.arange(key_span, dtype=jnp.int32)
    block_count = (ctx_index * block_rows + block_rows + key_span - 1) // key_span
    token_valid = positions[None, :] < lengths[:, None]

    def span_slice(array_data, block, axis_pos):
        return lax.dynamic_slice_in_dim(array_data, block * key_span, key_span, axis_pos)

    inputs = tokens.astype(jnp.float32).reshape(all_rows, model_width)
    first_out, first_hat, first_recip = layer_norm(inputs, ln1_gain, ln1_bias)
    first_low = first_out.astype(jnp.bfloat16)
    pre_low = jnp.einsum(
        "td,dcn->tcn", first_low, qkv_full, preferred_element_type=jnp.float32
    ).astype(jnp.bfloat16)
    pre_low = pre_low.reshape(batches, block_rows, 3, local_width)
    earlier = shifted(pre_low[:, block_rows - 2 :], "ctx", 1)
    extended = jnp.concatenate([earlier, pre_low], axis=1).astype(jnp.float32)
    conv_out = (
        conv_bias
        + conv_kernel[0] * extended[:, 2:]
        + conv_kernel[1] * extended[:, 1:-1]
        + conv_kernel[2] * extended[:, :-2]
    ).astype(jnp.bfloat16)
    query_heads = conv_out[:, :, 0].reshape(batches, block_rows, local_heads, HD)
    own_pairs = conv_out[:, :, 1:]
    whole_pairs = lax.all_gather(own_pairs, "ctx", axis=1, tiled=True)
    key_heads = whole_pairs[:, :, 0].reshape(batches, slot_span, local_heads, HD)
    value_heads = whole_pairs[:, :, 1].reshape(batches, slot_span, local_heads, HD)

    def stat_step(block, carry):
        row_max, total = carry
        key_pos = block * key_span + span_iota
        scores = tile_scores(
            query_heads, span_slice(key_heads, block, 1), positions, key_pos, lengths
        )
        new_max = jnp.maximum(row_max, jnp.max(scores, axis=-1, keepdims=True))
        total = total * jnp.exp(row_max - new_max) + jnp.sum(
            jnp.exp(scores - new_max), axis=-1, keepdims=True
        )
        return (new_max, total)

    stat_shape = (batches, local_heads, block_rows, 1)
    row_max, total = lax.fori_loop(
        0,
        block_count,
        stat_step,
        (jnp.full(stat_shape, MASKED, jnp.float32), jnp.zeros(stat_shape, jnp.float32)),
    )
    log_total = row_max + jnp.log(total)

    def value_step(block, accum):
        key_pos = block * key_span + span_iota
        scores = tile_scores(
            query_heads, span_slice(key_heads, block, 1), positions, key_pos, lengths
        )
        probs_low = jnp.exp(scores - log_total).astype(jnp.bfloat16)
        return accum + jnp.einsum(
            "mhqk,mkhd->mqhd",
            probs_low,
            span_slice(value_heads, block, 1),
            preferred_element_type=jnp.float32,
        )

    attn_acc = lax.fori_loop(
        0, block_count, value_step, jnp.zeros((batches, block_rows, local_heads, HD), jnp.float32)
    )
    attn_low = attn_acc.reshape(all_rows, local_width).astype(jnp.bfloat16)
    attn_out = lax.psum(jnp.dot(attn_low, out_full, preferred_element_type=jnp.float32), "tp")
    middle = inputs + attn_out
    second_out, second_hat, second_recip = layer_norm(middle, ln2_gain, ln2_bias)
    second_low = second_out.astype(jnp.bfloat16)
    up_full = jnp.dot(second_low, up_full_w, preferred_element_type=jnp.float32)
    rectified = jnp.maximum(up_full, 0.0)
    act_low = (rectified * rectified).astype(jnp.bfloat16)
    ffn_out = lax.psum(jnp.dot(act_low, down_full_w, preferred_element_type=jnp.float32), "tp")
    result = (middle + ffn_out).reshape(batches, block_rows, model_width).astype(jnp.bfloat16)
    grad_out = (
        cotangent.astype(jnp.float32) * token_valid[:, :, None].astype(jnp.float32)
    ).reshape(all_rows, model_width)
    grad_low = grad_out.astype(jnp.bfloat16)
    down_wgrad = jnp.einsum("tf,td->fd", act_low, grad_low, preferred_element_type=jnp.float32)
    act_grad = jnp.einsum("td,fd->tf", grad_low, down_full_w, preferred_element_type=jnp.float32)
    up_grad_low = (act_grad * 2.0 * rectified).astype(jnp.bfloat16)
    up_wgrad = jnp.einsum("td,tf->df", second_low, up_grad_low, preferred_element_type=jnp.float32)
    second_grad = lax.psum(
        jnp.einsum("tf,df->td", up_grad_low, up_full_w, preferred_element_type=jnp.float32), "tp"
    )
    gain_two_grad = jnp.sum(second_grad * second_hat, axis=0)
    bias_two_grad = jnp.sum(second_grad, axis=0)
    middle_grad = grad_out + norm_back(second_grad, second_hat, second_recip, ln2_gain)
    middle_low = middle_grad.astype(jnp.bfloat16)
    out_wgrad = jnp.einsum("tn,td->nd", attn_low, middle_low, preferred_element_type=jnp.float32)
    attn_flat = jnp.einsum(
        "td,nd->tn", middle_low, out_full, preferred_element_type=jnp.float32
    ).astype(jnp.bfloat16)
    attn_grad = attn_flat.reshape(batches, block_rows, local_heads, HD)

    def delta_step(block, accum):
        key_pos = block * key_span + span_iota
        probs_full = jnp.exp(
            tile_scores(query_heads, span_slice(key_heads, block, 1), positions, key_pos, lengths)
            - log_total
        )
        prob_grad = jnp.einsum(
            "mqhd,mkhd->mhqk",
            attn_grad,
            span_slice(value_heads, block, 1),
            preferred_element_type=jnp.float32,
        )
        return accum + jnp.sum(probs_full * prob_grad, axis=-1, keepdims=True)

    delta = lax.fori_loop(0, block_count, delta_step, jnp.zeros(stat_shape, jnp.float32))
    query_zero = jnp.zeros((batches, block_rows, local_heads, HD), jnp.float32)

    def back_step(block, carry):
        accum, buffer = carry
        key_pos = block * key_span + span_iota
        key_part = span_slice(key_heads, block, 1)
        probs_full, prob_grad, score_grad = tile_grads(
            query_heads,
            key_part,
            span_slice(value_heads, block, 1),
            attn_grad,
            log_total,
            delta,
            positions,
            key_pos,
            lengths,
        )
        probs_again = probs_full.astype(jnp.bfloat16)
        accum = (
            accum
            + jnp.einsum(
                "mhqk,mkhd->mqhd", score_grad, key_part, preferred_element_type=jnp.float32
            )
            * SCALING
        )
        key_term = (
            jnp.einsum(
                "mhqk,mqhd->mkhd", score_grad, query_heads, preferred_element_type=jnp.float32
            )
            * SCALING
        )
        value_term = jnp.einsum(
            "mhqk,mqhd->mkhd", probs_again, attn_grad, preferred_element_type=jnp.float32
        )
        stacked = jnp.stack(
            [
                key_term.reshape(batches, key_span, local_width),
                value_term.reshape(batches, key_span, local_width),
            ],
            axis=2,
        )
        buffer = lax.dynamic_update_slice_in_dim(buffer, stacked, block * key_span, 1)
        return (accum, buffer)

    buffer_zero = jnp.zeros((batches, slot_span, 2, local_width), jnp.float32)
    query_grad, pair_terms = lax.fori_loop(0, block_count, back_step, (query_zero, buffer_zero))
    pair_grad = lax.psum_scatter(pair_terms, "ctx", scatter_dimension=1, tiled=True)
    mixed_grad = jnp.concatenate(
        [query_grad.reshape(batches, block_rows, 1, local_width), pair_grad], axis=2
    )
    later = shifted(mixed_grad[:, :2], "ctx", -1)
    ahead = jnp.concatenate([mixed_grad, later], axis=1)
    pre_grad = (
        conv_kernel[0] * ahead[:, :block_rows]
        + conv_kernel[1] * ahead[:, 1 : block_rows + 1]
        + conv_kernel[2] * ahead[:, 2:]
    ).astype(jnp.bfloat16)
    kernel_grad = jnp.stack(
        [
            jnp.sum(extended[:, 2 - offset : 2 - offset + block_rows] * mixed_grad, axis=(0, 1))
            for offset in range(3)
        ]
    )
    shift_grad = jnp.sum(mixed_grad, axis=(0, 1))
    pre_grad = pre_grad.reshape(all_rows, 3, local_width)
    qkv_wgrad = jnp.einsum("td,tcn->dcn", first_low, pre_grad, preferred_element_type=jnp.float32)
    first_grad = lax.psum(
        jnp.einsum("tcn,dcn->td", pre_grad, qkv_full, preferred_element_type=jnp.float32), "tp"
    )
    gain_one_grad = jnp.sum(first_grad * first_hat, axis=0)
    bias_one_grad = jnp.sum(first_grad, axis=0)
    input_grad = middle_grad + norm_back(first_grad, first_hat, first_recip, ln1_gain)
    input_grad = input_grad.reshape(batches, block_rows, model_width)
    summed = lax.psum(
        (
            qkv_wgrad,
            out_wgrad,
            up_wgrad,
            down_wgrad,
            gain_one_grad,
            bias_one_grad,
            kernel_grad,
            shift_grad,
            gain_two_grad,
            bias_two_grad,
        ),
        ("fsdp", "ctx"),
    )
    share_rows = model_width // lax.axis_size("fsdp")
    owner_start = lax.axis_index("fsdp") * share_rows
    qkv_share = lax.dynamic_slice_in_dim(summed[0], owner_start, share_rows, 0)
    out_share = lax.dynamic_slice_in_dim(summed[1], owner_start, share_rows, 1)
    up_share = lax.dynamic_slice_in_dim(summed[2], owner_start, share_rows, 0)
    down_share = lax.dynamic_slice_in_dim(summed[3], owner_start, share_rows, 1)
    small_sums = summed[4:]
    return (
        result,
        input_grad,
        small_sums[0],
        small_sums[1],
        qkv_share,
        small_sums[2],
        small_sums[3],
        out_share,
        small_sums[4],
        small_sums[5],
        up_share,
        down_share,
    )


def local_fast(
    tokens,
    lengths,
    cotangent,
    ln1_gain,
    ln1_bias,
    qkv_weight,
    conv_kernel,
    conv_bias,
    out_weight,
    ln2_gain,
    ln2_bias,
    up_weight,
    down_weight,
):
    batches, block_rows, model_width = tokens.shape
    all_rows = batches * block_rows
    gathered = forward_call(
        lengths, tokens, qkv_weight.transpose(1, 0, 2), out_weight.T, up_weight, down_weight.T,
        ln1_gain[None], ln1_bias[None], conv_kernel, conv_bias,
    )
    qkv_full = lax.all_gather(qkv_weight, "fsdp", axis=0, tiled=True)
    out_full = gathered[1].reshape(model_width, -1).T
    up_full_w = gathered[2].reshape(model_width, -1)
    down_full_w = gathered[3].reshape(model_width, -1).T
    local_width = qkv_full.shape[2]
    local_heads = local_width // HD
    ctx_count = lax.axis_size("ctx")
    slot_span = block_rows * ctx_count
    group_blocks = 4
    key_span = block_rows * group_blocks
    ctx_index = lax.axis_index("ctx")
    positions = ctx_index * block_rows + jnp.arange(block_rows, dtype=jnp.int32)
    span_iota = jnp.arange(key_span, dtype=jnp.int32)
    block_count = (ctx_index * block_rows + block_rows + key_span - 1) // key_span
    token_valid = positions[None, :] < lengths[:, None]

    def span_slice(array_data, block, axis_pos):
        return lax.dynamic_slice_in_dim(array_data, block * key_span, key_span, axis_pos)

    inputs = tokens.astype(jnp.float32).reshape(all_rows, model_width)
    first_out, first_hat, first_recip = layer_norm(inputs, ln1_gain, ln1_bias)
    first_low = first_out.astype(jnp.bfloat16)
    pre_low = jnp.einsum(
        "td,dcn->tcn", first_low, qkv_full, preferred_element_type=jnp.float32
    ).astype(jnp.bfloat16)
    pre_low = pre_low.reshape(batches, block_rows, 3, local_width)
    earlier = shifted(pre_low[:, block_rows - 2 :], "ctx", 1)
    extended = jnp.concatenate([earlier, pre_low], axis=1).astype(jnp.float32)
    conv_out = (
        conv_bias
        + conv_kernel[0] * extended[:, 2:]
        + conv_kernel[1] * extended[:, 1:-1]
        + conv_kernel[2] * extended[:, :-2]
    ).astype(jnp.bfloat16)
    query_heads = conv_out[:, :, 0].reshape(batches, block_rows, local_heads, HD)
    own_pairs = conv_out[:, :, 1:]
    whole_pairs = lax.all_gather(own_pairs, "ctx", axis=1, tiled=True)
    key_heads = whole_pairs[:, :, 0].reshape(batches, slot_span, local_heads, HD)
    value_heads = whole_pairs[:, :, 1].reshape(batches, slot_span, local_heads, HD)

    def stat_step(block, carry):
        row_max, total = carry
        key_pos = block * key_span + span_iota
        scores = tile_scores(
            query_heads, span_slice(key_heads, block, 1), positions, key_pos, lengths
        )
        new_max = jnp.maximum(row_max, jnp.max(scores, axis=-1, keepdims=True))
        total = total * jnp.exp(row_max - new_max) + jnp.sum(
            jnp.exp(scores - new_max), axis=-1, keepdims=True
        )
        return (new_max, total)

    stat_shape = (batches, local_heads, block_rows, 1)
    row_max, total = lax.fori_loop(
        0,
        block_count,
        stat_step,
        (jnp.full(stat_shape, MASKED, jnp.float32), jnp.zeros(stat_shape, jnp.float32)),
    )
    log_total = row_max + jnp.log(total)

    attn_low = gathered[4].reshape(batches, local_width, block_rows)
    attn_low = attn_low.transpose(0, 2, 1).reshape(all_rows, local_width)
    attn_out = lax.psum(jnp.dot(attn_low, out_full, preferred_element_type=jnp.float32), "tp")
    middle = inputs + attn_out
    second_out, second_hat, second_recip = layer_norm(middle, ln2_gain, ln2_bias)
    second_low = second_out.astype(jnp.bfloat16)
    up_full = jnp.dot(second_low, up_full_w, preferred_element_type=jnp.float32)
    rectified = jnp.maximum(up_full, 0.0)
    act_low = (rectified * rectified).astype(jnp.bfloat16)
    ffn_out = lax.psum(jnp.dot(act_low, down_full_w, preferred_element_type=jnp.float32), "tp")
    result = (middle + ffn_out).reshape(batches, block_rows, model_width).astype(jnp.bfloat16)
    grad_out = (
        cotangent.astype(jnp.float32) * token_valid[:, :, None].astype(jnp.float32)
    ).reshape(all_rows, model_width)
    grad_low = grad_out.astype(jnp.bfloat16)
    down_wgrad = jnp.einsum("tf,td->fd", act_low, grad_low, preferred_element_type=jnp.float32)
    act_grad = jnp.einsum("td,fd->tf", grad_low, down_full_w, preferred_element_type=jnp.float32)
    up_grad_low = (act_grad * 2.0 * rectified).astype(jnp.bfloat16)
    up_wgrad = jnp.einsum("td,tf->df", second_low, up_grad_low, preferred_element_type=jnp.float32)
    second_grad = lax.psum(
        jnp.einsum("tf,df->td", up_grad_low, up_full_w, preferred_element_type=jnp.float32), "tp"
    )
    gain_two_grad = jnp.sum(second_grad * second_hat, axis=0)
    bias_two_grad = jnp.sum(second_grad, axis=0)
    middle_grad = grad_out + norm_back(second_grad, second_hat, second_recip, ln2_gain)
    middle_low = middle_grad.astype(jnp.bfloat16)
    out_wgrad = jnp.einsum("tn,td->nd", attn_low, middle_low, preferred_element_type=jnp.float32)
    attn_flat = jnp.einsum(
        "td,nd->tn", middle_low, out_full, preferred_element_type=jnp.float32
    ).astype(jnp.bfloat16)
    attn_grad = attn_flat.reshape(batches, block_rows, local_heads, HD)

    def delta_step(block, accum):
        key_pos = block * key_span + span_iota
        probs_full = jnp.exp(
            tile_scores(query_heads, span_slice(key_heads, block, 1), positions, key_pos, lengths)
            - log_total
        )
        prob_grad = jnp.einsum(
            "mqhd,mkhd->mhqk",
            attn_grad,
            span_slice(value_heads, block, 1),
            preferred_element_type=jnp.float32,
        )
        return accum + jnp.sum(probs_full * prob_grad, axis=-1, keepdims=True)

    delta = lax.fori_loop(0, block_count, delta_step, jnp.zeros(stat_shape, jnp.float32))
    query_zero = jnp.zeros((batches, block_rows, local_heads, HD), jnp.float32)

    def back_step(block, carry):
        accum, buffer = carry
        key_pos = block * key_span + span_iota
        key_part = span_slice(key_heads, block, 1)
        probs_full, prob_grad, score_grad = tile_grads(
            query_heads,
            key_part,
            span_slice(value_heads, block, 1),
            attn_grad,
            log_total,
            delta,
            positions,
            key_pos,
            lengths,
        )
        probs_again = probs_full.astype(jnp.bfloat16)
        accum = (
            accum
            + jnp.einsum(
                "mhqk,mkhd->mqhd", score_grad, key_part, preferred_element_type=jnp.float32
            )
            * SCALING
        )
        key_term = (
            jnp.einsum(
                "mhqk,mqhd->mkhd", score_grad, query_heads, preferred_element_type=jnp.float32
            )
            * SCALING
        )
        value_term = jnp.einsum(
            "mhqk,mqhd->mkhd", probs_again, attn_grad, preferred_element_type=jnp.float32
        )
        stacked = jnp.stack(
            [
                key_term.reshape(batches, key_span, local_width),
                value_term.reshape(batches, key_span, local_width),
            ],
            axis=2,
        )
        buffer = lax.dynamic_update_slice_in_dim(buffer, stacked, block * key_span, 1)
        return (accum, buffer)

    buffer_zero = jnp.zeros((batches, slot_span, 2, local_width), jnp.float32)
    query_grad, pair_terms = lax.fori_loop(0, block_count, back_step, (query_zero, buffer_zero))
    pair_grad = lax.psum_scatter(pair_terms, "ctx", scatter_dimension=1, tiled=True)
    mixed_grad = jnp.concatenate(
        [query_grad.reshape(batches, block_rows, 1, local_width), pair_grad], axis=2
    )
    later = shifted(mixed_grad[:, :2], "ctx", -1)
    ahead = jnp.concatenate([mixed_grad, later], axis=1)
    pre_grad = (
        conv_kernel[0] * ahead[:, :block_rows]
        + conv_kernel[1] * ahead[:, 1 : block_rows + 1]
        + conv_kernel[2] * ahead[:, 2:]
    ).astype(jnp.bfloat16)
    kernel_grad = jnp.stack(
        [
            jnp.sum(extended[:, 2 - offset : 2 - offset + block_rows] * mixed_grad, axis=(0, 1))
            for offset in range(3)
        ]
    )
    shift_grad = jnp.sum(mixed_grad, axis=(0, 1))
    pre_grad = pre_grad.reshape(all_rows, 3, local_width)
    qkv_wgrad = jnp.einsum("td,tcn->dcn", first_low, pre_grad, preferred_element_type=jnp.float32)
    first_grad = lax.psum(
        jnp.einsum("tcn,dcn->td", pre_grad, qkv_full, preferred_element_type=jnp.float32), "tp"
    )
    gain_one_grad = jnp.sum(first_grad * first_hat, axis=0)
    bias_one_grad = jnp.sum(first_grad, axis=0)
    input_grad = middle_grad + norm_back(first_grad, first_hat, first_recip, ln1_gain)
    input_grad = input_grad.reshape(batches, block_rows, model_width)
    summed = lax.psum(
        (
            qkv_wgrad,
            out_wgrad,
            up_wgrad,
            down_wgrad,
            gain_one_grad,
            bias_one_grad,
            kernel_grad,
            shift_grad,
            gain_two_grad,
            bias_two_grad,
        ),
        ("fsdp", "ctx"),
    )
    share_rows = model_width // lax.axis_size("fsdp")
    owner_start = lax.axis_index("fsdp") * share_rows
    qkv_share = lax.dynamic_slice_in_dim(summed[0], owner_start, share_rows, 0)
    out_share = lax.dynamic_slice_in_dim(summed[1], owner_start, share_rows, 1)
    up_share = lax.dynamic_slice_in_dim(summed[2], owner_start, share_rows, 0)
    down_share = lax.dynamic_slice_in_dim(summed[3], owner_start, share_rows, 1)
    small_sums = summed[4:]
    return (
        result,
        input_grad,
        small_sums[0],
        small_sums[1],
        qkv_share,
        small_sums[2],
        small_sums[3],
        out_share,
        small_sums[4],
        small_sums[5],
        up_share,
        down_share,
    )


def solution(mesh):
    placed = (
        P("fsdp", "ctx", None),
        P("fsdp"),
        P("fsdp", "ctx", None),
        P(),
        P(),
        P("fsdp", None, "tp"),
        P(None, None, "tp"),
        P(None, "tp"),
        P("tp", "fsdp"),
        P(),
        P(),
        P("fsdp", "tp"),
        P("tp", "fsdp"),
    )
    ctx, fsdp, tp = mesh.shape["ctx"], mesh.shape["fsdp"], mesh.shape["tp"]
    return jax.shard_map(
        local_fast if (fsdp, ctx, tp) == (4, 4, 2) else local,
        mesh=mesh,
        in_specs=placed,
        out_specs=(
            P("fsdp", "ctx", None),
            P("fsdp", "ctx", None),
            P(),
            P(),
            P("fsdp", None, "tp"),
            P(None, None, "tp"),
            P(None, "tp"),
            P("tp", "fsdp"),
            P(),
            P(),
            P("fsdp", "tp"),
            P("tp", "fsdp"),
        ),
        check_vma=False,
    )
```

```python
import jax
import jax.numpy as jnp
from jax import lax
from jax.experimental import pallas as pl
from jax.experimental.pallas import tpu as pltpu
from jax.sharding import PartitionSpec as P

HD = 64


EPSILON = 1e-05
SCALING = 0.125
MASKED = -1e30


def shifted(block, axis, distance):
    devices = range(lax.axis_size(axis))
    route = [(i - distance, i) for i in devices if i - distance in devices]
    return lax.ppermute(block, axis, route)


def layer_norm(row_data, norm_gain, shift_bias):
    centred = row_data - jnp.mean(row_data, axis=-1, keepdims=True)
    recip = lax.rsqrt(jnp.mean(centred * centred, axis=-1, keepdims=True) + EPSILON)
    normed = centred * recip
    return (normed * norm_gain + shift_bias, normed, recip)


def norm_back(grad_in, normed, recip, norm_gain):
    scaled = grad_in * norm_gain
    return recip * (
        scaled
        - jnp.mean(scaled, axis=-1, keepdims=True)
        - normed * jnp.mean(scaled * normed, axis=-1, keepdims=True)
    )


def tile_scores(query_part, key_part, query_pos, key_pos, lengths):
    scores = (
        jnp.einsum("mqhd,mkhd->mhqk", query_part, key_part, preferred_element_type=jnp.float32)
        * SCALING
    )
    allowed = (key_pos[None, None, :] <= query_pos[None, :, None]) & (
        key_pos[None, None, :] < lengths[:, None, None]
    )
    return jnp.where(allowed[:, None], scores, MASKED)


def tile_grads(
    query_part, key_part, value_part, grad_part, log_part, delta_part, query_pos, key_pos, lengths
):
    probs_full = jnp.exp(tile_scores(query_part, key_part, query_pos, key_pos, lengths) - log_part)
    prob_grad = jnp.einsum(
        "mqhd,mkhd->mhqk", grad_part, value_part, preferred_element_type=jnp.float32
    )
    score_grad = (probs_full * (prob_grad - delta_part)).astype(jnp.bfloat16)
    return (probs_full, prob_grad, score_grad)


BF = jnp.bfloat16
F32 = jnp.float32
MESH = pl.DeviceIdType.MESH
ANY = pl.BlockSpec(memory_space=pl.ANY)
VMEM = pl.BlockSpec(memory_space=pltpu.VMEM)
SMEM = pl.BlockSpec(memory_space=pltpu.SMEM)


def mm(left, right, left_dim, right_dim):
    return lax.dot_general(
        left, right, (((left_dim,), (right_dim,)), ((), ())), preferred_element_type=F32
    )


def remote(source, target, send_sem, recv_sem, device):
    return pltpu.make_async_remote_copy(
        src_ref=source,
        dst_ref=target,
        send_sem=send_sem,
        recv_sem=recv_sem,
        device_id=device,
        device_id_type=MESH,
    )


def place():
    f, c, t = lax.axis_index("fsdp"), lax.axis_index("ctx"), lax.axis_index("tp")
    fx = f + 1 - 2 * lax.rem(f, 2)
    fy = lax.rem(f + 2, 4)
    fd = lax.rem(fx + 2, 4)
    return f, c, t, fx, fy, fd


def greet(peers):
    barrier = pltpu.get_barrier_semaphore()
    for peer in peers:
        pl.semaphore_signal(barrier, inc=1, device_id=peer, device_id_type=MESH)
    pl.semaphore_wait(barrier, len(peers))


def norm_rows(x, gain, bias):
    centred = x - jnp.mean(x, axis=-1, keepdims=True)
    recip = lax.rsqrt(jnp.mean(centred * centred, axis=-1, keepdims=True) + EPSILON)
    normed = centred * recip
    return normed * gain + bias, normed, recip


def forward_kernel(
    lens, tok, wq3, wo, wu, wd, gain, bias, taps3, shift3,
    wq_all, wo_all, wu_all, wd_all, attn, heads, pre_all, first_all,
    tok_buf, wq_buf, wq, taps, shift, att, prev,
    own_sem, tok_send, tok_recv, pass_send, pass_recv, w_send, w_recv, att_send, att_recv,
):
    f, c, t, fx, fy, fd = place()
    slot = lax.div(c, 2)
    other = 1 - t
    ctx_peers = [lax.rem(c + d, 4) for d in (1, 2, 3)]
    greet(
        [(fx, c, t), (fy, c, t), (f, c, other)] + [(f, p, t) for p in ctx_peers]
    )
    half_rows = tok.shape[1] // 2
    mine = pl.ds(pl.multiple_of(t * half_rows, half_rows), half_rows)
    theirs = pl.ds(pl.multiple_of(other * half_rows, half_rows), half_rows)

    shards = [wq, wo, wu, wd]
    wholes = [wq_all, wo_all, wu_all, wd_all]

    def direct(w, kind):
        target = (fx, c, t) if kind == 0 else (fy, c, t)
        return remote(shards[w], wholes[w].at[f], w_send.at[w, kind], w_recv.at[w, kind], target)

    def part(w, kind):
        rows = wholes[w].shape[1] // 2
        return pl.ds(0, rows) if kind == 2 else pl.ds(rows, rows)

    def relay(w, kind):
        origin, target = (fx, (fy, c, t)) if kind == 2 else (fy, (fx, c, t))
        view = wholes[w].at[origin, part(w, kind)]
        return remote(view, view, w_send.at[w, kind], w_recv.at[w, kind], target)

    def landed(w, kind):
        if kind < 2:
            view = wholes[w].at[fx if kind == 0 else fy]
        else:
            view = wholes[w].at[fd, part(w, kind)]
        remote(view, view, w_send.at[w, kind], w_recv.at[w, kind], (f, c, other)).wait_recv()

    def send_direct(w):
        direct(w, 0).start()
        direct(w, 1).start()

    def pass_on(w):
        landed(w, 0)
        relay(w, 2).start()
        landed(w, 1)
        relay(w, 3).start()

    def tok_copy(d):
        target = lax.rem(c + d, 4)
        return remote(
            tok.at[lax.div(target, 2), mine],
            tok_buf.at[c, mine],
            tok_send.at[d],
            tok_recv.at[d],
            (f, target, t),
        )

    def tok_pass(source, d):
        view = tok_buf.at[source, mine]
        return remote(view, view, pass_send.at[d], pass_recv.at[d], (f, c, other))

    for d in (1, 2, 3):
        tok_copy(d).start()
    load_wq = pltpu.make_async_copy(wq3, wq_buf, own_sem.at[0])
    load_wq.start()
    load_tok = pltpu.make_async_copy(tok.at[slot], tok_buf.at[c], own_sem.at[1])
    load_tok.start()
    keep = [
        pltpu.make_async_copy(shards[w], wholes[w].at[f], own_sem.at[2 + w]) for w in range(4)
    ]
    for w in range(1, 4):
        keep[w].start()
    load_wq.wait()
    part_width = wq_buf.shape[2] // 2
    for half in (0, 1):

        @pl.when(lax.rem(c, 2) == half)
        def _():
            lanes = slice(half * part_width, (half + 1) * part_width)
            for kind in range(3):
                target = slice(kind * part_width, (kind + 1) * part_width)
                wq[:, target] = wq_buf[kind, :, lanes]
                shift[0:1, target] = shift3[kind : kind + 1, lanes]
                for tap in range(3):
                    taps[tap : tap + 1, target] = taps3[tap, kind : kind + 1, lanes]

    send_direct(0)
    send_direct(1)
    keep[0].start()

    def first_norm(block):
        out, _, _ = norm_rows(tok_buf[block].astype(F32), gain[...], bias[...])
        first_all[block] = out.astype(BF)

    load_tok.wait()
    first_norm(c)

    pass_on(0)
    send_direct(2)

    end = lax.div(c, 3)
    start = lax.div(3 - c, 3)
    d_near = 1 + 2 * start
    d_mid = 3 - start - end
    d_far = 2 - start + end
    for d in (d_near, d_mid, d_far):
        source = lax.rem(c - d + 4, 4)
        view = tok_buf.at[source, mine]
        remote(view, view, tok_send.at[d], tok_recv.at[d], (f, c, other)).wait_recv()
        tok_pass(source, d).start()
        view = tok_buf.at[source, theirs]
        remote(view, view, pass_send.at[d], pass_recv.at[d], (f, c, other)).wait_recv()
        first_norm(source)

    keep[0].wait()
    landed(0, 2)
    landed(0, 3)
    prev[...] = jnp.zeros_like(prev)
    width = wq_all.shape[2]

    def project(block, carry):
        weights = wq_all[...].reshape(-1, width)
        pre = mm(first_all[block], weights, 1, 0).astype(BF)
        pre_all[block] = pre
        pre = pre.astype(F32)
        joined = jnp.concatenate([prev[...], pre], axis=0)
        prev[...] = pre[-8:]
        out = (
            shift[0:1]
            + taps[0:1] * pre
            + taps[1:2] * pltpu.roll(joined, 1, 0)[8:]
            + taps[2:3] * pltpu.roll(joined, 2, 0)[8:]
        ).astype(BF)
        rows = pre.shape[0]
        at = pl.ds(pl.multiple_of(block * rows, rows), rows)
        for head in range(width // HD):
            piece = out[:, head * HD : (head + 1) * HD]
            if head < width // HD // 3:
                piece = (piece.astype(F32) * SCALING).astype(BF)
            heads[head, at, :] = piece
        return carry

    blocks = tok_buf.shape[0]
    block_rows = tok_buf.shape[1]
    lax.fori_loop(0, blocks, project, 0)
    pass_on(1)
    send_direct(3)

    count = width // HD // 3
    length = lens[slot]
    tile = 128
    tiles = block_rows // tile

    def att_copy(block):
        return remote(
            att.at[block],
            attn.at[c],
            att_send.at[block],
            att_recv.at[lax.rem(block - c + 4, 4)],
            (f, block, t),
        )

    for block in reversed(range(blocks)):
        keys = (block + 1) * block_rows

        def attend(n, carry, block=block, keys=keys):
            head, piece = lax.div(n, tiles), lax.rem(n, tiles)
            at = pl.multiple_of(block * block_rows + piece * tile, tile)
            scores = mm(heads[head, pl.ds(at, tile), :], heads[count + head, 0:keys, :], 1, 1)
            col = lax.broadcasted_iota(jnp.int32, scores.shape, 1)
            row = at + lax.broadcasted_iota(jnp.int32, (tile, 1), 0)
            scores = jnp.where(col < jnp.minimum(row + 1, length), scores, MASKED)
            powers = jnp.exp(scores - jnp.max(scores, axis=-1, keepdims=True))
            probs = powers * (1.0 / jnp.sum(powers, axis=-1, keepdims=True))
            out = mm(probs.astype(BF), heads[2 * count + head, 0:keys, :], 1, 0)
            att[
                block,
                pl.ds(pl.multiple_of(head * HD, HD), HD),
                pl.ds(pl.multiple_of(piece * tile, tile), tile),
            ] = out.T.astype(BF)
            return carry

        lax.fori_loop(0, count * tiles, attend, 0)

        @pl.when(block != c)
        def _():
            att_copy(block).start()

        if block == blocks - 1:
            pass_on(2)

    pass_on(3)
    own = pltpu.make_async_copy(att.at[c], attn.at[c], own_sem.at[6])
    own.start()
    own.wait()
    for d in (1, 2, 3):
        source = lax.rem(c - d + 4, 4)
        remote(
            attn.at[source], attn.at[source], att_send.at[0], att_recv.at[d], (f, c, other)
        ).wait_recv()
        tok_copy(d).wait_send()
        tok_pass(lax.rem(c - d + 4, 4), d).wait_send()
    for block in range(blocks):

        @pl.when(block != c)
        def _():
            att_copy(block).wait_send()

    for w in range(4):
        if w:
            landed(w, 2)
            landed(w, 3)
            keep[w].wait()
        direct(w, 0).wait_send()
        direct(w, 1).wait_send()
        relay(w, 2).wait_send()
        relay(w, 3).wait_send()


def forward_call(lens, tok, wq3, wo, wu, wd, gain, bias, taps3, shift3):
    slots, block_rows, model = tok.shape
    blocks = 4
    rows, width = wq3.shape[1], 3 * (wq3.shape[2] // 2)
    dma = pltpu.SemaphoreType.DMA

    def whole(shard):
        return jax.ShapeDtypeStruct((4,) + shard, BF)

    attn_width = width // 3
    return pl.pallas_call(
        forward_kernel,
        name="forward",
        out_shape=[
            whole((rows, width)),
            whole(wo.shape),
            whole(wu.shape),
            whole(wd.shape),
            whole((attn_width, block_rows)),
            jax.ShapeDtypeStruct((width // HD, blocks * block_rows, HD), BF),
            whole((block_rows, width)),
            whole((block_rows, model)),
        ],
        in_specs=[SMEM, ANY, ANY, ANY, ANY, ANY, VMEM, VMEM, VMEM, VMEM],
        out_specs=[VMEM, ANY, ANY, ANY, ANY, VMEM, VMEM, VMEM],
        scratch_shapes=[
            pltpu.VMEM((blocks, block_rows, model), BF),
            pltpu.VMEM(wq3.shape, BF),
            pltpu.VMEM((rows, width), BF),
            pltpu.VMEM((8, width), F32),
            pltpu.VMEM((8, width), F32),
            pltpu.VMEM((blocks, attn_width, block_rows), BF),
            pltpu.VMEM((8, width), F32),
            dma((7,)),
            dma((4,)),
            dma((4,)),
            dma((4,)),
            dma((4,)),
            dma((4, 4)),
            dma((4, 4)),
            dma((4,)),
            dma((4,)),
        ],
        compiler_params=pltpu.CompilerParams(collective_id=0, has_side_effects=True),
    )(lens, tok, wq3, wo, wu, wd, gain, bias, taps3, shift3)


def flipped_pair(index):
    return index + 1 - 2 * lax.rem(index, 2)


def backward_kernel(
    lens, tok_in, cot_in, attn_in, wo_in, wu_in, wd_in, wq_in, heads_in, pre_in, first_in,
    gain1, gain2, bias2, taps3,
    result, input_grad, down_out, up_out, out_out, qkv_out, small_out,
    tok, cot, attn, wo, wu, wd, wq, heads, pre_all, first_all,
    low, part_a, part_a_in, part_b, part_b_in, act_grad, middle, middle_grad,
    second, grad_low, act, up_grad, middle_low, flat, flat_in,
    g_down, g_up, g_out, g_qkv,
    near, far_send, far, z_own, z_in, q_own, q_in, q_sum,
    key_acc, value_acc, query_t, later, mixed_low, pre_grad, taps, conv_acc,
    fg_in, fg_low, fg_all, small_send, small_in,
    load_sem, part_send, part_recv, flat_send, flat_recv,
    near_send, near_recv, far_ssem, far_recv, z_send, z_recv, q_send, q_recv,
    fg_ssem, fg_recv, own_send, own_recv, in_send, in_recv, sm_send, sm_recv,
):
    f, c, t, fx, fy, fd = place()
    slot = lax.div(c, 2)
    half = lax.rem(c, 2)
    other = 1 - t
    partner = (f, c, other)
    greet([(fx, c, t), (fy, c, t), partner] + [(f, lax.rem(c + d, 4), t) for d in (1, 2, 3)])
    slots, block_rows, model = tok.shape
    units = act.shape[2]
    width = wq.shape[1]
    count = width // HD // 3
    blocks = 4
    tile = 128
    tiles = block_rows // tile
    half_rows = block_rows // 2
    mine = pl.ds(pl.multiple_of(t * half_rows, half_rows), half_rows)
    theirs = pl.ds(pl.multiple_of(other * half_rows, half_rows), half_rows)

    loads = {}
    for at, (name, source, target) in enumerate(
        [
            ("attn", attn_in, attn), ("wo", wo_in, wo), ("cot", cot_in, cot), ("wd", wd_in, wd),
            ("tok", tok_in, tok), ("wu", wu_in, wu), ("heads", heads_in, heads),
            ("wq", wq_in, wq), ("pre", pre_in, pre_all), ("first", first_in, first_all),
        ]
    ):
        loads[name] = pltpu.make_async_copy(source, target, load_sem.at[at])
        loads[name].start()

    def swap(source, target, kind, s):
        return remote(
            source.at[s], target.at[s], part_send.at[kind, s], part_recv.at[kind, s], partner
        )

    loads["attn"].wait()
    loads["wo"].wait()

    def attn_out(s, carry):
        rows = jnp.concatenate([attn[2 * s], attn[2 * s + 1]], axis=0).T
        low[s] = rows
        part_a[s] = mm(rows, wo[...], 1, 1)
        swap(part_a, part_a_in, 0, s).start()
        return carry

    lax.fori_loop(0, slots, attn_out, 0)
    loads["cot"].wait()
    loads["wd"].wait()

    def down_back(s, carry):
        row = c * block_rows + lax.broadcasted_iota(jnp.int32, (block_rows, 1), 0)
        grad = jnp.where(row < lens[s], cot[s].astype(F32), 0.0).astype(BF)
        grad_low[s] = grad
        act_grad[s] = mm(grad, wd[...], 1, 0)
        return carry

    lax.fori_loop(0, slots, down_back, 0)
    loads["tok"].wait()
    loads["wu"].wait()

    def feed(s, carry):
        swap(part_a, part_a_in, 0, s).wait()
        mid = tok[s].astype(F32) + (part_a[s] + part_a_in[s])
        middle[s] = mid
        out, _, _ = norm_rows(mid, gain2[...], bias2[...])
        low_out = out.astype(BF)
        second[s] = low_out
        rect = jnp.maximum(mm(low_out, wu[...], 1, 0), 0.0)
        act[s] = (rect * rect).astype(BF)
        grad = (act_grad[s] * 2.0 * rect).astype(BF)
        up_grad[s] = grad
        part_b[s] = mm(grad, wu[...], 1, 1)
        swap(part_b, part_b_in, 1, s).start()
        return carry

    lax.fori_loop(0, slots, feed, 0)

    def weight_grad(target, left, right):
        def step(j, carry):
            at = pl.ds(pl.multiple_of(j * 128, 128), 128)
            rows = slots * block_rows
            lhs = left[:, :, at].reshape(rows, 128)
            rhs = right[...].reshape(rows, right.shape[2])
            target[at, :] = mm(lhs, rhs, 0, 0).astype(BF)
            return carry

        lax.fori_loop(0, model // 128, step, 0)

    grads = [g_down, g_up, g_out, g_qkv]
    finals = [down_out, up_out, out_out]
    share = model // 4
    rows_half = share // 2
    cuts = [2, 2, 1, 1]
    inner = lax.rem(lax.div(c + 1, 2), 2)
    z_outer = jnp.where(c == 1, 0, 3)
    z_near = jnp.where(c == 0, 1, jnp.where(c == 3, 2, 3 - c))

    def rows_of(w, owner, side, u):
        size = rows_half // cuts[w]
        start = owner * share + side * rows_half + u * size
        return pl.ds(pl.multiple_of(start, 16), size)

    def cut(w, u):
        size = rows_half // cuts[w]
        return pl.ds(u * size, size)

    def near_copy(w, kind, u):
        owner = (fx, fd, fy, fd)[kind]
        target = (fx, c, t) if kind < 2 else (fy, c, t)
        return remote(
            grads[w].at[rows_of(w, owner, kind // 2, u)],
            near[w].at[kind, cut(w, u)],
            near_send[w].at[kind, u],
            near_recv[w].at[kind, u],
            target,
        )

    def far_copy(w, side, u):
        return remote(
            far_send[w].at[side, cut(w, u)],
            far[w].at[side, cut(w, u)],
            far_ssem[w].at[side, u],
            far_recv[w].at[side, u],
            (fy, c, t) if side == 0 else (fx, c, t),
        )

    def first_hop(w):
        for kinds in ((1, 3), (0, 2)):
            for u in range(cuts[w]):
                for kind in kinds:
                    near_copy(w, kind, u).start()

    def second_hop(w):
        for u in range(cuts[w]):
            for side in (0, 1):
                kind = 1 + 2 * side
                near_copy(w, kind, u).wait_recv()
                owner = fy if side == 0 else fx
                own = grads[w][rows_of(w, owner, side, u), :].astype(F32)
                come = near[w][kind, cut(w, u), :].astype(F32)
                far_send[w][side, cut(w, u), :] = (own + come).astype(BF)
                far_copy(w, side, u).start()

    def own_sum(w, side, u):
        near_copy(w, 2 * side, u).wait_recv()
        far_copy(w, side, u).wait_recv()
        own = grads[w][rows_of(w, f, side, u), :].astype(F32)
        return own + near[w][2 * side, cut(w, u), :] + far[w][side, cut(w, u), :]

    def z_rows(w, side, u):
        size = rows_half // cuts[w]
        return pl.ds(side * rows_half + u * size, size)

    def z_copy(w, stage, side, u):
        view = z_rows(w, side, u)
        source = (z_own[w], z_own[w], finals[w])[stage].at[view]
        target = (z_in[w].at[0, view], z_in[w].at[1, view], finals[w].at[view])[stage]
        device = (z_near, z_near, z_outer)[stage]
        return remote(
            source, target, z_send[w].at[stage, side, u], z_recv[w].at[stage, side, u],
            (f, device, t),
        )

    def each(w):
        return [(side, u) for u in range(cuts[w]) for side in (0, 1)]

    def z_first(w):
        for side, u in each(w):
            z_own[w][z_rows(w, side, u), :] = own_sum(w, side, u).astype(BF)

            @pl.when(inner == 0)
            def _():
                z_copy(w, 0, side, u).start()

    def z_second(w):
        @pl.when(inner == 1)
        def _():
            for side, u in each(w):
                z_copy(w, 0, side, u).wait_recv()
                at = z_rows(w, side, u)
                total = z_own[w][at, :].astype(F32) + z_in[w][0, at, :]
                z_own[w][at, :] = total.astype(BF)
                z_copy(w, 1, side, u).start()

    def z_third(w):
        @pl.when(inner == 1)
        def _():
            for side, u in each(w):
                z_copy(w, 1, side, u).wait_recv()
                at = z_rows(w, side, u)
                total = z_own[w][at, :].astype(F32) + z_in[w][1, at, :]
                finals[w][at, :] = total.astype(BF)
                z_copy(w, 2, side, u).start()

    def z_done(w):
        @pl.when(inner == 1)
        def _():
            for side, u in each(w):
                z_copy(w, 1, side, u).wait_send()
                z_copy(w, 2, side, u).wait_send()

        @pl.when(inner == 0)
        def _():
            for side, u in each(w):
                z_copy(w, 0, side, u).wait_send()
                z_copy(w, 2, side, u).wait_recv()

    def hops_done(w):
        for u in range(cuts[w]):
            for kind in range(4):
                near_copy(w, kind, u).wait_send()
            for side in (0, 1):
                far_copy(w, side, u).wait_send()

    weight_grad(g_down, grad_low, act)
    first_hop(0)

    def flat_copy(s, h):
        return remote(
            flat.at[s, h], flat_in.at[c], flat_send.at[s, h],
            flat_recv.at[lax.rem(2 * s + h - c + 4, 4)], (f, 2 * s + h, t),
        )

    small_send[0] = jnp.zeros(small_send.shape[1:], F32)
    in_half = (
        lax.div(lax.broadcasted_iota(jnp.int32, (block_rows, 1), 0), half_rows) == t
    ).astype(F32)

    def norm_two_back(s, carry):
        swap(part_b, part_b_in, 1, s).wait()
        grad = part_b[s] + part_b_in[s]
        _, normed, recip = norm_rows(middle[s], gain2[...], bias2[...])
        kept = grad * in_half
        small_send[0, 2:3, :] += jnp.sum(kept * normed, axis=0, keepdims=True)
        small_send[0, 3:4, :] += jnp.sum(kept, axis=0, keepdims=True)
        back = grad_low[s].astype(F32) + norm_back(grad, normed, recip, gain2[...])
        middle_grad[s] = back
        back = back.astype(BF)
        middle_low[s] = back
        flat_rows = mm(back, wo[...], 1, 0).T.astype(BF)
        for h in (0, 1):
            flat[s, h] = flat_rows[h * (width // 3) : (h + 1) * (width // 3)]

            @pl.when(2 * s + h != c)
            def _():
                flat_copy(s, h).start()

            @pl.when(2 * s + h == c)
            def _():
                flat_in[c] = flat[s, h]

        return carry

    lax.fori_loop(0, slots, norm_two_back, 0)
    weight_grad(g_up, second, up_grad)
    second_hop(0)
    first_hop(1)
    weight_grad(g_out, middle_low, low)
    first_hop(2)

    def down(s, carry):
        swap_out = swap(part_a, part_a_in, 2, s)
        part_a[s] = mm(act[s], wd[...], 1, 1)
        swap_out.start()
        return carry

    lax.fori_loop(0, slots, down, 0)

    for name in ("heads", "wq", "pre", "first"):
        loads[name].wait()
    part_width = width // 3
    for h in (0, 1):

        @pl.when(half == h)
        def _():
            lanes = slice(h * part_width, (h + 1) * part_width)
            for kind in range(3):
                for tap in range(3):
                    taps[tap : tap + 1, kind * part_width : (kind + 1) * part_width] = taps3[
                        tap, kind : kind + 1, lanes
                    ]

    key_acc[...] = jnp.zeros_like(key_acc)
    value_acc[...] = jnp.zeros_like(value_acc)
    later[...] = jnp.zeros_like(later)
    conv_acc[...] = jnp.zeros_like(conv_acc)
    length = lens[slot]

    def fg_view(block, rows):
        lanes = pl.ds(block % 2 * model, model)
        return act_grad.at[block // 2, rows, lanes]

    def own_copy(block):
        return remote(
            fg_view(block, theirs), fg_in.at[block], own_send.at[block], own_recv.at[block],
            partner,
        )

    def fg_copy(block):
        return remote(
            fg_low.at[block], fg_all.at[c], fg_ssem.at[block],
            fg_recv.at[lax.rem(block - c + 4, 4)], (f, block, t),
        )

    def hand_over(block):
        own_copy(block).wait_recv()
        fg_low[block] = (fg_view(block, mine)[...] + fg_in[block]).astype(BF)

        @pl.when(block != c)
        def _():
            fg_copy(block).start()

        @pl.when(block == c)
        def _():
            fg_all[c] = fg_low[block]

    for block in reversed(range(blocks)):

        @pl.when(block != c)
        def _():
            remote(
                flat_in.at[block], flat_in.at[block], flat_send.at[0, 0],
                flat_recv.at[lax.rem(c - block + 4, 4)], partner,
            ).wait_recv()

        keys = (block + 1) * block_rows

        def attend(n, carry, block=block, keys=keys):
            head, piece = lax.div(n, tiles), lax.rem(n, tiles)
            at = pl.multiple_of(block * block_rows + piece * tile, tile)
            query = heads[head, pl.ds(at, tile), :]
            key = heads[count + head, 0:keys, :]
            scores = mm(query, key, 1, 1)
            col = lax.broadcasted_iota(jnp.int32, scores.shape, 1)
            row = at + lax.broadcasted_iota(jnp.int32, (tile, 1), 0)
            scores = jnp.where(col < jnp.minimum(row + 1, length), scores, MASKED)
            powers = jnp.exp(scores - jnp.max(scores, axis=-1, keepdims=True))
            probs = powers * (1.0 / jnp.sum(powers, axis=-1, keepdims=True))
            lanes = pl.ds(pl.multiple_of(piece * tile, tile), tile)
            channels = pl.ds(pl.multiple_of(head * HD, HD), HD)
            grad_t = flat_in[block, channels, lanes]
            prob_grad = mm(grad_t.T, heads[2 * count + head, 0:keys, :], 1, 1)
            delta = jnp.sum(probs * prob_grad, axis=-1, keepdims=True)
            score_grad = (probs * (prob_grad - delta)).astype(BF)
            query_t[channels, lanes] = (mm(score_grad, key, 1, 0) * SCALING).T
            key_acc[head, :, 0:keys] += mm(query.T, score_grad, 1, 0)
            value_acc[head, :, 0:keys] += mm(grad_t, probs.astype(BF), 1, 0)
            return carry

        lax.fori_loop(0, count * tiles, attend, 0)
        span = slice(block * block_rows, (block + 1) * block_rows)
        mixed = jnp.concatenate(
            [
                query_t[...],
                key_acc[:, :, span].reshape(part_width, block_rows),
                value_acc[:, :, span].reshape(part_width, block_rows),
            ],
            axis=0,
        )
        mixed_low[...] = mixed.T
        mixed = mixed_low[...]
        joined = jnp.concatenate([mixed, later[...]], axis=0)
        next_one = pltpu.roll(joined, block_rows + 7, 0)[:block_rows]
        next_two = pltpu.roll(joined, block_rows + 6, 0)[:block_rows]
        later[...] = mixed[:8]
        before = pre_all[block].astype(F32)
        for at, shifted_mixed in enumerate((mixed, next_one, next_two)):
            conv_acc[at : at + 1, :] += jnp.sum(before * shifted_mixed, axis=0, keepdims=True)
        conv_acc[3:4, :] += jnp.sum(mixed, axis=0, keepdims=True)
        grad = (taps[0:1] * mixed + taps[1:2] * next_one + taps[2:3] * next_two).astype(BF)
        pre_grad[block] = grad
        fg_view(block, pl.ds(0, block_rows))[...] = mm(grad, wq[...], 1, 1)
        own_copy(block).start()
        if block == 3:
            z_first(0)
        if block == 2:
            hand_over(3)
            second_hop(1)
            z_second(0)
        if block == 1:
            hand_over(2)
            second_hop(2)
            z_third(0)
        if block == 0:
            hand_over(1)

    def qkv_grad(j, carry):
        at = pl.ds(pl.multiple_of(j * 128, 128), 128)
        rows = blocks * block_rows
        lhs = first_all[:, :, at].reshape(rows, 128)
        g_qkv[at, :] = mm(lhs, pre_grad[...].reshape(rows, width), 0, 0).astype(BF)
        return carry

    lax.fori_loop(0, model // 128, qkv_grad, 0)
    first_hop(3)
    hand_over(0)
    z_first(1)
    second_hop(3)

    for s in range(slots):
        swap(part_a, part_a_in, 2, s).wait()
        result[s] = (middle[s] + (part_a[s] + part_a_in[s])).astype(BF)

    z_second(1)
    z_first(2)
    z_second(2)

    def q_copy(stage):
        if stage == 0:
            return remote(
                q_own, q_in, q_send.at[0], q_recv.at[0], (f, lax.rem(c + 2, 4), t)
            )
        return remote(
            q_sum.at[half], q_sum.at[half], q_send.at[1], q_recv.at[1],
            (f, flipped_pair(c), t),
        )

    for side in (0, 1):
        q_own[side * rows_half : (side + 1) * rows_half, :] = own_sum(3, side, 0).astype(BF)
    q_copy(0).start()

    for d in (1, 2, 3):
        source = lax.rem(c - d + 4, 4)
        remote(
            fg_all.at[source], fg_all.at[source], fg_ssem.at[0], fg_recv.at[d], partner
        ).wait_recv()

    def in_copy(s):
        view = input_grad.at[s, mine]
        return remote(view, view, in_send.at[s], in_recv.at[s], partner)

    for s in range(slots):
        grad = fg_all[2 * s].astype(F32) + fg_all[2 * s + 1]
        rows = tok[s, mine, :].astype(F32)
        _, normed, recip = norm_rows(rows, gain1[...], gain1[...])
        small_send[0, 0:1, :] += jnp.sum(grad * normed, axis=0, keepdims=True)
        small_send[0, 1:2, :] += jnp.sum(grad, axis=0, keepdims=True)
        input_grad[s, mine, :] = middle_grad[s, mine, :] + norm_back(
            grad, normed, recip, gain1[...]
        )
        in_copy(s).start()

    for h in (0, 1):

        @pl.when(half == h)
        def _():
            lanes = slice(h * part_width, (h + 1) * part_width)
            for kind in range(3):
                channels = slice(kind * part_width, (kind + 1) * part_width)
                for tap in range(3):
                    row = 4 + 3 * tap + kind
                    small_send[0, row : row + 1, lanes] = conv_acc[tap : tap + 1, channels]
                small_send[0, 13 + kind : 14 + kind, lanes] = conv_acc[3:4, channels]

    peers = [
        (fx, c, t), (fy, c, t), (f, flipped_pair(c), t), (f, lax.rem(c + 2, 4), t), partner
    ]

    def small_copy(stage):
        return remote(
            small_send.at[stage], small_in.at[stage], sm_send.at[stage], sm_recv.at[stage],
            peers[stage],
        )

    def small_add(stage):
        small_copy(stage).wait()
        if stage < 4:
            small_send[stage + 1] = small_send[stage] + small_in[stage]
            small_copy(stage + 1).start()
        else:
            small_out[0:4] = small_send[4, 0:4] + small_in[4, 0:4]
            small_out[4:16] = small_send[4, 4:16]

    small_copy(0).start()
    z_third(1)
    small_add(0)
    z_third(2)
    small_add(1)
    q_copy(0).wait()
    q_sum[half] = (q_own[...].astype(F32) + q_in[...]).astype(BF)
    q_copy(1).start()
    small_add(2)
    small_add(3)
    small_add(4)
    remote(
        q_sum.at[1 - half], q_sum.at[1 - half], q_send.at[1], q_recv.at[1], partner
    ).wait_recv()
    q_copy(1).wait_send()
    for h in (0, 1):
        for kind in range(3):
            qkv_out[kind, :, h * part_width : (h + 1) * part_width] = q_sum[
                h, :, kind * part_width : (kind + 1) * part_width
            ]

    for w in range(4):
        hops_done(w)
    for w in range(3):
        z_done(w)
    for s in range(slots):
        in_copy(s).wait_send()
        view = input_grad.at[s, theirs]
        remote(view, view, in_send.at[s], in_recv.at[s], partner).wait_recv()
        for h in (0, 1):

            @pl.when(2 * s + h != c)
            def _():
                flat_copy(s, h).wait_send()

    for block in range(blocks):
        own_copy(block).wait_send()

        @pl.when(block != c)
        def _():
            fg_copy(block).wait_send()


def backward_call(
    lens, tok, cot, attn, wo, wu, wd, wq, heads, pre_all, first_all, gain1, gain2, bias2, taps3
):
    slots, block_rows, model = tok.shape
    units, width, channels = wu.shape[1], wq.shape[1], wo.shape[1]
    share = model // 4
    part = width // 3
    tall = (slots, block_rows, model)
    wide = (slots, block_rows, units)
    half = block_rows // 2
    columns = [units, units, channels, width]
    cuts = [2, 2, 1, 1]
    dma = pltpu.SemaphoreType.DMA

    def vmem(shape, kind=BF):
        return pltpu.VMEM(tuple(shape), kind)

    return pl.pallas_call(
        backward_kernel,
        name="backward",
        out_shape=[
            jax.ShapeDtypeStruct(tall, BF),
            jax.ShapeDtypeStruct(tall, F32),
            jax.ShapeDtypeStruct((share, units), BF),
            jax.ShapeDtypeStruct((share, units), BF),
            jax.ShapeDtypeStruct((share, channels), BF),
            jax.ShapeDtypeStruct((3, share, channels), BF),
            jax.ShapeDtypeStruct((16, model), F32),
        ],
        in_specs=[SMEM] + [ANY] * 10 + [VMEM] * 4,
        out_specs=[VMEM] * 7,
        scratch_shapes=[
            vmem(tall), vmem(tall), vmem(attn.shape), vmem(wo.shape), vmem(wu.shape),
            vmem(wd.shape), vmem(wq.shape), vmem(heads.shape), vmem(pre_all.shape),
            vmem(first_all.shape),
            vmem((slots, block_rows, channels)), vmem(tall, F32), vmem(tall, F32),
            vmem(tall, F32), vmem(tall, F32), vmem(wide, F32), vmem(tall, F32), vmem(tall, F32),
            vmem(tall), vmem(tall), vmem(wide), vmem(wide), vmem(tall),
            vmem((slots, 2, part, block_rows)), vmem((4, part, block_rows)),
            vmem((model, units)), vmem((model, units)), vmem((model, channels)),
            vmem((model, width)),
            [vmem((4, share // 2, n)) for n in columns],
            [vmem((2, share // 2, n)) for n in columns],
            [vmem((2, share // 2, n)) for n in columns],
            [vmem((share, n)) for n in columns[:3]],
            [vmem((2, share, n)) for n in columns[:3]],
            vmem((share, width)), vmem((share, width)), vmem((2, share, width)),
            vmem((part // HD, HD, 4 * block_rows), F32),
            vmem((part // HD, HD, 4 * block_rows), F32),
            vmem((part, block_rows), F32), vmem((8, width), F32),
            vmem((block_rows, width), F32), vmem((4, block_rows, width)),
            vmem((8, width), F32), vmem((8, width), F32),
            vmem((4, half, model), F32),
            vmem((4, half, model)), vmem((4, half, model)),
            vmem((5, 16, model), F32), vmem((5, 16, model), F32),
            dma((10,)), dma((3, slots)), dma((3, slots)), dma((slots, 2)), dma((4,)),
            [dma((4, n)) for n in cuts], [dma((4, n)) for n in cuts],
            [dma((2, n)) for n in cuts], [dma((2, n)) for n in cuts],
            [dma((3, 2, n)) for n in cuts[:3]], [dma((3, 2, n)) for n in cuts[:3]],
            dma((2,)), dma((2,)),
            dma((4,)), dma((4,)), dma((4,)), dma((4,)), dma((slots,)), dma((slots,)),
            dma((5,)), dma((5,)),
        ],
        compiler_params=pltpu.CompilerParams(
            collective_id=1, has_side_effects=True, vmem_limit_bytes=67043328
        ),
    )(lens, tok, cot, attn, wo, wu, wd, wq, heads, pre_all, first_all, gain1, gain2, bias2, taps3)


def local(
    tokens,
    lengths,
    cotangent,
    ln1_gain,
    ln1_bias,
    qkv_weight,
    conv_kernel,
    conv_bias,
    out_weight,
    ln2_gain,
    ln2_bias,
    up_weight,
    down_weight,
):
    batches, block_rows, model_width = tokens.shape
    all_rows = batches * block_rows
    qkv_full, out_full, up_full_w, down_full_w = (
        lax.all_gather(qkv_weight, "fsdp", axis=0, tiled=True),
        lax.all_gather(out_weight, "fsdp", axis=1, tiled=True),
        lax.all_gather(up_weight, "fsdp", axis=0, tiled=True),
        lax.all_gather(down_weight, "fsdp", axis=1, tiled=True),
    )
    local_width = qkv_full.shape[2]
    local_heads = local_width // HD
    ctx_count = lax.axis_size("ctx")
    slot_span = block_rows * ctx_count
    group_blocks = 4
    key_span = block_rows * group_blocks
    ctx_index = lax.axis_index("ctx")
    positions = ctx_index * block_rows + jnp.arange(block_rows, dtype=jnp.int32)
    span_iota = jnp.arange(key_span, dtype=jnp.int32)
    block_count = (ctx_index * block_rows + block_rows + key_span - 1) // key_span
    token_valid = positions[None, :] < lengths[:, None]

    def span_slice(array_data, block, axis_pos):
        return lax.dynamic_slice_in_dim(array_data, block * key_span, key_span, axis_pos)

    inputs = tokens.astype(jnp.float32).reshape(all_rows, model_width)
    first_out, first_hat, first_recip = layer_norm(inputs, ln1_gain, ln1_bias)
    first_low = first_out.astype(jnp.bfloat16)
    pre_low = jnp.einsum(
        "td,dcn->tcn", first_low, qkv_full, preferred_element_type=jnp.float32
    ).astype(jnp.bfloat16)
    pre_low = pre_low.reshape(batches, block_rows, 3, local_width)
    earlier = shifted(pre_low[:, block_rows - 2 :], "ctx", 1)
    extended = jnp.concatenate([earlier, pre_low], axis=1).astype(jnp.float32)
    conv_out = (
        conv_bias
        + conv_kernel[0] * extended[:, 2:]
        + conv_kernel[1] * extended[:, 1:-1]
        + conv_kernel[2] * extended[:, :-2]
    ).astype(jnp.bfloat16)
    query_heads = conv_out[:, :, 0].reshape(batches, block_rows, local_heads, HD)
    own_pairs = conv_out[:, :, 1:]
    whole_pairs = lax.all_gather(own_pairs, "ctx", axis=1, tiled=True)
    key_heads = whole_pairs[:, :, 0].reshape(batches, slot_span, local_heads, HD)
    value_heads = whole_pairs[:, :, 1].reshape(batches, slot_span, local_heads, HD)

    def stat_step(block, carry):
        row_max, total = carry
        key_pos = block * key_span + span_iota
        scores = tile_scores(
            query_heads, span_slice(key_heads, block, 1), positions, key_pos, lengths
        )
        new_max = jnp.maximum(row_max, jnp.max(scores, axis=-1, keepdims=True))
        total = total * jnp.exp(row_max - new_max) + jnp.sum(
            jnp.exp(scores - new_max), axis=-1, keepdims=True
        )
        return (new_max, total)

    stat_shape = (batches, local_heads, block_rows, 1)
    row_max, total = lax.fori_loop(
        0,
        block_count,
        stat_step,
        (jnp.full(stat_shape, MASKED, jnp.float32), jnp.zeros(stat_shape, jnp.float32)),
    )
    log_total = row_max + jnp.log(total)

    def value_step(block, accum):
        key_pos = block * key_span + span_iota
        scores = tile_scores(
            query_heads, span_slice(key_heads, block, 1), positions, key_pos, lengths
        )
        probs_low = jnp.exp(scores - log_total).astype(jnp.bfloat16)
        return accum + jnp.einsum(
            "mhqk,mkhd->mqhd",
            probs_low,
            span_slice(value_heads, block, 1),
            preferred_element_type=jnp.float32,
        )

    attn_acc = lax.fori_loop(
        0, block_count, value_step, jnp.zeros((batches, block_rows, local_heads, HD), jnp.float32)
    )
    attn_low = attn_acc.reshape(all_rows, local_width).astype(jnp.bfloat16)
    attn_out = lax.psum(jnp.dot(attn_low, out_full, preferred_element_type=jnp.float32), "tp")
    middle = inputs + attn_out
    second_out, second_hat, second_recip = layer_norm(middle, ln2_gain, ln2_bias)
    second_low = second_out.astype(jnp.bfloat16)
    up_full = jnp.dot(second_low, up_full_w, preferred_element_type=jnp.float32)
    rectified = jnp.maximum(up_full, 0.0)
    act_low = (rectified * rectified).astype(jnp.bfloat16)
    ffn_out = lax.psum(jnp.dot(act_low, down_full_w, preferred_element_type=jnp.float32), "tp")
    result = (middle + ffn_out).reshape(batches, block_rows, model_width).astype(jnp.bfloat16)
    grad_out = (
        cotangent.astype(jnp.float32) * token_valid[:, :, None].astype(jnp.float32)
    ).reshape(all_rows, model_width)
    grad_low = grad_out.astype(jnp.bfloat16)
    down_wgrad = jnp.einsum("tf,td->fd", act_low, grad_low, preferred_element_type=jnp.float32)
    act_grad = jnp.einsum("td,fd->tf", grad_low, down_full_w, preferred_element_type=jnp.float32)
    up_grad_low = (act_grad * 2.0 * rectified).astype(jnp.bfloat16)
    up_wgrad = jnp.einsum("td,tf->df", second_low, up_grad_low, preferred_element_type=jnp.float32)
    second_grad = lax.psum(
        jnp.einsum("tf,df->td", up_grad_low, up_full_w, preferred_element_type=jnp.float32), "tp"
    )
    gain_two_grad = jnp.sum(second_grad * second_hat, axis=0)
    bias_two_grad = jnp.sum(second_grad, axis=0)
    middle_grad = grad_out + norm_back(second_grad, second_hat, second_recip, ln2_gain)
    middle_low = middle_grad.astype(jnp.bfloat16)
    out_wgrad = jnp.einsum("tn,td->nd", attn_low, middle_low, preferred_element_type=jnp.float32)
    attn_flat = jnp.einsum(
        "td,nd->tn", middle_low, out_full, preferred_element_type=jnp.float32
    ).astype(jnp.bfloat16)
    attn_grad = attn_flat.reshape(batches, block_rows, local_heads, HD)

    def delta_step(block, accum):
        key_pos = block * key_span + span_iota
        probs_full = jnp.exp(
            tile_scores(query_heads, span_slice(key_heads, block, 1), positions, key_pos, lengths)
            - log_total
        )
        prob_grad = jnp.einsum(
            "mqhd,mkhd->mhqk",
            attn_grad,
            span_slice(value_heads, block, 1),
            preferred_element_type=jnp.float32,
        )
        return accum + jnp.sum(probs_full * prob_grad, axis=-1, keepdims=True)

    delta = lax.fori_loop(0, block_count, delta_step, jnp.zeros(stat_shape, jnp.float32))
    query_zero = jnp.zeros((batches, block_rows, local_heads, HD), jnp.float32)

    def back_step(block, carry):
        accum, buffer = carry
        key_pos = block * key_span + span_iota
        key_part = span_slice(key_heads, block, 1)
        probs_full, prob_grad, score_grad = tile_grads(
            query_heads,
            key_part,
            span_slice(value_heads, block, 1),
            attn_grad,
            log_total,
            delta,
            positions,
            key_pos,
            lengths,
        )
        probs_again = probs_full.astype(jnp.bfloat16)
        accum = (
            accum
            + jnp.einsum(
                "mhqk,mkhd->mqhd", score_grad, key_part, preferred_element_type=jnp.float32
            )
            * SCALING
        )
        key_term = (
            jnp.einsum(
                "mhqk,mqhd->mkhd", score_grad, query_heads, preferred_element_type=jnp.float32
            )
            * SCALING
        )
        value_term = jnp.einsum(
            "mhqk,mqhd->mkhd", probs_again, attn_grad, preferred_element_type=jnp.float32
        )
        stacked = jnp.stack(
            [
                key_term.reshape(batches, key_span, local_width),
                value_term.reshape(batches, key_span, local_width),
            ],
            axis=2,
        )
        buffer = lax.dynamic_update_slice_in_dim(buffer, stacked, block * key_span, 1)
        return (accum, buffer)

    buffer_zero = jnp.zeros((batches, slot_span, 2, local_width), jnp.float32)
    query_grad, pair_terms = lax.fori_loop(0, block_count, back_step, (query_zero, buffer_zero))
    pair_grad = lax.psum_scatter(pair_terms, "ctx", scatter_dimension=1, tiled=True)
    mixed_grad = jnp.concatenate(
        [query_grad.reshape(batches, block_rows, 1, local_width), pair_grad], axis=2
    )
    later = shifted(mixed_grad[:, :2], "ctx", -1)
    ahead = jnp.concatenate([mixed_grad, later], axis=1)
    pre_grad = (
        conv_kernel[0] * ahead[:, :block_rows]
        + conv_kernel[1] * ahead[:, 1 : block_rows + 1]
        + conv_kernel[2] * ahead[:, 2:]
    ).astype(jnp.bfloat16)
    kernel_grad = jnp.stack(
        [
            jnp.sum(extended[:, 2 - offset : 2 - offset + block_rows] * mixed_grad, axis=(0, 1))
            for offset in range(3)
        ]
    )
    shift_grad = jnp.sum(mixed_grad, axis=(0, 1))
    pre_grad = pre_grad.reshape(all_rows, 3, local_width)
    qkv_wgrad = jnp.einsum("td,tcn->dcn", first_low, pre_grad, preferred_element_type=jnp.float32)
    first_grad = lax.psum(
        jnp.einsum("tcn,dcn->td", pre_grad, qkv_full, preferred_element_type=jnp.float32), "tp"
    )
    gain_one_grad = jnp.sum(first_grad * first_hat, axis=0)
    bias_one_grad = jnp.sum(first_grad, axis=0)
    input_grad = middle_grad + norm_back(first_grad, first_hat, first_recip, ln1_gain)
    input_grad = input_grad.reshape(batches, block_rows, model_width)
    summed = lax.psum(
        (
            qkv_wgrad,
            out_wgrad,
            up_wgrad,
            down_wgrad,
            gain_one_grad,
            bias_one_grad,
            kernel_grad,
            shift_grad,
            gain_two_grad,
            bias_two_grad,
        ),
        ("fsdp", "ctx"),
    )
    share_rows = model_width // lax.axis_size("fsdp")
    owner_start = lax.axis_index("fsdp") * share_rows
    qkv_share = lax.dynamic_slice_in_dim(summed[0], owner_start, share_rows, 0)
    out_share = lax.dynamic_slice_in_dim(summed[1], owner_start, share_rows, 1)
    up_share = lax.dynamic_slice_in_dim(summed[2], owner_start, share_rows, 0)
    down_share = lax.dynamic_slice_in_dim(summed[3], owner_start, share_rows, 1)
    small_sums = summed[4:]
    return (
        result,
        input_grad,
        small_sums[0],
        small_sums[1],
        qkv_share,
        small_sums[2],
        small_sums[3],
        out_share,
        small_sums[4],
        small_sums[5],
        up_share,
        down_share,
    )


def local_fast(
    tokens,
    lengths,
    cotangent,
    ln1_gain,
    ln1_bias,
    qkv_weight,
    conv_kernel,
    conv_bias,
    out_weight,
    ln2_gain,
    ln2_bias,
    up_weight,
    down_weight,
):
    model = tokens.shape[2]
    gain1, bias1 = ln1_gain[None], ln1_bias[None]
    wq_all, wo_all, wu_all, wd_all, attn, heads, pre_all, first_all = forward_call(
        lengths, tokens, qkv_weight.transpose(1, 0, 2), out_weight.T, up_weight, down_weight.T,
        gain1, bias1, conv_kernel, conv_bias,
    )
    wq_all, wo_all, wu_all, wd_all = (
        w.reshape(model, w.shape[2]) for w in (wq_all, wo_all, wu_all, wd_all)
    )
    result, input_grad, down, up, out, qkv, small = backward_call(
        lengths, tokens, cotangent, attn, wo_all, wu_all, wd_all, wq_all, heads, pre_all,
        first_all, gain1, ln2_gain[None], ln2_bias[None], conv_kernel,
    )
    channels = out.shape[1]
    return (
        result,
        input_grad,
        small[0],
        small[1],
        qkv.astype(F32).transpose(1, 0, 2),
        small[4:13, :channels].reshape(3, 3, channels),
        small[13:16, :channels],
        out.astype(F32).T,
        small[2],
        small[3],
        up.astype(F32),
        down.astype(F32).T,
    )


def solution(mesh):
    placed = (
        P("fsdp", "ctx", None),
        P("fsdp"),
        P("fsdp", "ctx", None),
        P(),
        P(),
        P("fsdp", None, "tp"),
        P(None, None, "tp"),
        P(None, "tp"),
        P("tp", "fsdp"),
        P(),
        P(),
        P("fsdp", "tp"),
        P("tp", "fsdp"),
    )
    ctx, fsdp, tp = mesh.shape["ctx"], mesh.shape["fsdp"], mesh.shape["tp"]
    return jax.shard_map(
        local_fast if (fsdp, ctx, tp) == (4, 4, 2) else local,
        mesh=mesh,
        in_specs=placed,
        out_specs=(
            P("fsdp", "ctx", None),
            P("fsdp", "ctx", None),
            P(),
            P(),
            P("fsdp", None, "tp"),
            P(None, None, "tp"),
            P(None, "tp"),
            P("tp", "fsdp"),
            P(),
            P(),
            P("fsdp", "tp"),
            P("tp", "fsdp"),
        ),
        check_vma=False,
    )
```

```python
import jax
import jax.numpy as jnp
from jax import lax
from jax.experimental import pallas as pl
from jax.experimental.pallas import tpu as pltpu
from jax.sharding import PartitionSpec as P

HD = 64


EPSILON = 1e-05
SCALING = 0.125
MASKED = -1e30


def shifted(block, axis, distance):
    devices = range(lax.axis_size(axis))
    route = [(i - distance, i) for i in devices if i - distance in devices]
    return lax.ppermute(block, axis, route)


def layer_norm(row_data, norm_gain, shift_bias):
    centred = row_data - jnp.mean(row_data, axis=-1, keepdims=True)
    recip = lax.rsqrt(jnp.mean(centred * centred, axis=-1, keepdims=True) + EPSILON)
    normed = centred * recip
    return (normed * norm_gain + shift_bias, normed, recip)


def norm_back(grad_in, normed, recip, norm_gain):
    scaled = grad_in * norm_gain
    return recip * (
        scaled
        - jnp.mean(scaled, axis=-1, keepdims=True)
        - normed * jnp.mean(scaled * normed, axis=-1, keepdims=True)
    )


def tile_scores(query_part, key_part, query_pos, key_pos, lengths):
    scores = (
        jnp.einsum("mqhd,mkhd->mhqk", query_part, key_part, preferred_element_type=jnp.float32)
        * SCALING
    )
    allowed = (key_pos[None, None, :] <= query_pos[None, :, None]) & (
        key_pos[None, None, :] < lengths[:, None, None]
    )
    return jnp.where(allowed[:, None], scores, MASKED)


def tile_grads(
    query_part, key_part, value_part, grad_part, log_part, delta_part, query_pos, key_pos, lengths
):
    probs_full = jnp.exp(tile_scores(query_part, key_part, query_pos, key_pos, lengths) - log_part)
    prob_grad = jnp.einsum(
        "mqhd,mkhd->mhqk", grad_part, value_part, preferred_element_type=jnp.float32
    )
    score_grad = (probs_full * (prob_grad - delta_part)).astype(jnp.bfloat16)
    return (probs_full, prob_grad, score_grad)


def norm_rows(x, gain, bias):
    centred = x - jnp.mean(x, axis=-1, keepdims=True)
    recip = lax.rsqrt(jnp.mean(centred * centred, axis=-1, keepdims=True) + EPSILON)
    normed = centred * recip
    return normed * gain + bias, normed, recip


BF = jnp.bfloat16
F32 = jnp.float32
MESH = pl.DeviceIdType.MESH
ANY = pl.BlockSpec(memory_space=pl.ANY)
VMEM = pl.BlockSpec(memory_space=pltpu.VMEM)
SMEM = pl.BlockSpec(memory_space=pltpu.SMEM)
CUTS = (2, 2, 1, 2)
DOWN, UP, OUT, QKV = range(4)


def mm(left, right, left_dim, right_dim):
    return lax.dot_general(
        left, right, (((left_dim,), (right_dim,)), ((), ())), preferred_element_type=F32
    )


def remote(source, target, send_sem, recv_sem, device):
    return pltpu.make_async_remote_copy(
        src_ref=source,
        dst_ref=target,
        send_sem=send_sem,
        recv_sem=recv_sem,
        device_id=device,
        device_id_type=MESH,
    )


def span(start, size):
    return pl.ds(pl.multiple_of(start, 16), size)


def lanes_at(start, size):
    return pl.ds(pl.multiple_of(start, 128), size)


def layer_kernel(
    lens, tok_in, cot_in, wq_in, wo_in, wu_in, wd_in,
    gain1, bias1, gain2, bias2, taps3, shift3,
    result, input_grad, down_out, up_out, out_out, q_sum, early_out, late_out,
    tok, cot, wq_buf, wq, wo, wu, wd, taps, shift, prev,
    first_all, pre_all, heads, att, attn,
    low, part_a, part_a_in, part_b, part_b_in, wide_a, middle, middle_grad,
    second, grad_low, act, up_grad, middle_low, flat, flat_in,
    g_down, g_up, g_out, g_qkv, near, far_send, far, z_own, z_in, q_own, q_in,
    key_acc, value_acc, query_t, later, mixed_low, pre_grad, conv_acc,
    fg_in, fg_low, fg_all, early, early_xy, early_z, late, late_xy, late_z,
    load_sem, tok_send, tok_recv, pass_send, pass_recv, w_send, w_recv, att_send, att_recv,
    part_send, part_recv, flat_send, flat_recv,
    near_send, near_recv, far_ssem, far_recv, z_send, z_recv, q_send, q_recv,
    fg_ssem, fg_recv, own_send, own_recv, in_send, in_recv, sm_send, sm_recv,
):
    f, c, t = lax.axis_index("fsdp"), lax.axis_index("ctx"), lax.axis_index("tp")
    fx = f + 1 - 2 * lax.rem(f, 2)
    fy = lax.rem(f + 2, 4)
    fd = lax.rem(fx + 2, 4)
    slot = lax.div(c, 2)
    half = lax.rem(c, 2)
    other = 1 - t
    partner = (f, c, other)
    barrier = pltpu.get_barrier_semaphore()
    peers = [(fx, c, t), (fy, c, t), (fd, c, t), partner]
    peers += [(f, lax.rem(c + d, 4), t) for d in (1, 2, 3)]
    for peer in peers:
        pl.semaphore_signal(barrier, inc=1, device_id=peer, device_id_type=MESH)

    slots, block_rows, model = tok.shape
    width = wq.shape[1]
    part_width = width // 3
    count = part_width // HD
    blocks = 4
    tile = 128
    tiles = block_rows // tile
    half_rows = block_rows // 2
    share = model // 4
    rows_half = share // 2
    mine = span(t * half_rows, half_rows)
    theirs = span(other * half_rows, half_rows)

    def arrived(view, sem):
        remote(view, view, tok_send.at[0], sem, partner).wait_recv()

    wholes = [wd, wu, wo, wq]
    shard_rows = span(f * share, share)
    loads = {}
    for at, (name, source, target) in enumerate(
        [
            ("wq", wq_in, wq_buf),
            ("tok", tok_in, tok),
            (OUT, wo_in, wo.at[shard_rows]),
            (UP, wu_in, wu.at[shard_rows]),
            (DOWN, wd_in, wd.at[shard_rows]),
            ("cot", cot_in, cot),
        ]
    ):
        loads[name] = pltpu.make_async_copy(source, target, load_sem.at[at])
        loads[name].start()
    pl.semaphore_wait(barrier, len(peers))

    def tok_copy(d):
        target = lax.rem(c + d, 4)
        return remote(
            tok_in.at[lax.div(target, 2), mine],
            first_all.at[c, mine],
            tok_send.at[d],
            tok_recv.at[d],
            (f, target, t),
        )

    def tok_pass(source, d):
        view = first_all.at[source, mine]
        return remote(view, view, pass_send.at[d], pass_recv.at[d], partner)

    for d in (1, 3, 2):
        tok_copy(d).start()

    def shard_part(owner, kind):
        if kind < 2:
            return span(owner * share, share)
        return span(owner * share + (kind - 2) * rows_half, rows_half)

    def direct(w, kind):
        view = wholes[w].at[shard_rows]
        target = (fx, c, t) if kind == 0 else (fy, c, t)
        return remote(view, view, w_send.at[w, kind], w_recv.at[w, kind], target)

    def relay(w, kind):
        origin, target = (fx, (fy, c, t)) if kind == 2 else (fy, (fx, c, t))
        view = wholes[w].at[shard_part(origin, kind)]
        return remote(view, view, w_send.at[w, kind], w_recv.at[w, kind], target)

    def landed(w, kind):
        owner = (fx, fy, fd, fd)[kind]
        arrived(wholes[w].at[shard_part(owner, kind)], w_recv.at[w, kind])

    def send_direct(w):
        direct(w, 0).start()
        direct(w, 1).start()

    def pass_on(w):
        landed(w, 0)
        relay(w, 2).start()
        landed(w, 1)
        relay(w, 3).start()

    loads["wq"].wait()
    for h in (0, 1):

        @pl.when(half == h)
        def _():
            lanes = slice(h * part_width, (h + 1) * part_width)
            for kind in range(3):
                target = slice(kind * part_width, (kind + 1) * part_width)
                wq[shard_rows, target] = wq_buf[kind, :, lanes]
                shift[0:1, target] = shift3[kind : kind + 1, lanes]
                for tap in range(3):
                    taps[tap : tap + 1, target] = taps3[tap, kind : kind + 1, lanes]

    send_direct(QKV)
    loads[OUT].wait()
    send_direct(OUT)

    def first_norm(x):
        return norm_rows(x.astype(F32), gain1[...], bias1[...])[0].astype(BF)

    loads["tok"].wait()
    first_all[c] = first_norm(tok[slot])
    loads[UP].wait()
    pass_on(QKV)
    send_direct(UP)
    end = lax.div(c, 3)
    start = lax.div(3 - c, 3)
    for d in (1 + 2 * start, 3 - start - end, 2 - start + end):
        source = lax.rem(c - d + 4, 4)
        arrived(first_all.at[source, mine], tok_recv.at[d])
        first_all[source, mine, :] = first_norm(first_all[source, mine, :])
        tok_pass(source, d).start()

    pass_on(OUT)
    for d in (1 + 2 * start, 3 - start - end, 2 - start + end):
        source = lax.rem(c - d + 4, 4)
        arrived(first_all.at[source, theirs], pass_recv.at[d])
    landed(QKV, 2)
    landed(QKV, 3)
    prev[...] = jnp.zeros_like(prev)

    def project(block, carry):
        pre = mm(first_all[block], wq[...], 1, 0).astype(BF)
        pre_all[block] = pre
        pre = pre.astype(F32)
        joined = jnp.concatenate([prev[...], pre], axis=0)
        prev[...] = pre[-8:]
        out = (
            shift[0:1]
            + taps[0:1] * pre
            + taps[1:2] * pltpu.roll(joined, 1, 0)[8:]
            + taps[2:3] * pltpu.roll(joined, 2, 0)[8:]
        ).astype(BF)
        at = span(block * block_rows, block_rows)
        for head in range(3 * count):
            piece = out[:, head * HD : (head + 1) * HD]
            if head < count:
                piece = (piece.astype(F32) * SCALING).astype(BF)
            heads[head, at, :] = piece
        return carry

    lax.fori_loop(0, blocks, project, 0)
    length = lens[slot]

    def soft(head, at, keys):
        query = heads[head, span(at, tile), :]
        key = heads[count + head, 0:keys, :]
        scores = mm(query, key, 1, 1)
        col = lax.broadcasted_iota(jnp.int32, scores.shape, 1)
        row = at + lax.broadcasted_iota(jnp.int32, (tile, 1), 0)
        scores = jnp.where(col < jnp.minimum(row + 1, length), scores, MASKED)
        powers = jnp.exp(scores - jnp.max(scores, axis=-1, keepdims=True))
        probs = powers * (1.0 / jnp.sum(powers, axis=-1, keepdims=True))
        return query, key, probs

    def att_copy(block):
        return remote(
            att.at[block],
            attn.at[c],
            att_send.at[block],
            att_recv.at[lax.rem(block - c + 4, 4)],
            (f, block, t),
        )

    for block in reversed(range(blocks)):
        keys = (block + 1) * block_rows

        def attend(n, carry, block=block, keys=keys):
            head, piece = lax.div(n, tiles), lax.rem(n, tiles)
            _, _, probs = soft(head, block * block_rows + piece * tile, keys)
            out = mm(probs.astype(BF), heads[2 * count + head, 0:keys, :], 1, 0)
            att[block, span(head * HD, HD), lanes_at(piece * tile, tile)] = out.T.astype(BF)
            return carry

        lax.fori_loop(0, count * tiles, attend, 0)

        @pl.when(block != c)
        def _():
            att_copy(block).start()

        @pl.when(block == c)
        def _():
            attn[c] = att[block]

        if block == 2:
            pass_on(UP)
            loads[DOWN].wait()
            send_direct(DOWN)

    loads["cot"].wait()

    def mask_grad(s, carry):
        row = c * block_rows + lax.broadcasted_iota(jnp.int32, (block_rows, 1), 0)
        grad_low[s] = jnp.where(row < lens[s], cot[s].astype(F32), 0.0).astype(BF)
        return carry

    lax.fori_loop(0, slots, mask_grad, 0)

    def swap(source, target, kind, s):
        return remote(
            source.at[s], target.at[s], part_send.at[kind, s], part_recv.at[kind, s], partner
        )

    for kind in (2, 3):
        landed(OUT, kind)
    for d in (1, 2, 3):
        arrived(attn.at[lax.rem(c - d + 4, 4)], att_recv.at[d])

    def attn_out(s, carry):
        rows = jnp.concatenate([attn[2 * s], attn[2 * s + 1]], axis=0).T
        low[s] = rows
        part_a[s] = mm(rows, wo[...], 1, 1)
        swap(part_a, part_a_in, 0, s).start()
        return carry

    lax.fori_loop(0, slots, attn_out, 0)
    for kind in (2, 3):
        landed(UP, kind)

    def feed(s, carry):
        swap(part_a, part_a_in, 0, s).wait()
        mid = tok[s].astype(F32) + (part_a[s] + part_a_in[s])
        middle[s] = mid
        low_out = norm_rows(mid, gain2[...], bias2[...])[0].astype(BF)
        second[s] = low_out
        rect = jnp.maximum(mm(low_out, wu[...], 1, 0), 0.0)
        wide_a[s] = rect
        act[s] = (rect * rect).astype(BF)
        return carry

    lax.fori_loop(0, slots, feed, 0)

    def weight_grad(target, left, right):
        def step(j, carry):
            at = lanes_at(j * 128, 128)
            rows = left.shape[0] * left.shape[1]
            lhs = left[:, :, at].reshape(rows, 128)
            rhs = right[...].reshape(rows, right.shape[2])
            target[at, :] = mm(lhs, rhs, 0, 0).astype(BF)
            return carry

        lax.fori_loop(0, model // 128, step, 0)

    grads = [g_down, g_up, g_out, g_qkv]
    finals = [down_out, up_out, out_out]
    inner = lax.rem(lax.div(c + 1, 2), 2)
    z_outer = 3 * lax.div(c, 2)
    z_near = jnp.where(c == 0, 1, jnp.where(c == 3, 2, 3 - c))

    def size_of(w):
        return rows_half // CUTS[w]

    def rows_of(w, owner, side, u):
        return span(owner * share + side * rows_half + u * size_of(w), size_of(w))

    def cut(w, u):
        return pl.ds(u * size_of(w), size_of(w))

    def near_copy(w, kind, u):
        owner = (fx, fd, fy, fd)[kind]
        return remote(
            grads[w].at[rows_of(w, owner, kind // 2, u)],
            near[w].at[kind, cut(w, u)],
            near_send[w].at[kind, u],
            near_recv[w].at[kind, u],
            (fx, c, t) if kind < 2 else (fy, c, t),
        )

    def far_copy(w, side, u):
        return remote(
            far_send[w].at[side, cut(w, u)],
            far[w].at[side, cut(w, u)],
            far_ssem[w].at[side, u],
            far_recv[w].at[side, u],
            (fy, c, t) if side == 0 else (fx, c, t),
        )

    def hop_one(w, kinds, u):
        for kind in kinds:
            near_copy(w, kind, u).start()

    def hop_two(w, u):
        for side in (0, 1):
            kind = 1 + 2 * side
            near_copy(w, kind, u).wait_recv()
            owner = fy if side == 0 else fx
            own = grads[w][rows_of(w, owner, side, u), :].astype(F32)
            come = near[w][kind, cut(w, u), :].astype(F32)
            far_send[w][side, cut(w, u), :] = (own + come).astype(BF)
            far_copy(w, side, u).start()

    def own_sum(w, side, u):
        near_copy(w, 2 * side, u).wait_recv()
        far_copy(w, side, u).wait_recv()
        own = grads[w][rows_of(w, f, side, u), :].astype(F32)
        return own + near[w][2 * side, cut(w, u), :] + far[w][side, cut(w, u), :]

    def z_rows(w, side, u):
        return pl.ds(side * rows_half + u * size_of(w), size_of(w))

    def z_copy(w, stage, side, u):
        view = z_rows(w, side, u)
        source = (z_own[w], z_own[w], finals[w])[stage].at[view]
        target = (z_in[w].at[0, view], z_in[w].at[1, view], finals[w].at[view])[stage]
        return remote(
            source, target, z_send[w].at[stage, side, u], z_recv[w].at[stage, side, u],
            (f, (z_near, z_near, z_outer)[stage], t),
        )

    def z_one(w, u):
        for side in (0, 1):
            z_own[w][z_rows(w, side, u), :] = own_sum(w, side, u).astype(BF)

            @pl.when(inner == 0)
            def _():
                z_copy(w, 0, side, u).start()

    def z_two(w, u):
        @pl.when(inner == 1)
        def _():
            for side in (0, 1):
                z_copy(w, 0, side, u).wait_recv()
                at = z_rows(w, side, u)
                z_own[w][at, :] = (z_own[w][at, :].astype(F32) + z_in[w][0, at, :]).astype(BF)
                z_copy(w, 1, side, u).start()

    def z_three(w, u):
        @pl.when(inner == 1)
        def _():
            for side in (0, 1):
                z_copy(w, 1, side, u).wait_recv()
                at = z_rows(w, side, u)
                finals[w][at, :] = (z_own[w][at, :].astype(F32) + z_in[w][1, at, :]).astype(BF)
                z_copy(w, 2, side, u).start()

    def reduced(w):
        for u in range(CUTS[w]):
            for kind in range(4):
                near_copy(w, kind, u).wait_send()
            for side in (0, 1):
                far_copy(w, side, u).wait_send()
                if w == QKV:
                    continue

                @pl.when(inner == 1)
                def _():
                    z_copy(w, 1, side, u).wait_send()
                    z_copy(w, 2, side, u).wait_send()

                @pl.when(inner == 0)
                def _():
                    z_copy(w, 0, side, u).wait_send()
                    z_copy(w, 2, side, u).wait_recv()

    pass_on(DOWN)
    weight_grad(g_down, grad_low, act)
    hop_one(DOWN, (1, 3), 0)
    hop_one(DOWN, (1, 3), 1)
    for kind in (2, 3):
        landed(DOWN, kind)

    def feed_back(s, carry):
        grad = (mm(grad_low[s], wd[...], 1, 0) * 2.0 * wide_a[s]).astype(BF)
        up_grad[s] = grad
        part_b[s] = mm(grad, wu[...], 1, 1)
        swap(part_b, part_b_in, 1, s).start()
        return carry

    lax.fori_loop(0, slots, feed_back, 0)
    weight_grad(g_up, second, up_grad)
    hop_two(DOWN, 0)
    hop_one(DOWN, (0, 2), 0)

    def flat_copy(s, h):
        return remote(
            flat.at[s, h], flat_in.at[c], flat_send.at[s, h],
            flat_recv.at[lax.rem(2 * s + h - c + 4, 4)], (f, 2 * s + h, t),
        )

    early[0] = jnp.zeros(early.shape[1:], F32)
    in_half = (
        lax.div(lax.broadcasted_iota(jnp.int32, (block_rows, 1), 0), half_rows) == t
    ).astype(F32)

    def norm_two_back(s, carry):
        swap(part_b, part_b_in, 1, s).wait()
        grad = part_b[s] + part_b_in[s]
        _, normed, recip = norm_rows(middle[s], gain2[...], bias2[...])
        kept = grad * in_half
        early[0, 0:1, :] += jnp.sum(kept * normed, axis=0, keepdims=True)
        early[0, 1:2, :] += jnp.sum(kept, axis=0, keepdims=True)
        back = grad_low[s].astype(F32) + norm_back(grad, normed, recip, gain2[...])
        middle_grad[s] = back
        back = back.astype(BF)
        middle_low[s] = back
        flat_rows = mm(back, wo[...], 1, 0).T.astype(BF)
        for h in (0, 1):
            flat[s, h] = flat_rows[h * part_width : (h + 1) * part_width]

            @pl.when(2 * s + h != c)
            def _():
                flat_copy(s, h).start()

            @pl.when(2 * s + h == c)
            def _():
                flat_in[c] = flat[s, h]

        return carry

    lax.fori_loop(0, slots, norm_two_back, 0)
    hop_two(DOWN, 1)
    hop_one(DOWN, (0, 2), 1)
    for u in (0, 1):
        hop_one(UP, (1, 3), u)
    for u in (0, 1):
        hop_one(UP, (0, 2), u)
    weight_grad(g_out, middle_low, low)
    hop_one(OUT, (1, 3, 0, 2), 0)

    def down(s, carry):
        part_a[s] = mm(act[s], wd[...], 1, 1)
        swap(part_a, part_a_in, 2, s).start()
        return carry

    lax.fori_loop(0, slots, down, 0)
    key_acc[...] = jnp.zeros_like(key_acc)
    value_acc[...] = jnp.zeros_like(value_acc)
    later[...] = jnp.zeros_like(later)
    conv_acc[...] = jnp.zeros_like(conv_acc)
    for s in range(slots):
        swap(part_a, part_a_in, 2, s).wait()
        result[s] = (middle[s] + (part_a[s] + part_a_in[s])).astype(BF)

    def fg_view(block, rows):
        return wide_a.at[block // 2, rows, pl.ds(block % 2 * model, model)]

    def own_copy(block):
        return remote(
            fg_view(block, theirs), fg_in.at[block], own_send.at[block], own_recv.at[block],
            partner,
        )

    def fg_copy(block):
        return remote(
            fg_low.at[block], fg_all.at[c], fg_ssem.at[block],
            fg_recv.at[lax.rem(block - c + 4, 4)], (f, block, t),
        )

    def hand_over(block):
        own_copy(block).wait_recv()
        fg_low[block] = (fg_view(block, mine)[...] + fg_in[block]).astype(BF)

        @pl.when(block != c)
        def _():
            fg_copy(block).start()

        @pl.when(block == c)
        def _():
            fg_all[c] = fg_low[block]

    z_one(DOWN, 0)
    for block in reversed(range(blocks)):

        @pl.when(block != c)
        def _():
            arrived(flat_in.at[block], flat_recv.at[lax.rem(c - block + 4, 4)])

        keys = (block + 1) * block_rows

        def attend_back(n, carry, block=block, keys=keys):
            head, piece = lax.div(n, tiles), lax.rem(n, tiles)
            query, key, probs = soft(head, block * block_rows + piece * tile, keys)
            lanes = lanes_at(piece * tile, tile)
            channels = span(head * HD, HD)
            grad_t = flat_in[block, channels, lanes]
            prob_grad = mm(grad_t.T, heads[2 * count + head, 0:keys, :], 1, 1)
            delta = jnp.sum(probs * prob_grad, axis=-1, keepdims=True)
            score_grad = (probs * (prob_grad - delta)).astype(BF)
            query_t[channels, lanes] = (mm(score_grad, key, 1, 0) * SCALING).T
            key_acc[head, :, 0:keys] += mm(query.T, score_grad, 1, 0)
            value_acc[head, :, 0:keys] += mm(grad_t, probs.astype(BF), 1, 0)
            return carry

        lax.fori_loop(0, count * tiles, attend_back, 0)
        columns = slice(block * block_rows, (block + 1) * block_rows)
        mixed_low[...] = jnp.concatenate(
            [
                query_t[...],
                key_acc[:, :, columns].reshape(part_width, block_rows),
                value_acc[:, :, columns].reshape(part_width, block_rows),
            ],
            axis=0,
        ).T
        mixed = mixed_low[...]
        joined = jnp.concatenate([mixed, later[...]], axis=0)
        next_one = pltpu.roll(joined, block_rows + 7, 0)[:block_rows]
        next_two = pltpu.roll(joined, block_rows + 6, 0)[:block_rows]
        later[...] = mixed[:8]
        before = pre_all[block].astype(F32)
        for at, moved in enumerate((mixed, next_one, next_two)):
            conv_acc[at : at + 1, :] += jnp.sum(before * moved, axis=0, keepdims=True)
        conv_acc[3:4, :] += jnp.sum(mixed, axis=0, keepdims=True)
        grad = (taps[0:1] * mixed + taps[1:2] * next_one + taps[2:3] * next_two).astype(BF)
        pre_grad[block] = grad
        fg_view(block, pl.ds(0, block_rows))[...] = mm(grad, wq[...], 1, 1)
        own_copy(block).start()
        if block == 3:
            z_one(DOWN, 1)
            z_two(DOWN, 0)
        if block == 2:
            hand_over(3)
            z_two(DOWN, 1)
            hop_two(UP, 0)
            hop_two(UP, 1)
            z_three(DOWN, 0)
        if block == 1:
            hand_over(2)
            z_three(DOWN, 1)
            hop_two(OUT, 0)
        if block == 0:
            hand_over(1)

    weight_grad(g_qkv, first_all, pre_grad)
    for u in (0, 1):
        hop_one(QKV, (1, 3), u)
    for u in (0, 1):
        hop_one(QKV, (0, 2), u)
    hand_over(0)

    smalls = [(early, early_xy, early_z), (late, late_xy, late_z)]

    def tp_copy(k):
        return remote(
            smalls[k][0].at[0], smalls[k][0].at[1], sm_send.at[k, 0], sm_recv.at[k, 0], partner
        )

    def xy_copy(k, at):
        view = smalls[k][1].at[f]
        return remote(
            view, view, sm_send.at[k, 1 + at], sm_recv.at[k, 1 + at], ((fx, fy, fd)[at], c, t)
        )

    def z_small(k, d):
        view = smalls[k][2].at[c]
        return remote(
            view, view, sm_send.at[k, 3 + d], sm_recv.at[k, 3 + d], (f, lax.rem(c + d, 4), t)
        )

    def small_tp(k):
        tp_copy(k).wait()
        mixed_rows = 2 if k == 0 else smalls[k][0].shape[1]
        total = smalls[k][0][0] + smalls[k][0][1]
        smalls[k][1][f] = smalls[k][0][0]
        smalls[k][1][f, 0:mixed_rows, :] = total[0:mixed_rows]
        for at in range(3):
            xy_copy(k, at).start()

    def small_xy(k):
        for at, owner in enumerate((fx, fy, fd)):
            xy_copy(k, at).wait_send()
            arrived(smalls[k][1].at[owner], sm_recv.at[k, 1 + at])
        own = smalls[k][1]
        smalls[k][2][c] = own[0] + own[1] + own[2] + own[3]
        for d in (1, 2, 3):
            z_small(k, d).start()

    def small_z(k, out):
        for d in (1, 2, 3):
            z_small(k, d).wait_send()
            arrived(smalls[k][2].at[lax.rem(c - d + 4, 4)], sm_recv.at[k, 3 + d])
        own = smalls[k][2]
        out[...] = own[0] + own[1] + own[2] + own[3]

    for h in (0, 1):

        @pl.when(half == h)
        def _():
            lanes = slice(h * part_width, (h + 1) * part_width)
            for kind in range(3):
                channels = slice(kind * part_width, (kind + 1) * part_width)
                for tap in range(4):
                    row = 2 + 3 * tap + kind
                    early[0, row : row + 1, lanes] = conv_acc[tap : tap + 1, channels]

    tp_copy(0).start()
    z_one(UP, 0)
    z_one(UP, 1)
    small_tp(0)
    z_one(OUT, 0)
    hop_two(QKV, 0)
    z_two(UP, 0)
    hop_two(QKV, 1)
    z_two(UP, 1)
    z_two(OUT, 0)
    small_xy(0)

    def q_copy(stage, side, u):
        view = z_rows(QKV, side, u)
        if stage == 0:
            source, target, device = q_own.at[view], q_in.at[view], lax.rem(c + 2, 4)
        else:
            source = target = q_sum.at[half, view]
            device = c + 1 - 2 * half
        return remote(
            source, target, q_send.at[stage, side, u], q_recv.at[stage, side, u], (f, device, t)
        )

    def q_one(u):
        for side in (0, 1):
            q_own[z_rows(QKV, side, u), :] = own_sum(QKV, side, u).astype(BF)
            q_copy(0, side, u).start()

    def q_two(u):
        for side in (0, 1):
            q_copy(0, side, u).wait()
            at = z_rows(QKV, side, u)
            q_sum[half, at, :] = (q_own[at, :].astype(F32) + q_in[at, :]).astype(BF)
            q_copy(1, side, u).start()

    for d in (1, 2, 3):
        arrived(fg_all.at[lax.rem(c - d + 4, 4)], fg_recv.at[d])
    late[0] = jnp.zeros(late.shape[1:], F32)
    lane = late.shape[2]

    def in_copy(s):
        view = input_grad.at[s, mine]
        return remote(view, view, in_send.at[s], in_recv.at[s], partner)

    for s in range(slots):
        grad = fg_all[2 * s].astype(F32) + fg_all[2 * s + 1]
        rows = tok[s, mine, :].astype(F32)
        _, normed, recip = norm_rows(rows, gain1[...], bias1[...])
        gain_sum = jnp.sum(grad * normed, axis=0, keepdims=True)
        bias_sum = jnp.sum(grad, axis=0, keepdims=True)
        for at in range(model // lane):
            lanes = slice(at * lane, (at + 1) * lane)
            late[0, at : at + 1, :] += gain_sum[:, lanes]
            late[0, 4 + at : 5 + at, :] += bias_sum[:, lanes]
        input_grad[s, mine, :] = middle_grad[s, mine, :] + norm_back(
            grad, normed, recip, gain1[...]
        )
        in_copy(s).start()

    tp_copy(1).start()
    q_one(0)
    small_tp(1)
    z_three(UP, 0)
    q_one(1)
    z_three(UP, 1)
    small_xy(1)
    z_three(OUT, 0)
    small_z(0, early_out)
    q_two(0)
    q_two(1)
    small_z(1, late_out)

    for w in range(4):
        reduced(w)
        for kind in (0, 1):
            direct(w, kind).wait_send()
        for kind in (2, 3):
            relay(w, kind).wait_send()
    for side in (0, 1):
        for u in (0, 1):
            q_copy(1, side, u).wait_send()
            arrived(q_sum.at[1 - half, z_rows(QKV, side, u)], q_recv.at[1, side, u])
    for d in (1, 2, 3):
        tok_copy(d).wait_send()
        tok_pass(lax.rem(c - d + 4, 4), d).wait_send()
    for s in range(slots):
        in_copy(s).wait_send()
        arrived(input_grad.at[s, theirs], in_recv.at[s])
        for h in (0, 1):

            @pl.when(2 * s + h != c)
            def _():
                flat_copy(s, h).wait_send()

    for block in range(blocks):
        own_copy(block).wait_send()

        @pl.when(block != c)
        def _():
            att_copy(block).wait_send()
            fg_copy(block).wait_send()


def layer_call(
    lens, tok, cot, wq3, wo, wu, wd, gain1, bias1, gain2, bias2, taps3, shift3
):
    slots, block_rows, model = tok.shape
    share, units, channels = wu.shape[0], wu.shape[1], wo.shape[1]
    part = channels // 2
    width = 3 * part
    blocks = 4
    tall = (slots, block_rows, model)
    wide = (slots, block_rows, units)
    half = block_rows // 2
    columns = [units, units, channels, width]
    dma = pltpu.SemaphoreType.DMA

    def vmem(shape, kind=BF):
        return pltpu.VMEM(tuple(shape), kind)

    def struct(shape, kind=BF):
        return jax.ShapeDtypeStruct(tuple(shape), kind)

    return pl.pallas_call(
        layer_kernel,
        name="layer",
        out_shape=[
            struct(tall), struct(tall, F32), struct((share, units)), struct((share, units)),
            struct((share, channels)), struct((2, share, width)), struct((16, model), F32),
            struct((8, 256), F32),
        ],
        in_specs=[SMEM] + [ANY] * 6 + [VMEM] * 6,
        out_specs=[VMEM] * 8,
        scratch_shapes=[
            vmem(tall), vmem(tall), vmem(wq3.shape), vmem((model, width)),
            vmem((model, channels)), vmem((model, units)), vmem((model, units)),
            vmem((8, width), F32), vmem((8, width), F32), vmem((8, width), F32),
            vmem((blocks, block_rows, model)), vmem((blocks, block_rows, width)),
            vmem((width // HD, blocks * block_rows, HD)),
            vmem((blocks, part, block_rows)), vmem((blocks, part, block_rows)),
            vmem((slots, block_rows, channels)), vmem(tall, F32), vmem(tall, F32),
            vmem(tall, F32), vmem(tall, F32), vmem(wide, F32), vmem(tall, F32), vmem(tall, F32),
            vmem(tall), vmem(tall), vmem(wide), vmem(wide), vmem(tall),
            vmem((slots, 2, part, block_rows)), vmem((4, part, block_rows)),
            vmem((model, units)), vmem((model, units)), vmem((model, channels)),
            vmem((model, width)),
            [vmem((4, share // 2, n)) for n in columns],
            [vmem((2, share // 2, n)) for n in columns],
            [vmem((2, share // 2, n)) for n in columns],
            [vmem((share, n)) for n in columns[:3]],
            [vmem((2, share, n)) for n in columns[:3]],
            vmem((share, width)), vmem((share, width)),
            vmem((part // HD, HD, blocks * block_rows), F32),
            vmem((part // HD, HD, blocks * block_rows), F32),
            vmem((part, block_rows), F32), vmem((8, width), F32),
            vmem((block_rows, width), F32), vmem((blocks, block_rows, width)),
            vmem((8, width), F32),
            vmem((blocks, half, model), F32), vmem((blocks, half, model)),
            vmem((blocks, half, model)),
            vmem((2, 16, model), F32), vmem((4, 16, model), F32), vmem((4, 16, model), F32),
            vmem((2, 8, 256), F32), vmem((4, 8, 256), F32), vmem((4, 8, 256), F32),
            dma((6,)), dma((4,)), dma((4,)), dma((4,)), dma((4,)), dma((4, 4)), dma((4, 4)),
            dma((4,)), dma((4,)),
            dma((3, slots)), dma((3, slots)), dma((slots, 2)), dma((4,)),
            [dma((4, n)) for n in CUTS], [dma((4, n)) for n in CUTS],
            [dma((2, n)) for n in CUTS], [dma((2, n)) for n in CUTS],
            [dma((3, 2, n)) for n in CUTS[:3]], [dma((3, 2, n)) for n in CUTS[:3]],
            dma((2, 2, 2)), dma((2, 2, 2)),
            dma((4,)), dma((4,)), dma((4,)), dma((4,)), dma((slots,)), dma((slots,)),
            dma((2, 7)), dma((2, 7)),
        ],
        compiler_params=pltpu.CompilerParams(
            collective_id=0, has_side_effects=True, vmem_limit_bytes=67043328
        ),
    )(lens, tok, cot, wq3, wo, wu, wd, gain1, bias1, gain2, bias2, taps3, shift3)


def finish_kernel(
    result_in, grad_in, down_in, up_in, out_in, qkv_in, early, late,
    result, grad, gain1, bias1, qkv, taps, shift, out, gain2, bias2, up, down,
):
    result[...] = result_in[...]
    grad[...] = grad_in[...]
    down[...] = down_in[...].astype(F32)
    up[...] = up_in[...].astype(F32)
    out[...] = out_in[...].astype(F32)
    part = qkv_in.shape[2] // 3
    for kind in range(3):
        for h in (0, 1):
            qkv[kind, :, h * part : (h + 1) * part] = qkv_in[
                h, :, kind * part : (kind + 1) * part
            ].astype(F32)
    lane = late.shape[1]
    for at in range(gain1.shape[0] // lane):
        lanes = slice(at * lane, (at + 1) * lane)
        gain1[lanes] = late[at]
        bias1[lanes] = late[4 + at]
    gain2[...] = early[0]
    bias2[...] = early[1]
    for tap in range(3):
        taps[tap] = early[2 + 3 * tap : 5 + 3 * tap, 0 : 2 * part]
    shift[...] = early[11:14, 0 : 2 * part]


def finish_call(result, grad, down, up, out, qkv, early, late):
    channels, share, model = out.shape[1], out.shape[0], result.shape[2]

    def struct(shape, kind=F32):
        return jax.ShapeDtypeStruct(tuple(shape), kind)

    vector = struct((model,))
    return pl.pallas_call(
        finish_kernel,
        name="finish",
        out_shape=[
            struct(result.shape, BF), struct(grad.shape), vector, vector,
            struct((3, share, channels)), struct((3, 3, channels)), struct((3, channels)),
            struct(out.shape), vector, vector, struct(up.shape), struct(down.shape),
        ],
    )(result, grad, down, up, out, qkv, early, late)


def local(
    tokens,
    lengths,
    cotangent,
    ln1_gain,
    ln1_bias,
    qkv_weight,
    conv_kernel,
    conv_bias,
    out_weight,
    ln2_gain,
    ln2_bias,
    up_weight,
    down_weight,
):
    batches, block_rows, model_width = tokens.shape
    all_rows = batches * block_rows
    qkv_full, out_full, up_full_w, down_full_w = (
        lax.all_gather(qkv_weight, "fsdp", axis=0, tiled=True),
        lax.all_gather(out_weight, "fsdp", axis=1, tiled=True),
        lax.all_gather(up_weight, "fsdp", axis=0, tiled=True),
        lax.all_gather(down_weight, "fsdp", axis=1, tiled=True),
    )
    local_width = qkv_full.shape[2]
    local_heads = local_width // HD
    ctx_count = lax.axis_size("ctx")
    slot_span = block_rows * ctx_count
    group_blocks = 4
    key_span = block_rows * group_blocks
    ctx_index = lax.axis_index("ctx")
    positions = ctx_index * block_rows + jnp.arange(block_rows, dtype=jnp.int32)
    span_iota = jnp.arange(key_span, dtype=jnp.int32)
    block_count = (ctx_index * block_rows + block_rows + key_span - 1) // key_span
    token_valid = positions[None, :] < lengths[:, None]

    def span_slice(array_data, block, axis_pos):
        return lax.dynamic_slice_in_dim(array_data, block * key_span, key_span, axis_pos)

    inputs = tokens.astype(jnp.float32).reshape(all_rows, model_width)
    first_out, first_hat, first_recip = layer_norm(inputs, ln1_gain, ln1_bias)
    first_low = first_out.astype(jnp.bfloat16)
    pre_low = jnp.einsum(
        "td,dcn->tcn", first_low, qkv_full, preferred_element_type=jnp.float32
    ).astype(jnp.bfloat16)
    pre_low = pre_low.reshape(batches, block_rows, 3, local_width)
    earlier = shifted(pre_low[:, block_rows - 2 :], "ctx", 1)
    extended = jnp.concatenate([earlier, pre_low], axis=1).astype(jnp.float32)
    conv_out = (
        conv_bias
        + conv_kernel[0] * extended[:, 2:]
        + conv_kernel[1] * extended[:, 1:-1]
        + conv_kernel[2] * extended[:, :-2]
    ).astype(jnp.bfloat16)
    query_heads = conv_out[:, :, 0].reshape(batches, block_rows, local_heads, HD)
    own_pairs = conv_out[:, :, 1:]
    whole_pairs = lax.all_gather(own_pairs, "ctx", axis=1, tiled=True)
    key_heads = whole_pairs[:, :, 0].reshape(batches, slot_span, local_heads, HD)
    value_heads = whole_pairs[:, :, 1].reshape(batches, slot_span, local_heads, HD)

    def stat_step(block, carry):
        row_max, total = carry
        key_pos = block * key_span + span_iota
        scores = tile_scores(
            query_heads, span_slice(key_heads, block, 1), positions, key_pos, lengths
        )
        new_max = jnp.maximum(row_max, jnp.max(scores, axis=-1, keepdims=True))
        total = total * jnp.exp(row_max - new_max) + jnp.sum(
            jnp.exp(scores - new_max), axis=-1, keepdims=True
        )
        return (new_max, total)

    stat_shape = (batches, local_heads, block_rows, 1)
    row_max, total = lax.fori_loop(
        0,
        block_count,
        stat_step,
        (jnp.full(stat_shape, MASKED, jnp.float32), jnp.zeros(stat_shape, jnp.float32)),
    )
    log_total = row_max + jnp.log(total)

    def value_step(block, accum):
        key_pos = block * key_span + span_iota
        scores = tile_scores(
            query_heads, span_slice(key_heads, block, 1), positions, key_pos, lengths
        )
        probs_low = jnp.exp(scores - log_total).astype(jnp.bfloat16)
        return accum + jnp.einsum(
            "mhqk,mkhd->mqhd",
            probs_low,
            span_slice(value_heads, block, 1),
            preferred_element_type=jnp.float32,
        )

    attn_acc = lax.fori_loop(
        0, block_count, value_step, jnp.zeros((batches, block_rows, local_heads, HD), jnp.float32)
    )
    attn_low = attn_acc.reshape(all_rows, local_width).astype(jnp.bfloat16)
    attn_out = lax.psum(jnp.dot(attn_low, out_full, preferred_element_type=jnp.float32), "tp")
    middle = inputs + attn_out
    second_out, second_hat, second_recip = layer_norm(middle, ln2_gain, ln2_bias)
    second_low = second_out.astype(jnp.bfloat16)
    up_full = jnp.dot(second_low, up_full_w, preferred_element_type=jnp.float32)
    rectified = jnp.maximum(up_full, 0.0)
    act_low = (rectified * rectified).astype(jnp.bfloat16)
    ffn_out = lax.psum(jnp.dot(act_low, down_full_w, preferred_element_type=jnp.float32), "tp")
    result = (middle + ffn_out).reshape(batches, block_rows, model_width).astype(jnp.bfloat16)
    grad_out = (
        cotangent.astype(jnp.float32) * token_valid[:, :, None].astype(jnp.float32)
    ).reshape(all_rows, model_width)
    grad_low = grad_out.astype(jnp.bfloat16)
    down_wgrad = jnp.einsum("tf,td->fd", act_low, grad_low, preferred_element_type=jnp.float32)
    act_grad = jnp.einsum("td,fd->tf", grad_low, down_full_w, preferred_element_type=jnp.float32)
    up_grad_low = (act_grad * 2.0 * rectified).astype(jnp.bfloat16)
    up_wgrad = jnp.einsum("td,tf->df", second_low, up_grad_low, preferred_element_type=jnp.float32)
    second_grad = lax.psum(
        jnp.einsum("tf,df->td", up_grad_low, up_full_w, preferred_element_type=jnp.float32), "tp"
    )
    gain_two_grad = jnp.sum(second_grad * second_hat, axis=0)
    bias_two_grad = jnp.sum(second_grad, axis=0)
    middle_grad = grad_out + norm_back(second_grad, second_hat, second_recip, ln2_gain)
    middle_low = middle_grad.astype(jnp.bfloat16)
    out_wgrad = jnp.einsum("tn,td->nd", attn_low, middle_low, preferred_element_type=jnp.float32)
    attn_flat = jnp.einsum(
        "td,nd->tn", middle_low, out_full, preferred_element_type=jnp.float32
    ).astype(jnp.bfloat16)
    attn_grad = attn_flat.reshape(batches, block_rows, local_heads, HD)

    def delta_step(block, accum):
        key_pos = block * key_span + span_iota
        probs_full = jnp.exp(
            tile_scores(query_heads, span_slice(key_heads, block, 1), positions, key_pos, lengths)
            - log_total
        )
        prob_grad = jnp.einsum(
            "mqhd,mkhd->mhqk",
            attn_grad,
            span_slice(value_heads, block, 1),
            preferred_element_type=jnp.float32,
        )
        return accum + jnp.sum(probs_full * prob_grad, axis=-1, keepdims=True)

    delta = lax.fori_loop(0, block_count, delta_step, jnp.zeros(stat_shape, jnp.float32))
    query_zero = jnp.zeros((batches, block_rows, local_heads, HD), jnp.float32)

    def back_step(block, carry):
        accum, buffer = carry
        key_pos = block * key_span + span_iota
        key_part = span_slice(key_heads, block, 1)
        probs_full, prob_grad, score_grad = tile_grads(
            query_heads,
            key_part,
            span_slice(value_heads, block, 1),
            attn_grad,
            log_total,
            delta,
            positions,
            key_pos,
            lengths,
        )
        probs_again = probs_full.astype(jnp.bfloat16)
        accum = (
            accum
            + jnp.einsum(
                "mhqk,mkhd->mqhd", score_grad, key_part, preferred_element_type=jnp.float32
            )
            * SCALING
        )
        key_term = (
            jnp.einsum(
                "mhqk,mqhd->mkhd", score_grad, query_heads, preferred_element_type=jnp.float32
            )
            * SCALING
        )
        value_term = jnp.einsum(
            "mhqk,mqhd->mkhd", probs_again, attn_grad, preferred_element_type=jnp.float32
        )
        stacked = jnp.stack(
            [
                key_term.reshape(batches, key_span, local_width),
                value_term.reshape(batches, key_span, local_width),
            ],
            axis=2,
        )
        buffer = lax.dynamic_update_slice_in_dim(buffer, stacked, block * key_span, 1)
        return (accum, buffer)

    buffer_zero = jnp.zeros((batches, slot_span, 2, local_width), jnp.float32)
    query_grad, pair_terms = lax.fori_loop(0, block_count, back_step, (query_zero, buffer_zero))
    pair_grad = lax.psum_scatter(pair_terms, "ctx", scatter_dimension=1, tiled=True)
    mixed_grad = jnp.concatenate(
        [query_grad.reshape(batches, block_rows, 1, local_width), pair_grad], axis=2
    )
    later = shifted(mixed_grad[:, :2], "ctx", -1)
    ahead = jnp.concatenate([mixed_grad, later], axis=1)
    pre_grad = (
        conv_kernel[0] * ahead[:, :block_rows]
        + conv_kernel[1] * ahead[:, 1 : block_rows + 1]
        + conv_kernel[2] * ahead[:, 2:]
    ).astype(jnp.bfloat16)
    kernel_grad = jnp.stack(
        [
            jnp.sum(extended[:, 2 - offset : 2 - offset + block_rows] * mixed_grad, axis=(0, 1))
            for offset in range(3)
        ]
    )
    shift_grad = jnp.sum(mixed_grad, axis=(0, 1))
    pre_grad = pre_grad.reshape(all_rows, 3, local_width)
    qkv_wgrad = jnp.einsum("td,tcn->dcn", first_low, pre_grad, preferred_element_type=jnp.float32)
    first_grad = lax.psum(
        jnp.einsum("tcn,dcn->td", pre_grad, qkv_full, preferred_element_type=jnp.float32), "tp"
    )
    gain_one_grad = jnp.sum(first_grad * first_hat, axis=0)
    bias_one_grad = jnp.sum(first_grad, axis=0)
    input_grad = middle_grad + norm_back(first_grad, first_hat, first_recip, ln1_gain)
    input_grad = input_grad.reshape(batches, block_rows, model_width)
    summed = lax.psum(
        (
            qkv_wgrad,
            out_wgrad,
            up_wgrad,
            down_wgrad,
            gain_one_grad,
            bias_one_grad,
            kernel_grad,
            shift_grad,
            gain_two_grad,
            bias_two_grad,
        ),
        ("fsdp", "ctx"),
    )
    share_rows = model_width // lax.axis_size("fsdp")
    owner_start = lax.axis_index("fsdp") * share_rows
    qkv_share = lax.dynamic_slice_in_dim(summed[0], owner_start, share_rows, 0)
    out_share = lax.dynamic_slice_in_dim(summed[1], owner_start, share_rows, 1)
    up_share = lax.dynamic_slice_in_dim(summed[2], owner_start, share_rows, 0)
    down_share = lax.dynamic_slice_in_dim(summed[3], owner_start, share_rows, 1)
    small_sums = summed[4:]
    return (
        result,
        input_grad,
        small_sums[0],
        small_sums[1],
        qkv_share,
        small_sums[2],
        small_sums[3],
        out_share,
        small_sums[4],
        small_sums[5],
        up_share,
        down_share,
    )


def local_fast(
    tokens,
    lengths,
    cotangent,
    ln1_gain,
    ln1_bias,
    qkv_weight,
    conv_kernel,
    conv_bias,
    out_weight,
    ln2_gain,
    ln2_bias,
    up_weight,
    down_weight,
):
    parts = layer_call(
        lengths, tokens, cotangent, qkv_weight.transpose(1, 0, 2), out_weight.T, up_weight,
        down_weight.T, ln1_gain, ln1_bias, ln2_gain, ln2_bias, conv_kernel, conv_bias,
    )
    result, grad, gain1, bias1, qkv, taps, shift, out, gain2, bias2, up, down = finish_call(*parts)
    return (
        result, grad, gain1, bias1, qkv.transpose(1, 0, 2), taps, shift, out.T, gain2, bias2, up,
        down.T,
    )


def solution(mesh):
    placed = (
        P("fsdp", "ctx", None),
        P("fsdp"),
        P("fsdp", "ctx", None),
        P(),
        P(),
        P("fsdp", None, "tp"),
        P(None, None, "tp"),
        P(None, "tp"),
        P("tp", "fsdp"),
        P(),
        P(),
        P("fsdp", "tp"),
        P("tp", "fsdp"),
    )
    ctx, fsdp, tp = mesh.shape["ctx"], mesh.shape["fsdp"], mesh.shape["tp"]
    return jax.shard_map(
        local_fast if (fsdp, ctx, tp) == (4, 4, 2) else local,
        mesh=mesh,
        in_specs=placed,
        out_specs=(
            P("fsdp", "ctx", None),
            P("fsdp", "ctx", None),
            P(),
            P(),
            P("fsdp", None, "tp"),
            P(None, None, "tp"),
            P(None, "tp"),
            P("tp", "fsdp"),
            P(),
            P(),
            P("fsdp", "tp"),
            P("tp", "fsdp"),
        ),
        check_vma=False,
    )
```

```python
import jax
import jax.numpy as jnp
from jax import lax
from jax.experimental import pallas as pl
from jax.experimental.pallas import tpu as pltpu
from jax.sharding import PartitionSpec as P

HD = 64


EPSILON = 1e-05
SCALING = 0.125
MASKED = -1e30


def shifted(block, axis, distance):
    devices = range(lax.axis_size(axis))
    route = [(i - distance, i) for i in devices if i - distance in devices]
    return lax.ppermute(block, axis, route)


def layer_norm(row_data, norm_gain, shift_bias):
    centred = row_data - jnp.mean(row_data, axis=-1, keepdims=True)
    recip = lax.rsqrt(jnp.mean(centred * centred, axis=-1, keepdims=True) + EPSILON)
    normed = centred * recip
    return (normed * norm_gain + shift_bias, normed, recip)


def norm_back(grad_in, normed, recip, norm_gain):
    scaled = grad_in * norm_gain
    return recip * (
        scaled
        - jnp.mean(scaled, axis=-1, keepdims=True)
        - normed * jnp.mean(scaled * normed, axis=-1, keepdims=True)
    )


def tile_scores(query_part, key_part, query_pos, key_pos, lengths):
    scores = (
        jnp.einsum("mqhd,mkhd->mhqk", query_part, key_part, preferred_element_type=jnp.float32)
        * SCALING
    )
    allowed = (key_pos[None, None, :] <= query_pos[None, :, None]) & (
        key_pos[None, None, :] < lengths[:, None, None]
    )
    return jnp.where(allowed[:, None], scores, MASKED)


def tile_grads(
    query_part, key_part, value_part, grad_part, log_part, delta_part, query_pos, key_pos, lengths
):
    probs_full = jnp.exp(tile_scores(query_part, key_part, query_pos, key_pos, lengths) - log_part)
    prob_grad = jnp.einsum(
        "mqhd,mkhd->mhqk", grad_part, value_part, preferred_element_type=jnp.float32
    )
    score_grad = (probs_full * (prob_grad - delta_part)).astype(jnp.bfloat16)
    return (probs_full, prob_grad, score_grad)


def norm_rows(x, gain, bias):
    centred = x - jnp.mean(x, axis=-1, keepdims=True)
    recip = lax.rsqrt(jnp.mean(centred * centred, axis=-1, keepdims=True) + EPSILON)
    normed = centred * recip
    return normed * gain + bias, normed, recip


BF = jnp.bfloat16
F32 = jnp.float32
MESH = pl.DeviceIdType.MESH
ANY = pl.BlockSpec(memory_space=pl.ANY)
VMEM = pl.BlockSpec(memory_space=pltpu.VMEM)
SMEM = pl.BlockSpec(memory_space=pltpu.SMEM)
CUTS = (2, 2, 1, 2)
DOWN, UP, OUT, QKV = range(4)


def mm(left, right, left_dim, right_dim):
    return lax.dot_general(
        left, right, (((left_dim,), (right_dim,)), ((), ())), preferred_element_type=F32
    )


def remote(source, target, send_sem, recv_sem, device):
    return pltpu.make_async_remote_copy(
        src_ref=source,
        dst_ref=target,
        send_sem=send_sem,
        recv_sem=recv_sem,
        device_id=device,
        device_id_type=MESH,
    )


def span(start, size):
    return pl.ds(pl.multiple_of(start, 16), size)


def lanes_at(start, size):
    return pl.ds(pl.multiple_of(start, 128), size)


def layer_kernel(
    lens, tok_in, cot_in, wq_in, wo_in, wu_in, wd_in,
    gain1, bias1, gain2, bias2, taps3, shift3,
    result, input_grad, down_out, up_out, out_out, q_sum, early_out, late_out,
    tok, cot, wq_buf, wq, wo, wu, wd, taps, shift, prev,
    first_all, pre_all, heads, att, attn,
    low, part_a, part_a_in, part_b, part_b_in, wide_a, middle, middle_grad,
    second, grad_low, act, up_grad, middle_low, flat, flat_in,
    g_down, g_up, g_out, g_qkv, near, far_send, far, z_own, z_in, q_own, q_in,
    key_bias, key_acc, value_acc, query_t, later, mixed_low, pre_grad, conv_acc,
    fg_in, fg_low, pair_in, fg_own, fg_other, early, early_xy, early_z, late, late_xy, late_z,
    load_sem, tok_send, tok_recv, pass_send, pass_recv, w_send, w_recv, att_send, att_recv,
    part_send, part_recv, flat_send, flat_recv,
    near_send, near_recv, far_ssem, far_recv, z_send, z_recv, q_send, q_recv,
    fg_ssem, fg_recv, pair_send, pair_recv, own_send, own_recv, in_send, in_recv, sm_send, sm_recv,
):
    f, c, t = lax.axis_index("fsdp"), lax.axis_index("ctx"), lax.axis_index("tp")
    fx = f + 1 - 2 * lax.rem(f, 2)
    fy = lax.rem(f + 2, 4)
    fd = lax.rem(fx + 2, 4)
    slot = lax.div(c, 2)
    half = lax.rem(c, 2)
    other = 1 - t
    partner = (f, c, other)
    barrier = pltpu.get_barrier_semaphore()
    peers = [(fx, c, t), (fy, c, t), (fd, c, t), partner]
    peers += [(f, lax.rem(c + d, 4), t) for d in (1, 2, 3)]
    for peer in peers:
        pl.semaphore_signal(barrier, inc=1, device_id=peer, device_id_type=MESH)

    slots, block_rows, model = tok.shape
    width = wq.shape[1]
    part_width = width // 3
    count = part_width // HD
    blocks = 4
    half_rows = block_rows // 2
    share = model // 4
    rows_half = share // 2
    mine = span(t * half_rows, half_rows)
    theirs = span(other * half_rows, half_rows)

    def arrived(view, sem):
        remote(view, view, tok_send.at[0], sem, partner).wait_recv()

    wholes = [wd, wu, wo, wq]
    shard_rows = span(f * share, share)
    loads = {}
    for at, (name, source, target) in enumerate(
        [
            ("wq", wq_in, wq_buf),
            ("tok", tok_in, tok),
            (OUT, wo_in, wo.at[shard_rows]),
            (UP, wu_in, wu.at[shard_rows]),
            (DOWN, wd_in, wd.at[shard_rows]),
            ("cot", cot_in, cot),
        ]
    ):
        loads[name] = pltpu.make_async_copy(source, target, load_sem.at[at])
        loads[name].start()
    pl.semaphore_wait(barrier, len(peers))

    inner = lax.rem(lax.div(c + 1, 2), 2)
    mate = c + 1 - 2 * half
    across = 2 - slot
    far_side = 3 - 3 * slot

    def tok_copy(k):
        return remote(
            tok_in.at[slot if k == 0 else 1 - slot, mine],
            first_all.at[c, mine],
            tok_send.at[k],
            tok_recv.at[c],
            (f, mate if k == 0 else across, t),
        )

    def tok_order(k):
        near_in, near_out = ((across, mate), (far_side, across), (mate, far_side))[k]
        return inner * near_in + (1 - inner) * near_out

    def tok_relay(k):
        view = first_all.at[tok_order(k), mine]
        return remote(
            view, view, tok_send.at[2 + k], tok_recv.at[tok_order(k)], (f, mate, t)
        )

    def tok_pass(k):
        view = first_all.at[tok_order(k), mine]
        return remote(view, view, pass_send.at[k], pass_recv.at[k], partner)

    for k in (0, 1):
        tok_copy(k).start()

    def shard_part(owner, kind):
        if kind < 2:
            return span(owner * share, share)
        return span(owner * share + (kind - 2) * rows_half, rows_half)

    def direct(w, kind):
        view = wholes[w].at[shard_rows]
        target = (fx, c, t) if kind == 0 else (fy, c, t)
        return remote(view, view, w_send.at[w, kind], w_recv.at[w, kind], target)

    def relay(w, kind):
        origin, target = (fx, (fy, c, t)) if kind == 2 else (fy, (fx, c, t))
        view = wholes[w].at[shard_part(origin, kind)]
        return remote(view, view, w_send.at[w, kind], w_recv.at[w, kind], target)

    def landed(w, kind):
        owner = (fx, fy, fd, fd)[kind]
        arrived(wholes[w].at[shard_part(owner, kind)], w_recv.at[w, kind])

    def send_direct(w):
        direct(w, 0).start()
        direct(w, 1).start()

    def pass_on(w):
        landed(w, 0)
        relay(w, 2).start()
        landed(w, 1)
        relay(w, 3).start()

    loads["wq"].wait()
    for h in (0, 1):

        @pl.when(half == h)
        def _():
            lanes = slice(h * part_width, (h + 1) * part_width)
            for kind in range(3):
                target = slice(kind * part_width, (kind + 1) * part_width)
                wq[shard_rows, target] = wq_buf[kind, :, lanes]
                shift[0:1, target] = shift3[kind : kind + 1, lanes]
                for tap in range(3):
                    taps[tap : tap + 1, target] = taps3[tap, kind : kind + 1, lanes]

    def first_norm(x):
        return norm_rows(x.astype(F32), gain1[...], bias1[...])[0].astype(BF)

    def own_norm():
        loads["tok"].wait()
        first_all[c] = first_norm(tok[slot])

    def tokens():
        for k in range(3):
            source = tok_order(k)
            arrived(first_all.at[source, mine], tok_recv.at[source])

            @pl.when((inner == 1) | (k == 0))
            def _():
                first_all[source, mine, :] = first_norm(first_all[source, mine, :])

            if k < 2:

                @pl.when(inner == 1)
                def _():
                    tok_relay(k).start()

            tok_pass(k).start()
        for k in range(3):
            arrived(first_all.at[tok_order(k), theirs], pass_recv.at[k])

    def send_out():
        loads[OUT].wait()
        send_direct(OUT)

    def send_up():
        loads[UP].wait()
        send_direct(UP)

    def send_down():
        loads[DOWN].wait()
        send_direct(DOWN)

    def project(block, carry):
        pre = mm(first_all[block], wq[...], 1, 0).astype(BF)
        pre_all[block] = pre
        pre = pre.astype(F32)
        joined = jnp.concatenate([prev[...], pre], axis=0)
        prev[...] = pre[-8:]
        out = (
            shift[0:1]
            + taps[0:1] * pre
            + taps[1:2] * pltpu.roll(joined, 1, 0)[8:]
            + taps[2:3] * pltpu.roll(joined, 2, 0)[8:]
        ).astype(BF)
        at = span(block * block_rows, block_rows)
        for head in range(3 * count):
            piece = out[:, head * HD : (head + 1) * HD]
            if head < count:
                piece = (piece.astype(F32) * SCALING).astype(BF)
            heads[head, at, :] = piece
        return carry

    def projections():
        landed(QKV, 2)
        landed(QKV, 3)
        prev[...] = jnp.zeros_like(prev)
        lax.fori_loop(0, blocks, project, 0)
        at = lax.broadcasted_iota(jnp.int32, key_bias.shape, 1)
        key_bias[...] = jnp.where(at < lens[slot], 0.0, MASKED)

    def soft(head, block):
        at = block * block_rows
        query = heads[head, at : at + block_rows, :]
        key = heads[count + head, 0 : at + block_rows, :]
        scores = mm(query, key, 1, 1) + key_bias[0:1, 0 : at + block_rows]
        col = lax.broadcasted_iota(jnp.int32, (block_rows, block_rows), 1)
        row = lax.broadcasted_iota(jnp.int32, (block_rows, 1), 0)
        last = jnp.where(col <= row, scores[:, at:], MASKED)
        scores = jnp.concatenate([scores[:, :at], last], axis=1) if block else last
        powers = jnp.exp(scores - jnp.max(scores, axis=-1, keepdims=True))
        probs = powers * (1.0 / jnp.sum(powers, axis=-1, keepdims=True))
        return query, key, probs

    def att_copy(block):
        return remote(
            att.at[block],
            attn.at[c],
            att_send.at[block],
            att_recv.at[lax.rem(block - c + 4, 4)],
            (f, block, t),
        )

    def attention(block):
        keys = (block + 1) * block_rows

        def attend(head, carry, block=block, keys=keys):
            _, _, probs = soft(head, block)
            out = mm(probs.astype(BF), heads[2 * count + head, 0:keys, :], 1, 0)
            att[block, span(head * HD, HD), :] = out.T.astype(BF)
            return carry

        lax.fori_loop(0, count, attend, 0)

        @pl.when(block != c)
        def _():
            att_copy(block).start()

        @pl.when(block == c)
        def _():
            attn[c] = att[block]

    def mask_grad(s, carry):
        row = c * block_rows + lax.broadcasted_iota(jnp.int32, (block_rows, 1), 0)
        grad_low[s] = jnp.where(row < lens[s], cot[s].astype(F32), 0.0).astype(BF)
        return carry

    def masks():
        loads["cot"].wait()
        lax.fori_loop(0, slots, mask_grad, 0)

    def swap(source, target, kind, s):
        return remote(
            source.at[s], target.at[s], part_send.at[kind, s], part_recv.at[kind, s], partner
        )

    def attn_out(s, carry):
        rows = jnp.concatenate([attn[2 * s], attn[2 * s + 1]], axis=0).T
        low[s] = rows
        part_a[s] = mm(rows, wo[...], 1, 1)
        swap(part_a, part_a_in, 0, s).start()
        return carry

    def out_projection():
        for kind in (2, 3):
            landed(OUT, kind)
        for d in (1, 2, 3):
            arrived(attn.at[lax.rem(c - d + 4, 4)], att_recv.at[d])
        lax.fori_loop(0, slots, attn_out, 0)

    def feed(s, carry):
        swap(part_a, part_a_in, 0, s).wait()
        mid = tok[s].astype(F32) + (part_a[s] + part_a_in[s])
        middle[s] = mid
        low_out = norm_rows(mid, gain2[...], bias2[...])[0].astype(BF)
        second[s] = low_out
        rect = jnp.maximum(mm(low_out, wu[...], 1, 0), 0.0)
        wide_a[s] = rect
        act[s] = (rect * rect).astype(BF)
        return carry

    def feed_forward():
        for kind in (2, 3):
            landed(UP, kind)
        lax.fori_loop(0, slots, feed, 0)

    def weight_grad(target, left, right):
        def step(j, carry):
            at = lanes_at(j * 128, 128)
            rows = left.shape[0] * left.shape[1]
            lhs = left[:, :, at].reshape(rows, 128)
            rhs = right[...].reshape(rows, right.shape[2])
            target[at, :] = mm(lhs, rhs, 0, 0).astype(BF)
            return carry

        lax.fori_loop(0, model // 128, step, 0)

    grads = [g_down, g_up, g_out, g_qkv]
    finals = [down_out, up_out, out_out]
    z_outer = 3 * lax.div(c, 2)
    z_near = jnp.where(c == 0, 1, jnp.where(c == 3, 2, 3 - c))

    def size_of(w):
        return rows_half // CUTS[w]

    def rows_of(w, owner, side, u):
        return span(owner * share + side * rows_half + u * size_of(w), size_of(w))

    def cut(w, u):
        return pl.ds(u * size_of(w), size_of(w))

    def near_copy(w, kind, u):
        owner = (fx, fd, fy, fd)[kind]
        return remote(
            grads[w].at[rows_of(w, owner, kind // 2, u)],
            near[w].at[kind, cut(w, u)],
            near_send[w].at[kind, u],
            near_recv[w].at[kind, u],
            (fx, c, t) if kind < 2 else (fy, c, t),
        )

    def far_copy(w, side, u):
        return remote(
            far_send[w].at[side, cut(w, u)],
            far[w].at[side, cut(w, u)],
            far_ssem[w].at[side, u],
            far_recv[w].at[side, u],
            (fy, c, t) if side == 0 else (fx, c, t),
        )

    def hop_one(w, kinds, u):
        for kind in kinds:
            near_copy(w, kind, u).start()

    def hop_two(w, u):
        for side in (0, 1):
            kind = 1 + 2 * side
            near_copy(w, kind, u).wait_recv()
            owner = fy if side == 0 else fx
            own = grads[w][rows_of(w, owner, side, u), :].astype(F32)
            come = near[w][kind, cut(w, u), :].astype(F32)
            far_send[w][side, cut(w, u), :] = (own + come).astype(BF)
            far_copy(w, side, u).start()

    def own_sum(w, side, u):
        near_copy(w, 2 * side, u).wait_recv()
        far_copy(w, side, u).wait_recv()
        own = grads[w][rows_of(w, f, side, u), :].astype(F32)
        return own + near[w][2 * side, cut(w, u), :] + far[w][side, cut(w, u), :]

    def z_rows(w, side, u):
        return pl.ds(side * rows_half + u * size_of(w), size_of(w))

    def z_copy(w, stage, side, u):
        view = z_rows(w, side, u)
        source = (z_own[w], z_own[w], finals[w])[stage].at[view]
        target = (z_in[w].at[0, view], z_in[w].at[1, view], finals[w].at[view])[stage]
        return remote(
            source, target, z_send[w].at[stage, side, u], z_recv[w].at[stage, side, u],
            (f, (z_near, z_near, z_outer)[stage], t),
        )

    def z_one(w, u):
        for side in (0, 1):
            z_own[w][z_rows(w, side, u), :] = own_sum(w, side, u).astype(BF)

            @pl.when(inner == 0)
            def _():
                z_copy(w, 0, side, u).start()

    def z_two(w, u):
        @pl.when(inner == 1)
        def _():
            for side in (0, 1):
                z_copy(w, 0, side, u).wait_recv()
                at = z_rows(w, side, u)
                z_own[w][at, :] = (z_own[w][at, :].astype(F32) + z_in[w][0, at, :]).astype(BF)
                z_copy(w, 1, side, u).start()

    def z_three(w, u):
        @pl.when(inner == 1)
        def _():
            for side in (0, 1):
                z_copy(w, 1, side, u).wait_recv()
                at = z_rows(w, side, u)
                finals[w][at, :] = (z_own[w][at, :].astype(F32) + z_in[w][1, at, :]).astype(BF)
                z_copy(w, 2, side, u).start()

    def reduced(w):
        for u in range(CUTS[w]):
            for kind in range(4):
                near_copy(w, kind, u).wait_send()
            for side in (0, 1):
                far_copy(w, side, u).wait_send()
                if w == QKV:
                    continue

                @pl.when(inner == 1)
                def _():
                    z_copy(w, 1, side, u).wait_send()
                    z_copy(w, 2, side, u).wait_send()

                @pl.when(inner == 0)
                def _():
                    z_copy(w, 0, side, u).wait_send()
                    z_copy(w, 2, side, u).wait_recv()

    def feed_back(s):
        if s == 0:
            for kind in (2, 3):
                landed(DOWN, kind)
        grad = (mm(grad_low[s], wd[...], 1, 0) * 2.0 * wide_a[s]).astype(BF)
        up_grad[s] = grad
        part_b[s] = mm(grad, wu[...], 1, 1)
        swap(part_b, part_b_in, 1, s).start()

    def flat_copy(s, h):
        return remote(
            flat.at[s, h], flat_in.at[c], flat_send.at[s, h],
            flat_recv.at[lax.rem(2 * s + h - c + 4, 4)], (f, 2 * s + h, t),
        )

    in_half = (
        lax.div(lax.broadcasted_iota(jnp.int32, (block_rows, 1), 0), half_rows) == t
    ).astype(F32)

    def norm_two_back(s):
        if s == 0:
            early[0] = jnp.zeros(early.shape[1:], F32)
        swap(part_b, part_b_in, 1, s).wait()
        grad = part_b[s] + part_b_in[s]
        _, normed, recip = norm_rows(middle[s], gain2[...], bias2[...])
        kept = grad * in_half
        early[0, 0:1, :] += jnp.sum(kept * normed, axis=0, keepdims=True)
        early[0, 1:2, :] += jnp.sum(kept, axis=0, keepdims=True)
        back = grad_low[s].astype(F32) + norm_back(grad, normed, recip, gain2[...])
        middle_grad[s] = back
        back = back.astype(BF)
        middle_low[s] = back
        flat_rows = mm(back, wo[...], 1, 0).T.astype(BF)
        for h in (0, 1):
            flat[s, h] = flat_rows[h * part_width : (h + 1) * part_width]

            @pl.when(2 * s + h != c)
            def _():
                flat_copy(s, h).start()

            @pl.when(2 * s + h == c)
            def _():
                flat_in[c] = flat[s, h]

    def down(s, carry):
        part_a[s] = mm(act[s], wd[...], 1, 1)
        swap(part_a, part_a_in, 2, s).start()
        return carry

    def feed_down():
        lax.fori_loop(0, slots, down, 0)

    def put_result():
        for s in range(slots):
            swap(part_a, part_a_in, 2, s).wait()
            result[s] = (middle[s] + (part_a[s] + part_a_in[s])).astype(BF)

    def fg_view(block, rows):
        return wide_a.at[block // 2, rows, pl.ds(block % 2 * model, model)]

    def own_copy(block):
        return remote(
            fg_view(block, theirs), fg_in.at[block], own_send.at[block], own_recv.at[block],
            partner,
        )

    def pair_copy(block):
        return remote(
            fg_low.at[block], pair_in.at[block], pair_send.at[block], pair_recv.at[block],
            (f, mate, t),
        )

    def fg_copy(block):
        return remote(
            fg_low.at[block], fg_other, fg_ssem.at[block], fg_recv.at[0], (f, block, t)
        )

    def collects(block):
        return inner * (1 - (mate == block)) + (1 - inner) * (c == block) == 1

    def hand_over(block):
        own_copy(block).wait_recv()
        total = fg_view(block, mine)[...] + fg_in[block]
        fg_in[block] = total

        @pl.when(jnp.logical_not(collects(block)))
        def _():
            fg_low[block] = total.astype(BF)
            pair_copy(block).start()

    def collect(block):
        @pl.when(collects(block))
        def _():
            arrived(pair_in.at[block], pair_recv.at[block])
            total = fg_in[block] + pair_in[block]

            @pl.when(block == c)
            def _():
                fg_own[...] = total

            @pl.when(block != c)
            def _():
                fg_low[block] = total.astype(BF)
                fg_copy(block).start()

    def attention_back(block):
        if block == blocks - 1:
            key_acc[...] = jnp.zeros_like(key_acc)
            value_acc[...] = jnp.zeros_like(value_acc)
            later[...] = jnp.zeros_like(later)
            conv_acc[...] = jnp.zeros_like(conv_acc)

        @pl.when(block != c)
        def _():
            arrived(flat_in.at[block], flat_recv.at[lax.rem(c - block + 4, 4)])

        keys = (block + 1) * block_rows

        def attend_back(head, carry, block=block, keys=keys):
            query, key, probs = soft(head, block)
            channels = span(head * HD, HD)
            grad_t = flat_in[block, channels, :]
            prob_grad = mm(grad_t.T, heads[2 * count + head, 0:keys, :], 1, 1)
            delta = jnp.sum(probs * prob_grad, axis=-1, keepdims=True)
            score_grad = (probs * (prob_grad - delta)).astype(BF)
            query_t[channels, :] = (mm(score_grad, key, 1, 0) * SCALING).T
            key_acc[head, :, 0:keys] += mm(query.T, score_grad, 1, 0)
            value_acc[head, :, 0:keys] += mm(grad_t, probs.astype(BF), 1, 0)
            return carry

        lax.fori_loop(0, count, attend_back, 0)
        columns = slice(block * block_rows, (block + 1) * block_rows)
        mixed_low[...] = jnp.concatenate(
            [
                query_t[...],
                key_acc[:, :, columns].reshape(part_width, block_rows),
                value_acc[:, :, columns].reshape(part_width, block_rows),
            ],
            axis=0,
        ).T
        mixed = mixed_low[...]
        joined = jnp.concatenate([mixed, later[...]], axis=0)
        next_one = pltpu.roll(joined, block_rows + 7, 0)[:block_rows]
        next_two = pltpu.roll(joined, block_rows + 6, 0)[:block_rows]
        later[...] = mixed[:8]
        before = pre_all[block].astype(F32)
        for at, moved in enumerate((mixed, next_one, next_two)):
            conv_acc[at : at + 1, :] += jnp.sum(before * moved, axis=0, keepdims=True)
        conv_acc[3:4, :] += jnp.sum(mixed, axis=0, keepdims=True)
        grad = (taps[0:1] * mixed + taps[1:2] * next_one + taps[2:3] * next_two).astype(BF)
        pre_grad[block] = grad
        fg_view(block, pl.ds(0, block_rows))[...] = mm(grad, wq[...], 1, 1)
        own_copy(block).start()

    smalls = [(early, early_xy, early_z), (late, late_xy, late_z)]

    def tp_copy(k):
        return remote(
            smalls[k][0].at[0], smalls[k][0].at[1], sm_send.at[k, 0], sm_recv.at[k, 0], partner
        )

    def xy_copy(k, at):
        view = smalls[k][1].at[f]
        return remote(
            view, view, sm_send.at[k, 1 + at], sm_recv.at[k, 1 + at], ((fx, fy, fd)[at], c, t)
        )

    def z_small(k, d):
        view = smalls[k][2].at[c]
        return remote(
            view, view, sm_send.at[k, 3 + d], sm_recv.at[k, 3 + d], (f, lax.rem(c + d, 4), t)
        )

    def small_tp(k):
        tp_copy(k).wait()
        mixed_rows = 2 if k == 0 else smalls[k][0].shape[1]
        total = smalls[k][0][0] + smalls[k][0][1]
        smalls[k][1][f] = smalls[k][0][0]
        smalls[k][1][f, 0:mixed_rows, :] = total[0:mixed_rows]
        for at in range(3):
            xy_copy(k, at).start()

    def small_xy(k):
        for at, owner in enumerate((fx, fy, fd)):
            xy_copy(k, at).wait_send()
            arrived(smalls[k][1].at[owner], sm_recv.at[k, 1 + at])
        own = smalls[k][1]
        smalls[k][2][c] = own[0] + own[1] + own[2] + own[3]
        for d in (1, 2, 3):
            z_small(k, d).start()

    def small_z(k, out):
        for d in (1, 2, 3):
            z_small(k, d).wait_send()
            arrived(smalls[k][2].at[lax.rem(c - d + 4, 4)], sm_recv.at[k, 3 + d])
        own = smalls[k][2]
        out[...] = own[0] + own[1] + own[2] + own[3]

    def small_start(k):
        if k == 0:
            for h in (0, 1):

                @pl.when(half == h)
                def _():
                    for tap in range(4):
                        for kind in range(3):
                            at = 3 * tap + kind
                            lane = (at % 2 * 2 + h) * part_width
                            channels = slice(kind * part_width, (kind + 1) * part_width)
                            early[0, 2 + at // 2 : 3 + at // 2, lane : lane + part_width] = (
                                conv_acc[tap : tap + 1, channels]
                            )

        tp_copy(k).start()

    def q_copy(stage, side, u):
        view = z_rows(QKV, side, u)
        if stage == 0:
            source, target, device = q_own.at[view], q_in.at[view], lax.rem(c + 2, 4)
        else:
            source = target = q_sum.at[half, view]
            device = c + 1 - 2 * half
        return remote(
            source, target, q_send.at[stage, side, u], q_recv.at[stage, side, u], (f, device, t)
        )

    def q_one(u):
        for side in (0, 1):
            q_own[z_rows(QKV, side, u), :] = own_sum(QKV, side, u).astype(BF)
            q_copy(0, side, u).start()

    def q_two(u):
        for side in (0, 1):
            q_copy(0, side, u).wait()
            at = z_rows(QKV, side, u)
            q_sum[half, at, :] = (q_own[at, :].astype(F32) + q_in[at, :]).astype(BF)
            q_copy(1, side, u).start()

    lane = late.shape[2]

    def norm_one_back(k):
        s = slot if k == 0 else 1 - slot
        if k == 0:
            late[0] = jnp.zeros(late.shape[1:], F32)
            grad = fg_own[...]
        else:
            arrived(fg_other, fg_recv.at[0])
            grad = fg_other[...].astype(F32)
        _, normed, recip = norm_rows(tok[s, mine, :].astype(F32), gain1[...], bias1[...])
        gain_sum = jnp.sum(grad * normed, axis=0, keepdims=True)
        bias_sum = jnp.sum(grad, axis=0, keepdims=True)
        for at in range(model // lane):
            lanes = slice(at * lane, (at + 1) * lane)
            late[0, at : at + 1, :] += gain_sum[:, lanes]
            late[0, 4 + at : 5 + at, :] += bias_sum[:, lanes]
        input_grad[s, mine, :] = middle_grad[s, mine, :] + norm_back(
            grad, normed, recip, gain1[...]
        )
        in_copy(k).start()

    def in_copy(k):
        view = input_grad.at[slot if k == 0 else 1 - slot, mine]
        return remote(view, view, in_send.at[k], in_recv.at[k], partner)

    send_up()
    send_direct(QKV)
    own_norm()
    send_out()
    pass_on(QKV)
    send_down()
    tokens()
    pass_on(OUT)
    pass_on(UP)
    projections()
    attention(3)
    attention(2)
    attention(1)
    pass_on(DOWN)
    attention(0)
    masks()
    out_projection()
    feed_forward()
    weight_grad(g_down, grad_low, act)
    hop_one(DOWN, (1, 3), 0)
    feed_back(0)
    feed_back(1)
    hop_one(DOWN, (1, 3), 1)
    norm_two_back(0)
    hop_two(DOWN, 0)
    norm_two_back(1)
    weight_grad(g_up, second, up_grad)
    hop_one(DOWN, (0, 2), 0)
    weight_grad(g_out, middle_low, low)
    hop_one(DOWN, (0, 2), 1)
    attention_back(3)
    z_one(DOWN, 0)
    hop_two(DOWN, 1)
    hop_one(UP, (1, 3), 0)
    hop_one(UP, (0, 2), 0)
    attention_back(2)
    z_one(DOWN, 1)
    attention_back(1)
    z_two(DOWN, 0)
    hop_two(UP, 0)
    hand_over(2)
    attention_back(0)
    hand_over(0)
    z_two(DOWN, 1)
    hop_one(OUT, (0, 2), 0)
    feed_down()
    hop_one(UP, (1, 3), 1)
    z_one(UP, 0)
    z_three(DOWN, 0)
    weight_grad(g_qkv, first_all, pre_grad)
    hop_one(QKV, (1, 3), 0)
    collect(2)
    hop_one(QKV, (1, 3), 1)
    collect(0)
    hand_over(3)
    put_result()
    hop_one(QKV, (0, 2), 0)
    hand_over(1)
    z_two(UP, 0)
    small_start(0)
    hop_one(OUT, (1, 3), 0)
    hop_one(UP, (0, 2), 1)
    z_three(DOWN, 1)
    hop_one(QKV, (0, 2), 1)
    collect(3)
    hop_two(QKV, 0)
    hop_two(QKV, 1)
    hop_two(OUT, 0)
    z_three(UP, 0)
    q_one(0)
    collect(1)
    q_one(1)
    small_tp(0)
    hop_two(UP, 1)
    z_one(OUT, 0)
    norm_one_back(0)
    z_one(UP, 1)
    z_two(OUT, 0)
    norm_one_back(1)
    q_two(0)
    small_start(1)
    small_tp(1)
    small_xy(1)
    small_xy(0)
    q_two(1)
    z_two(UP, 1)
    z_three(OUT, 0)
    z_three(UP, 1)
    small_z(0, early_out)
    small_z(1, late_out)
    for w in range(4):
        reduced(w)
        for kind in (0, 1):
            direct(w, kind).wait_send()
        for kind in (2, 3):
            relay(w, kind).wait_send()
    for side in (0, 1):
        for u in (0, 1):
            q_copy(1, side, u).wait_send()
            arrived(q_sum.at[1 - half, z_rows(QKV, side, u)], q_recv.at[1, side, u])
    for k in range(3):
        tok_pass(k).wait_send()
        if k < 2:
            tok_copy(k).wait_send()

            @pl.when(inner == 1)
            def _():
                tok_relay(k).wait_send()

    for s in range(slots):
        in_copy(s).wait_send()
        view = input_grad.at[slot if s == 0 else 1 - slot, theirs]
        arrived(view, in_recv.at[s])
        for h in (0, 1):

            @pl.when(2 * s + h != c)
            def _():
                flat_copy(s, h).wait_send()

    for block in range(blocks):
        own_copy(block).wait_send()

        @pl.when(block != c)
        def _():
            att_copy(block).wait_send()

        @pl.when(jnp.logical_not(collects(block)))
        def _():
            pair_copy(block).wait_send()

        @pl.when(collects(block))
        def _():
            @pl.when(block != c)
            def _():
                fg_copy(block).wait_send()


def layer_call(
    lens, tok, cot, wq3, wo, wu, wd, gain1, bias1, gain2, bias2, taps3, shift3
):
    slots, block_rows, model = tok.shape
    share, units, channels = wu.shape[0], wu.shape[1], wo.shape[1]
    part = channels // 2
    width = 3 * part
    blocks = 4
    tall = (slots, block_rows, model)
    wide = (slots, block_rows, units)
    half = block_rows // 2
    columns = [units, units, channels, width]
    dma = pltpu.SemaphoreType.DMA

    def vmem(shape, kind=BF):
        return pltpu.VMEM(tuple(shape), kind)

    def struct(shape, kind=BF):
        return jax.ShapeDtypeStruct(tuple(shape), kind)

    return pl.pallas_call(
        layer_kernel,
        name="layer",
        out_shape=[
            struct(tall), struct(tall, F32), struct((share, units)), struct((share, units)),
            struct((share, channels)), struct((2, share, width)), struct((8, model), F32),
            struct((8, 256), F32),
        ],
        in_specs=[SMEM] + [ANY] * 6 + [VMEM] * 6,
        out_specs=[VMEM] * 8,
        scratch_shapes=[
            vmem(tall), vmem(tall), vmem(wq3.shape), vmem((model, width)),
            vmem((model, channels)), vmem((model, units)), vmem((model, units)),
            vmem((8, width), F32), vmem((8, width), F32), vmem((8, width), F32),
            vmem((blocks, block_rows, model)), vmem((blocks, block_rows, width)),
            vmem((width // HD, blocks * block_rows, HD)),
            vmem((blocks, part, block_rows)), vmem((blocks, part, block_rows)),
            vmem((slots, block_rows, channels)), vmem(tall, F32), vmem(tall, F32),
            vmem(tall, F32), vmem(tall, F32), vmem(wide, F32), vmem(tall, F32), vmem(tall, F32),
            vmem(tall), vmem(tall), vmem(wide), vmem(wide), vmem(tall),
            vmem((slots, 2, part, block_rows)), vmem((4, part, block_rows)),
            vmem((model, units)), vmem((model, units)), vmem((model, channels)),
            vmem((model, width)),
            [vmem((4, share // 2, n)) for n in columns],
            [vmem((2, share // 2, n)) for n in columns],
            [vmem((2, share // 2, n)) for n in columns],
            [vmem((share, n)) for n in columns[:3]],
            [vmem((2, share, n)) for n in columns[:3]],
            vmem((share, width)), vmem((share, width)),
            vmem((8, blocks * block_rows), F32),
            vmem((part // HD, HD, blocks * block_rows), F32),
            vmem((part // HD, HD, blocks * block_rows), F32),
            vmem((part, block_rows), F32), vmem((8, width), F32),
            vmem((block_rows, width), F32), vmem((blocks, block_rows, width)),
            vmem((8, width), F32),
            vmem((blocks, half, model), F32), vmem((blocks, half, model)),
            vmem((blocks, half, model)), vmem((half, model), F32), vmem((half, model)),
            vmem((2, 8, model), F32), vmem((4, 8, model), F32), vmem((4, 8, model), F32),
            vmem((2, 8, 256), F32), vmem((4, 8, 256), F32), vmem((4, 8, 256), F32),
            dma((6,)), dma((4,)), dma((4,)), dma((4,)), dma((4,)), dma((4, 4)), dma((4, 4)),
            dma((4,)), dma((4,)),
            dma((3, slots)), dma((3, slots)), dma((slots, 2)), dma((4,)),
            [dma((4, n)) for n in CUTS], [dma((4, n)) for n in CUTS],
            [dma((2, n)) for n in CUTS], [dma((2, n)) for n in CUTS],
            [dma((3, 2, n)) for n in CUTS[:3]], [dma((3, 2, n)) for n in CUTS[:3]],
            dma((2, 2, 2)), dma((2, 2, 2)),
            dma((4,)), dma((1,)), dma((4,)), dma((4,)), dma((4,)), dma((4,)), dma((slots,)),
            dma((slots,)),
            dma((2, 7)), dma((2, 7)),
        ],
        compiler_params=pltpu.CompilerParams(
            collective_id=0, has_side_effects=True, vmem_limit_bytes=67043328
        ),
    )(lens, tok, cot, wq3, wo, wu, wd, gain1, bias1, gain2, bias2, taps3, shift3)


def finish_kernel(
    result_in, grad_in, down_in, up_in, out_in, qkv_in, early, late,
    result, grad, gain1, bias1, qkv, taps, shift, out, gain2, bias2, up, down,
):
    result[...] = result_in[...]
    grad[...] = grad_in[...]
    down[...] = down_in[...].astype(F32)
    up[...] = up_in[...].astype(F32)
    out[...] = out_in[...].astype(F32)
    part = qkv_in.shape[2] // 3
    for kind in range(3):
        for h in (0, 1):
            qkv[kind, :, h * part : (h + 1) * part] = qkv_in[
                h, :, kind * part : (kind + 1) * part
            ].astype(F32)
    lane = late.shape[1]
    for at in range(gain1.shape[0] // lane):
        lanes = slice(at * lane, (at + 1) * lane)
        gain1[lanes] = late[at]
        bias1[lanes] = late[4 + at]
    gain2[...] = early[0]
    bias2[...] = early[1]
    for at in range(12):
        lane = at % 2 * 2 * part
        values = early[2 + at // 2 : 3 + at // 2, lane : lane + 2 * part]
        tap, kind = at // 3, at % 3
        if tap < 3:
            taps[tap, kind : kind + 1, :] = values
        else:
            shift[kind : kind + 1, :] = values


def finish_call(result, grad, down, up, out, qkv, early, late):
    channels, share, model = out.shape[1], out.shape[0], result.shape[2]

    def struct(shape, kind=F32):
        return jax.ShapeDtypeStruct(tuple(shape), kind)

    vector = struct((model,))
    return pl.pallas_call(
        finish_kernel,
        name="finish",
        out_shape=[
            struct(result.shape, BF), struct(grad.shape), vector, vector,
            struct((3, share, channels)), struct((3, 3, channels)), struct((3, channels)),
            struct(out.shape), vector, vector, struct(up.shape), struct(down.shape),
        ],
    )(result, grad, down, up, out, qkv, early, late)


def local(
    tokens,
    lengths,
    cotangent,
    ln1_gain,
    ln1_bias,
    qkv_weight,
    conv_kernel,
    conv_bias,
    out_weight,
    ln2_gain,
    ln2_bias,
    up_weight,
    down_weight,
):
    batches, block_rows, model_width = tokens.shape
    all_rows = batches * block_rows
    qkv_full, out_full, up_full_w, down_full_w = (
        lax.all_gather(qkv_weight, "fsdp", axis=0, tiled=True),
        lax.all_gather(out_weight, "fsdp", axis=1, tiled=True),
        lax.all_gather(up_weight, "fsdp", axis=0, tiled=True),
        lax.all_gather(down_weight, "fsdp", axis=1, tiled=True),
    )
    local_width = qkv_full.shape[2]
    local_heads = local_width // HD
    ctx_count = lax.axis_size("ctx")
    slot_span = block_rows * ctx_count
    group_blocks = 4
    key_span = block_rows * group_blocks
    ctx_index = lax.axis_index("ctx")
    positions = ctx_index * block_rows + jnp.arange(block_rows, dtype=jnp.int32)
    span_iota = jnp.arange(key_span, dtype=jnp.int32)
    block_count = (ctx_index * block_rows + block_rows + key_span - 1) // key_span
    token_valid = positions[None, :] < lengths[:, None]

    def span_slice(array_data, block, axis_pos):
        return lax.dynamic_slice_in_dim(array_data, block * key_span, key_span, axis_pos)

    inputs = tokens.astype(jnp.float32).reshape(all_rows, model_width)
    first_out, first_hat, first_recip = layer_norm(inputs, ln1_gain, ln1_bias)
    first_low = first_out.astype(jnp.bfloat16)
    pre_low = jnp.einsum(
        "td,dcn->tcn", first_low, qkv_full, preferred_element_type=jnp.float32
    ).astype(jnp.bfloat16)
    pre_low = pre_low.reshape(batches, block_rows, 3, local_width)
    earlier = shifted(pre_low[:, block_rows - 2 :], "ctx", 1)
    extended = jnp.concatenate([earlier, pre_low], axis=1).astype(jnp.float32)
    conv_out = (
        conv_bias
        + conv_kernel[0] * extended[:, 2:]
        + conv_kernel[1] * extended[:, 1:-1]
        + conv_kernel[2] * extended[:, :-2]
    ).astype(jnp.bfloat16)
    query_heads = conv_out[:, :, 0].reshape(batches, block_rows, local_heads, HD)
    own_pairs = conv_out[:, :, 1:]
    whole_pairs = lax.all_gather(own_pairs, "ctx", axis=1, tiled=True)
    key_heads = whole_pairs[:, :, 0].reshape(batches, slot_span, local_heads, HD)
    value_heads = whole_pairs[:, :, 1].reshape(batches, slot_span, local_heads, HD)

    def stat_step(block, carry):
        row_max, total = carry
        key_pos = block * key_span + span_iota
        scores = tile_scores(
            query_heads, span_slice(key_heads, block, 1), positions, key_pos, lengths
        )
        new_max = jnp.maximum(row_max, jnp.max(scores, axis=-1, keepdims=True))
        total = total * jnp.exp(row_max - new_max) + jnp.sum(
            jnp.exp(scores - new_max), axis=-1, keepdims=True
        )
        return (new_max, total)

    stat_shape = (batches, local_heads, block_rows, 1)
    row_max, total = lax.fori_loop(
        0,
        block_count,
        stat_step,
        (jnp.full(stat_shape, MASKED, jnp.float32), jnp.zeros(stat_shape, jnp.float32)),
    )
    log_total = row_max + jnp.log(total)

    def value_step(block, accum):
        key_pos = block * key_span + span_iota
        scores = tile_scores(
            query_heads, span_slice(key_heads, block, 1), positions, key_pos, lengths
        )
        probs_low = jnp.exp(scores - log_total).astype(jnp.bfloat16)
        return accum + jnp.einsum(
            "mhqk,mkhd->mqhd",
            probs_low,
            span_slice(value_heads, block, 1),
            preferred_element_type=jnp.float32,
        )

    attn_acc = lax.fori_loop(
        0, block_count, value_step, jnp.zeros((batches, block_rows, local_heads, HD), jnp.float32)
    )
    attn_low = attn_acc.reshape(all_rows, local_width).astype(jnp.bfloat16)
    attn_out = lax.psum(jnp.dot(attn_low, out_full, preferred_element_type=jnp.float32), "tp")
    middle = inputs + attn_out
    second_out, second_hat, second_recip = layer_norm(middle, ln2_gain, ln2_bias)
    second_low = second_out.astype(jnp.bfloat16)
    up_full = jnp.dot(second_low, up_full_w, preferred_element_type=jnp.float32)
    rectified = jnp.maximum(up_full, 0.0)
    act_low = (rectified * rectified).astype(jnp.bfloat16)
    ffn_out = lax.psum(jnp.dot(act_low, down_full_w, preferred_element_type=jnp.float32), "tp")
    result = (middle + ffn_out).reshape(batches, block_rows, model_width).astype(jnp.bfloat16)
    grad_out = (
        cotangent.astype(jnp.float32) * token_valid[:, :, None].astype(jnp.float32)
    ).reshape(all_rows, model_width)
    grad_low = grad_out.astype(jnp.bfloat16)
    down_wgrad = jnp.einsum("tf,td->fd", act_low, grad_low, preferred_element_type=jnp.float32)
    act_grad = jnp.einsum("td,fd->tf", grad_low, down_full_w, preferred_element_type=jnp.float32)
    up_grad_low = (act_grad * 2.0 * rectified).astype(jnp.bfloat16)
    up_wgrad = jnp.einsum("td,tf->df", second_low, up_grad_low, preferred_element_type=jnp.float32)
    second_grad = lax.psum(
        jnp.einsum("tf,df->td", up_grad_low, up_full_w, preferred_element_type=jnp.float32), "tp"
    )
    gain_two_grad = jnp.sum(second_grad * second_hat, axis=0)
    bias_two_grad = jnp.sum(second_grad, axis=0)
    middle_grad = grad_out + norm_back(second_grad, second_hat, second_recip, ln2_gain)
    middle_low = middle_grad.astype(jnp.bfloat16)
    out_wgrad = jnp.einsum("tn,td->nd", attn_low, middle_low, preferred_element_type=jnp.float32)
    attn_flat = jnp.einsum(
        "td,nd->tn", middle_low, out_full, preferred_element_type=jnp.float32
    ).astype(jnp.bfloat16)
    attn_grad = attn_flat.reshape(batches, block_rows, local_heads, HD)

    def delta_step(block, accum):
        key_pos = block * key_span + span_iota
        probs_full = jnp.exp(
            tile_scores(query_heads, span_slice(key_heads, block, 1), positions, key_pos, lengths)
            - log_total
        )
        prob_grad = jnp.einsum(
            "mqhd,mkhd->mhqk",
            attn_grad,
            span_slice(value_heads, block, 1),
            preferred_element_type=jnp.float32,
        )
        return accum + jnp.sum(probs_full * prob_grad, axis=-1, keepdims=True)

    delta = lax.fori_loop(0, block_count, delta_step, jnp.zeros(stat_shape, jnp.float32))
    query_zero = jnp.zeros((batches, block_rows, local_heads, HD), jnp.float32)

    def back_step(block, carry):
        accum, buffer = carry
        key_pos = block * key_span + span_iota
        key_part = span_slice(key_heads, block, 1)
        probs_full, prob_grad, score_grad = tile_grads(
            query_heads,
            key_part,
            span_slice(value_heads, block, 1),
            attn_grad,
            log_total,
            delta,
            positions,
            key_pos,
            lengths,
        )
        probs_again = probs_full.astype(jnp.bfloat16)
        accum = (
            accum
            + jnp.einsum(
                "mhqk,mkhd->mqhd", score_grad, key_part, preferred_element_type=jnp.float32
            )
            * SCALING
        )
        key_term = (
            jnp.einsum(
                "mhqk,mqhd->mkhd", score_grad, query_heads, preferred_element_type=jnp.float32
            )
            * SCALING
        )
        value_term = jnp.einsum(
            "mhqk,mqhd->mkhd", probs_again, attn_grad, preferred_element_type=jnp.float32
        )
        stacked = jnp.stack(
            [
                key_term.reshape(batches, key_span, local_width),
                value_term.reshape(batches, key_span, local_width),
            ],
            axis=2,
        )
        buffer = lax.dynamic_update_slice_in_dim(buffer, stacked, block * key_span, 1)
        return (accum, buffer)

    buffer_zero = jnp.zeros((batches, slot_span, 2, local_width), jnp.float32)
    query_grad, pair_terms = lax.fori_loop(0, block_count, back_step, (query_zero, buffer_zero))
    pair_grad = lax.psum_scatter(pair_terms, "ctx", scatter_dimension=1, tiled=True)
    mixed_grad = jnp.concatenate(
        [query_grad.reshape(batches, block_rows, 1, local_width), pair_grad], axis=2
    )
    later = shifted(mixed_grad[:, :2], "ctx", -1)
    ahead = jnp.concatenate([mixed_grad, later], axis=1)
    pre_grad = (
        conv_kernel[0] * ahead[:, :block_rows]
        + conv_kernel[1] * ahead[:, 1 : block_rows + 1]
        + conv_kernel[2] * ahead[:, 2:]
    ).astype(jnp.bfloat16)
    kernel_grad = jnp.stack(
        [
            jnp.sum(extended[:, 2 - offset : 2 - offset + block_rows] * mixed_grad, axis=(0, 1))
            for offset in range(3)
        ]
    )
    shift_grad = jnp.sum(mixed_grad, axis=(0, 1))
    pre_grad = pre_grad.reshape(all_rows, 3, local_width)
    qkv_wgrad = jnp.einsum("td,tcn->dcn", first_low, pre_grad, preferred_element_type=jnp.float32)
    first_grad = lax.psum(
        jnp.einsum("tcn,dcn->td", pre_grad, qkv_full, preferred_element_type=jnp.float32), "tp"
    )
    gain_one_grad = jnp.sum(first_grad * first_hat, axis=0)
    bias_one_grad = jnp.sum(first_grad, axis=0)
    input_grad = middle_grad + norm_back(first_grad, first_hat, first_recip, ln1_gain)
    input_grad = input_grad.reshape(batches, block_rows, model_width)
    summed = lax.psum(
        (
            qkv_wgrad,
            out_wgrad,
            up_wgrad,
            down_wgrad,
            gain_one_grad,
            bias_one_grad,
            kernel_grad,
            shift_grad,
            gain_two_grad,
            bias_two_grad,
        ),
        ("fsdp", "ctx"),
    )
    share_rows = model_width // lax.axis_size("fsdp")
    owner_start = lax.axis_index("fsdp") * share_rows
    qkv_share = lax.dynamic_slice_in_dim(summed[0], owner_start, share_rows, 0)
    out_share = lax.dynamic_slice_in_dim(summed[1], owner_start, share_rows, 1)
    up_share = lax.dynamic_slice_in_dim(summed[2], owner_start, share_rows, 0)
    down_share = lax.dynamic_slice_in_dim(summed[3], owner_start, share_rows, 1)
    small_sums = summed[4:]
    return (
        result,
        input_grad,
        small_sums[0],
        small_sums[1],
        qkv_share,
        small_sums[2],
        small_sums[3],
        out_share,
        small_sums[4],
        small_sums[5],
        up_share,
        down_share,
    )


def local_fast(
    tokens,
    lengths,
    cotangent,
    ln1_gain,
    ln1_bias,
    qkv_weight,
    conv_kernel,
    conv_bias,
    out_weight,
    ln2_gain,
    ln2_bias,
    up_weight,
    down_weight,
):
    parts = layer_call(
        lengths, tokens, cotangent, qkv_weight.transpose(1, 0, 2), out_weight.T, up_weight,
        down_weight.T, ln1_gain, ln1_bias, ln2_gain, ln2_bias, conv_kernel, conv_bias,
    )
    result, grad, gain1, bias1, qkv, taps, shift, out, gain2, bias2, up, down = finish_call(*parts)
    return (
        result, grad, gain1, bias1, qkv.transpose(1, 0, 2), taps, shift, out.T, gain2, bias2, up,
        down.T,
    )


def solution(mesh):
    placed = (
        P("fsdp", "ctx", None),
        P("fsdp"),
        P("fsdp", "ctx", None),
        P(),
        P(),
        P("fsdp", None, "tp"),
        P(None, None, "tp"),
        P(None, "tp"),
        P("tp", "fsdp"),
        P(),
        P(),
        P("fsdp", "tp"),
        P("tp", "fsdp"),
    )
    ctx, fsdp, tp = mesh.shape["ctx"], mesh.shape["fsdp"], mesh.shape["tp"]
    return jax.shard_map(
        local_fast if (fsdp, ctx, tp) == (4, 4, 2) else local,
        mesh=mesh,
        in_specs=placed,
        out_specs=(
            P("fsdp", "ctx", None),
            P("fsdp", "ctx", None),
            P(),
            P(),
            P("fsdp", None, "tp"),
            P(None, None, "tp"),
            P(None, "tp"),
            P("tp", "fsdp"),
            P(),
            P(),
            P("fsdp", "tp"),
            P("tp", "fsdp"),
        ),
        check_vma=False,
    )
```

```python
import jax
import jax.numpy as jnp
from jax import lax
from jax.experimental import pallas as pl
from jax.experimental.pallas import tpu as pltpu
from jax.sharding import PartitionSpec as P

HD = 64


EPSILON = 1e-05
SCALING = 0.125
MASKED = -1e30


def shifted(block, axis, distance):
    devices = range(lax.axis_size(axis))
    route = [(i - distance, i) for i in devices if i - distance in devices]
    return lax.ppermute(block, axis, route)


def layer_norm(row_data, norm_gain, shift_bias):
    centred = row_data - jnp.mean(row_data, axis=-1, keepdims=True)
    recip = lax.rsqrt(jnp.mean(centred * centred, axis=-1, keepdims=True) + EPSILON)
    normed = centred * recip
    return (normed * norm_gain + shift_bias, normed, recip)


def norm_back(grad_in, normed, recip, norm_gain):
    scaled = grad_in * norm_gain
    return recip * (
        scaled
        - jnp.mean(scaled, axis=-1, keepdims=True)
        - normed * jnp.mean(scaled * normed, axis=-1, keepdims=True)
    )


def tile_scores(query_part, key_part, query_pos, key_pos, lengths):
    scores = (
        jnp.einsum("mqhd,mkhd->mhqk", query_part, key_part, preferred_element_type=jnp.float32)
        * SCALING
    )
    allowed = (key_pos[None, None, :] <= query_pos[None, :, None]) & (
        key_pos[None, None, :] < lengths[:, None, None]
    )
    return jnp.where(allowed[:, None], scores, MASKED)


def tile_grads(
    query_part, key_part, value_part, grad_part, log_part, delta_part, query_pos, key_pos, lengths
):
    probs_full = jnp.exp(tile_scores(query_part, key_part, query_pos, key_pos, lengths) - log_part)
    prob_grad = jnp.einsum(
        "mqhd,mkhd->mhqk", grad_part, value_part, preferred_element_type=jnp.float32
    )
    score_grad = (probs_full * (prob_grad - delta_part)).astype(jnp.bfloat16)
    return (probs_full, prob_grad, score_grad)


def norm_rows(x, gain, bias):
    centred = x - jnp.mean(x, axis=-1, keepdims=True)
    recip = lax.rsqrt(jnp.mean(centred * centred, axis=-1, keepdims=True) + EPSILON)
    normed = centred * recip
    return normed * gain + bias, normed, recip


BF = jnp.bfloat16
F32 = jnp.float32
MESH = pl.DeviceIdType.MESH
ANY = pl.BlockSpec(memory_space=pl.ANY)
VMEM = pl.BlockSpec(memory_space=pltpu.VMEM)
SMEM = pl.BlockSpec(memory_space=pltpu.SMEM)
CUTS = (3, 3, 1, 2)
DOWN, UP, OUT, QKV = range(4)


def mm(left, right, left_dim, right_dim):
    return lax.dot_general(
        left, right, (((left_dim,), (right_dim,)), ((), ())), preferred_element_type=F32
    )


def remote(source, target, send_sem, recv_sem, device):
    return pltpu.make_async_remote_copy(
        src_ref=source,
        dst_ref=target,
        send_sem=send_sem,
        recv_sem=recv_sem,
        device_id=device,
        device_id_type=MESH,
    )


def span(start, size):
    return pl.ds(pl.multiple_of(start, 16), size)


def lanes_at(start, size):
    return pl.ds(pl.multiple_of(start, 128), size)


def layer_kernel(
    lens, tok_in, cot_in, wq_in, wo_in, wu_in, wd_in,
    gain1, bias1, gain2, bias2, taps3, shift3,
    result, input_grad, down_out, up_out, out_out, q_sum, early_out, late_out,
    tok, cot, wq_buf, wq, wo, wu, wd, taps, shift, prev,
    first_all, pre_all, heads, att, attn,
    low, part_a, part_a_in, part_b, part_b_in, wide_a, middle, middle_grad,
    second, grad_low, act, up_grad, middle_low, flat, flat_in,
    g_down, g_up, g_out, g_qkv, near, far_send, far, z_own, z_in, q_own, q_in,
    key_bias, key_acc, value_acc, query_t, later, mixed_low, pre_grad, conv_acc,
    fg_in, fg_low, pair_in, fg_own, fg_other, early, early_xy, early_z, late, late_xy, late_z,
    load_sem, tok_send, tok_recv, pass_send, pass_recv, mate_send, mate_recv, w_send, w_recv, att_send, att_recv,
    part_send, part_recv, flat_send, flat_recv,
    near_send, near_recv, far_ssem, far_recv, z_send, z_recv, q_send, q_recv,
    fg_ssem, fg_recv, pair_send, pair_recv, own_send, own_recv, in_send, in_recv, sm_send, sm_recv,
):
    f, c, t = lax.axis_index("fsdp"), lax.axis_index("ctx"), lax.axis_index("tp")
    fx = f + 1 - 2 * lax.rem(f, 2)
    fy = lax.rem(f + 2, 4)
    fd = lax.rem(fx + 2, 4)
    slot = lax.div(c, 2)
    half = lax.rem(c, 2)
    other = 1 - t
    partner = (f, c, other)
    barrier = pltpu.get_barrier_semaphore()
    peers = [(fx, c, t), (fy, c, t), (fd, c, t), partner]
    peers += [(f, lax.rem(c + d, 4), t) for d in (1, 2, 3)]
    for peer in peers:
        pl.semaphore_signal(barrier, inc=1, device_id=peer, device_id_type=MESH)

    slots, block_rows, model = tok.shape
    width = wq.shape[1]
    part_width = width // 3
    count = part_width // HD
    blocks = 4
    half_rows = block_rows // 2
    share = model // 4
    rows_half = share // 2
    mine = span(t * half_rows, half_rows)
    theirs = span(other * half_rows, half_rows)

    def arrived(view, sem):
        remote(view, view, tok_send.at[0], sem, partner).wait_recv()

    wholes = [wd, wu, wo, wq]
    shard_rows = span(f * share, share)
    loads = {}
    for at, (name, source, target) in enumerate(
        [
            ("wq", wq_in, wq_buf),
            ("tok", tok_in, tok),
            (OUT, wo_in, wo.at[shard_rows]),
            (UP, wu_in, wu.at[shard_rows]),
            (DOWN, wd_in, wd.at[shard_rows]),
            ("cot", cot_in, cot),
        ]
    ):
        loads[name] = pltpu.make_async_copy(source, target, load_sem.at[at])
        loads[name].start()
    pl.semaphore_wait(barrier, len(peers))

    inner = lax.rem(lax.div(c + 1, 2), 2)
    mate = c + 1 - 2 * half
    across = 2 - slot
    far_side = 3 - 3 * slot

    def tok_copy(k):
        return remote(
            tok_in.at[slot if k == 0 else 1 - slot, mine],
            first_all.at[c, mine],
            tok_send.at[k],
            tok_recv.at[c],
            (f, mate if k == 0 else across, t),
        )

    def tok_order(k):
        near_in, near_out = ((across, mate), (far_side, across), (mate, far_side))[k]
        return inner * near_in + (1 - inner) * near_out

    def tok_relay(k):
        view = first_all.at[tok_order(k), mine]
        return remote(
            view, view, tok_send.at[2 + k], tok_recv.at[tok_order(k)], (f, mate, t)
        )

    def tok_pass(k):
        view = first_all.at[tok_order(k), mine]
        return remote(view, view, pass_send.at[k], pass_recv.at[k], partner)

    for k in (0, 1):
        tok_copy(k).start()


    def shard_part(w, owner, kind):
        start, size = owner * share, share
        if w == DOWN:
            start, size = start + half * rows_half, rows_half
        if kind < 2:
            return span(start, size)
        return span(start + (kind - 2) * (size // 2), size // 2)

    def direct(w, kind):
        view = wholes[w].at[shard_part(w, f, 0)]
        target = (fx, c, t) if kind == 0 else (fy, c, t)
        return remote(view, view, w_send.at[w, kind], w_recv.at[w, kind], target)

    def relay(w, kind):
        origin, target = (fx, (fy, c, t)) if kind == 2 else (fy, (fx, c, t))
        view = wholes[w].at[shard_part(w, origin, kind)]
        return remote(view, view, w_send.at[w, kind], w_recv.at[w, kind], target)

    def landed(w, kind):
        owner = (fx, fy, fd, fd)[kind]
        arrived(wholes[w].at[shard_part(w, owner, kind)], w_recv.at[w, kind])

    def send_direct(w):
        direct(w, 0).start()
        direct(w, 1).start()

    def pass_on(w):
        landed(w, 0)
        relay(w, 2).start()
        landed(w, 1)
        relay(w, 3).start()

    def half_of(k, side):
        return wd.at[span((fx, fy, fd)[k] * share + side * rows_half, rows_half)]

    def mate_copy(k):
        view = half_of(k, half)
        return remote(view, view, mate_send.at[k], mate_recv.at[k], (f, mate, t))

    def pass_down():
        for k in (0, 1):
            landed(DOWN, k)
            relay(DOWN, 2 + k).start()
            mate_copy(k).start()

    def pass_down_last():
        landed(DOWN, 2)
        landed(DOWN, 3)
        mate_copy(2).start()

    loads["wq"].wait()
    for h in (0, 1):

        @pl.when(half == h)
        def _():
            lanes = slice(h * part_width, (h + 1) * part_width)
            for kind in range(3):
                target = slice(kind * part_width, (kind + 1) * part_width)
                wq[shard_rows, target] = wq_buf[kind, :, lanes]
                shift[0:1, target] = shift3[kind : kind + 1, lanes]
                for tap in range(3):
                    taps[tap : tap + 1, target] = taps3[tap, kind : kind + 1, lanes]

    def first_norm(x):
        return norm_rows(x.astype(F32), gain1[...], bias1[...])[0].astype(BF)

    def own_norm():
        loads["tok"].wait()
        first_all[c] = first_norm(tok[slot])

    def tokens(k):
        source = tok_order(k)
        arrived(first_all.at[source, mine], tok_recv.at[source])

        @pl.when((inner == 1) | (k == 0))
        def _():
            first_all[source, mine, :] = first_norm(first_all[source, mine, :])

        if k < 2:

            @pl.when(inner == 1)
            def _():
                tok_relay(k).start()

        tok_pass(k).start()

    def tokens_passed():
        for k in range(3):
            arrived(first_all.at[tok_order(k), theirs], pass_recv.at[k])

    def send_out():
        loads[OUT].wait()
        send_direct(OUT)

    def send_up():
        loads[UP].wait()
        send_direct(UP)

    def send_down():
        loads[DOWN].wait()
        send_direct(DOWN)

    def project(block, carry):
        pre = mm(first_all[block], wq[...], 1, 0).astype(BF)
        pre_all[block] = pre
        pre = pre.astype(F32)
        joined = jnp.concatenate([prev[...], pre], axis=0)
        prev[...] = pre[-8:]
        out = (
            shift[0:1]
            + taps[0:1] * pre
            + taps[1:2] * pltpu.roll(joined, 1, 0)[8:]
            + taps[2:3] * pltpu.roll(joined, 2, 0)[8:]
        ).astype(BF)
        at = span(block * block_rows, block_rows)
        for head in range(3 * count):
            piece = out[:, head * HD : (head + 1) * HD]
            if head < count:
                piece = (piece.astype(F32) * SCALING).astype(BF)
            heads[head, at, :] = piece
        return carry

    def projections():
        landed(QKV, 2)
        landed(QKV, 3)
        prev[...] = jnp.zeros_like(prev)
        lax.fori_loop(0, blocks, project, 0)
        at = lax.broadcasted_iota(jnp.int32, key_bias.shape, 1)
        key_bias[...] = jnp.where(at < lens[slot], 0.0, MASKED)

    def soft(head, block):
        at = block * block_rows
        query = heads[head, at : at + block_rows, :]
        key = heads[count + head, 0 : at + block_rows, :]
        scores = mm(query, key, 1, 1) + key_bias[0:1, 0 : at + block_rows]
        col = lax.broadcasted_iota(jnp.int32, (block_rows, block_rows), 1)
        row = lax.broadcasted_iota(jnp.int32, (block_rows, 1), 0)
        last = jnp.where(col <= row, scores[:, at:], MASKED)
        scores = jnp.concatenate([scores[:, :at], last], axis=1) if block else last
        powers = jnp.exp(scores - jnp.max(scores, axis=-1, keepdims=True))
        probs = powers * (1.0 / jnp.sum(powers, axis=-1, keepdims=True))
        return query, key, probs

    def att_copy(block):
        return remote(
            att.at[block],
            attn.at[c],
            att_send.at[block],
            att_recv.at[lax.rem(block - c + 4, 4)],
            (f, block, t),
        )

    def attention(block):
        keys = (block + 1) * block_rows

        def attend(head, carry, block=block, keys=keys):
            _, _, probs = soft(head, block)
            out = mm(probs.astype(BF), heads[2 * count + head, 0:keys, :], 1, 0)
            att[block, span(head * HD, HD), :] = out.T.astype(BF)
            return carry

        lax.fori_loop(0, count, attend, 0)

        @pl.when(block != c)
        def _():
            att_copy(block).start()

        @pl.when(block == c)
        def _():
            attn[c] = att[block]

    def mask_grad(s, carry):
        row = c * block_rows + lax.broadcasted_iota(jnp.int32, (block_rows, 1), 0)
        grad_low[s] = jnp.where(row < lens[s], cot[s].astype(F32), 0.0).astype(BF)
        return carry

    def masks():
        loads["cot"].wait()
        lax.fori_loop(0, slots, mask_grad, 0)

    def swap(source, target, kind, s):
        return remote(
            source.at[s], target.at[s], part_send.at[kind, s], part_recv.at[kind, s], partner
        )

    def attn_out(s, carry):
        rows = jnp.concatenate([attn[2 * s], attn[2 * s + 1]], axis=0).T
        low[s] = rows
        part_a[s] = mm(rows, wo[...], 1, 1)
        swap(part_a, part_a_in, 0, s).start()
        return carry

    def out_projection():
        for kind in (2, 3):
            landed(OUT, kind)
        for d in (1, 2, 3):
            arrived(attn.at[lax.rem(c - d + 4, 4)], att_recv.at[d])
        lax.fori_loop(0, slots, attn_out, 0)

    def feed(s, carry):
        swap(part_a, part_a_in, 0, s).wait()
        mid = tok[s].astype(F32) + (part_a[s] + part_a_in[s])
        middle[s] = mid
        low_out = norm_rows(mid, gain2[...], bias2[...])[0].astype(BF)
        second[s] = low_out
        rect = jnp.maximum(mm(low_out, wu[...], 1, 0), 0.0)
        wide_a[s] = rect
        act[s] = (rect * rect).astype(BF)
        return carry

    def feed_forward():
        for kind in (2, 3):
            landed(UP, kind)
        lax.fori_loop(0, slots, feed, 0)

    def weight_grad(target, left, right, part):
        chunks = model // 256
        first = chunks * lax.rem(lax.div(f, 2) + 1 - part, 2)

        def step(j, carry):
            at = lanes_at((first + j) * 128, 128)
            rows = left.shape[0] * left.shape[1]
            lhs = left[:, :, at].reshape(rows, 128)
            rhs = right[...].reshape(rows, right.shape[2])
            target[at, :] = mm(lhs, rhs, 0, 0).astype(BF)
            return carry

        lax.fori_loop(0, chunks, step, 0)

    grads = [g_down, g_up, g_out, g_qkv]
    finals = [down_out, up_out, out_out]
    z_outer = 3 * lax.div(c, 2)
    z_near = jnp.where(c == 0, 1, jnp.where(c == 3, 2, 3 - c))

    def size_of(w):
        return rows_half // CUTS[w]

    def rows_of(w, owner, side, u):
        return span(owner * share + side * rows_half + u * size_of(w), size_of(w))

    def cut(w, u):
        return pl.ds(u * size_of(w), size_of(w))

    def near_copy(w, kind, u):
        owner = (fx, fd, fy, fd)[kind]
        return remote(
            grads[w].at[rows_of(w, owner, kind // 2, u)],
            near[w].at[kind, cut(w, u)],
            near_send[w].at[kind, u],
            near_recv[w].at[kind, u],
            (fx, c, t) if kind < 2 else (fy, c, t),
        )

    def far_copy(w, side, u):
        return remote(
            far_send[w].at[side, cut(w, u)],
            far[w].at[side, cut(w, u)],
            far_ssem[w].at[side, u],
            far_recv[w].at[side, u],
            (fy, c, t) if side == 0 else (fx, c, t),
        )

    def hop_one(w, kinds, u):
        for kind in kinds:
            near_copy(w, kind, u).start()

    def hop_two(w, u):
        for side in (0, 1):
            kind = 1 + 2 * side
            near_copy(w, kind, u).wait_recv()
            owner = fy if side == 0 else fx
            own = grads[w][rows_of(w, owner, side, u), :].astype(F32)
            come = near[w][kind, cut(w, u), :].astype(F32)
            far_send[w][side, cut(w, u), :] = (own + come).astype(BF)
            far_copy(w, side, u).start()

    def own_sum(w, side, u):
        near_copy(w, 2 * side, u).wait_recv()
        far_copy(w, side, u).wait_recv()
        own = grads[w][rows_of(w, f, side, u), :].astype(F32)
        return own + near[w][2 * side, cut(w, u), :] + far[w][side, cut(w, u), :]

    def z_rows(w, side, u):
        return pl.ds(side * rows_half + u * size_of(w), size_of(w))

    def z_copy(w, stage, side, u):
        view = z_rows(w, side, u)
        source = (z_own[w], z_own[w], finals[w])[stage].at[view]
        target = (z_in[w].at[0, view], z_in[w].at[1, view], finals[w].at[view])[stage]
        return remote(
            source, target, z_send[w].at[stage, side, u], z_recv[w].at[stage, side, u],
            (f, (z_near, z_near, z_outer)[stage], t),
        )

    def z_one(w, u):
        for side in (0, 1):
            z_own[w][z_rows(w, side, u), :] = own_sum(w, side, u).astype(BF)

            @pl.when(inner == 0)
            def _():
                z_copy(w, 0, side, u).start()

    def z_two(w, u):
        @pl.when(inner == 1)
        def _():
            for side in (0, 1):
                z_copy(w, 0, side, u).wait_recv()
                at = z_rows(w, side, u)
                z_own[w][at, :] = (z_own[w][at, :].astype(F32) + z_in[w][0, at, :]).astype(BF)
                z_copy(w, 1, side, u).start()

    def z_three(w, u):
        @pl.when(inner == 1)
        def _():
            for side in (0, 1):
                z_copy(w, 1, side, u).wait_recv()
                at = z_rows(w, side, u)
                finals[w][at, :] = (z_own[w][at, :].astype(F32) + z_in[w][1, at, :]).astype(BF)
                z_copy(w, 2, side, u).start()

    def reduced(w):
        for u in range(CUTS[w]):
            for kind in range(4):
                near_copy(w, kind, u).wait_send()
            for side in (0, 1):
                far_copy(w, side, u).wait_send()
                if w == QKV:
                    continue

                @pl.when(inner == 1)
                def _():
                    z_copy(w, 1, side, u).wait_send()
                    z_copy(w, 2, side, u).wait_send()

                @pl.when(inner == 0)
                def _():
                    z_copy(w, 0, side, u).wait_send()
                    z_copy(w, 2, side, u).wait_recv()

    def feed_back(s):
        if s == 0:
            for k in range(3):
                arrived(half_of(k, 1 - half), mate_recv.at[k])
        grad = (mm(grad_low[s], wd[...], 1, 0) * 2.0 * wide_a[s]).astype(BF)
        up_grad[s] = grad
        part_b[s] = mm(grad, wu[...], 1, 1)
        swap(part_b, part_b_in, 1, s).start()

    def flat_copy(s, h):
        return remote(
            flat.at[s, h], flat_in.at[c], flat_send.at[s, h],
            flat_recv.at[lax.rem(2 * s + h - c + 4, 4)], (f, 2 * s + h, t),
        )

    in_half = (
        lax.div(lax.broadcasted_iota(jnp.int32, (block_rows, 1), 0), half_rows) == t
    ).astype(F32)

    def norm_two_back(s):
        if s == 0:
            early[0] = jnp.zeros(early.shape[1:], F32)
        swap(part_b, part_b_in, 1, s).wait()
        grad = part_b[s] + part_b_in[s]
        _, normed, recip = norm_rows(middle[s], gain2[...], bias2[...])
        kept = grad * in_half
        early[0, 0:1, :] += jnp.sum(kept * normed, axis=0, keepdims=True)
        early[0, 1:2, :] += jnp.sum(kept, axis=0, keepdims=True)
        back = grad_low[s].astype(F32) + norm_back(grad, normed, recip, gain2[...])
        middle_grad[s] = back
        back = back.astype(BF)
        middle_low[s] = back
        flat_rows = mm(back, wo[...], 1, 0).T.astype(BF)
        for h in (0, 1):
            flat[s, h] = flat_rows[h * part_width : (h + 1) * part_width]

            @pl.when(2 * s + h != c)
            def _():
                flat_copy(s, h).start()

            @pl.when(2 * s + h == c)
            def _():
                flat_in[c] = flat[s, h]

    def down(s, carry):
        part_a[s] = mm(act[s], wd[...], 1, 1)
        swap(part_a, part_a_in, 2, s).start()
        return carry

    def feed_down():
        lax.fori_loop(0, slots, down, 0)

    def put_result():
        for s in range(slots):
            swap(part_a, part_a_in, 2, s).wait()
            result[s] = (middle[s] + (part_a[s] + part_a_in[s])).astype(BF)

    def fg_view(block, rows):
        return wide_a.at[block // 2, rows, pl.ds(block % 2 * model, model)]

    def own_copy(block):
        return remote(
            fg_view(block, theirs), fg_in.at[block], own_send.at[block], own_recv.at[block],
            partner,
        )

    def pair_copy(block):
        return remote(
            fg_low.at[block], pair_in.at[block], pair_send.at[block], pair_recv.at[block],
            (f, mate, t),
        )

    def fg_copy(block):
        return remote(
            fg_low.at[block], fg_other, fg_ssem.at[block], fg_recv.at[0], (f, block, t)
        )

    def collects(block):
        return inner * (1 - (mate == block)) + (1 - inner) * (c == block) == 1

    def hand_over(block):
        own_copy(block).wait_recv()
        total = fg_view(block, mine)[...] + fg_in[block]
        fg_in[block] = total

        @pl.when(jnp.logical_not(collects(block)))
        def _():
            fg_low[block] = total.astype(BF)
            pair_copy(block).start()

    def collect(block):
        @pl.when(collects(block))
        def _():
            arrived(pair_in.at[block], pair_recv.at[block])
            total = fg_in[block] + pair_in[block]

            @pl.when(block == c)
            def _():
                fg_own[...] = total

            @pl.when(block != c)
            def _():
                fg_low[block] = total.astype(BF)
                fg_copy(block).start()

    def attention_back(block):
        if block == blocks - 1:
            key_acc[...] = jnp.zeros_like(key_acc)
            value_acc[...] = jnp.zeros_like(value_acc)
            later[...] = jnp.zeros_like(later)
            conv_acc[...] = jnp.zeros_like(conv_acc)

        @pl.when(block != c)
        def _():
            arrived(flat_in.at[block], flat_recv.at[lax.rem(c - block + 4, 4)])

        keys = (block + 1) * block_rows

        def attend_back(head, carry, block=block, keys=keys):
            query, key, probs = soft(head, block)
            channels = span(head * HD, HD)
            grad_t = flat_in[block, channels, :]
            prob_grad = mm(grad_t.T, heads[2 * count + head, 0:keys, :], 1, 1)
            delta = jnp.sum(probs * prob_grad, axis=-1, keepdims=True)
            score_grad = (probs * (prob_grad - delta)).astype(BF)
            query_t[channels, :] = (mm(score_grad, key, 1, 0) * SCALING).T
            key_acc[head, :, 0:keys] += mm(query.T, score_grad, 1, 0)
            value_acc[head, :, 0:keys] += mm(grad_t, probs.astype(BF), 1, 0)
            return carry

        lax.fori_loop(0, count, attend_back, 0)
        columns = slice(block * block_rows, (block + 1) * block_rows)
        mixed_low[...] = jnp.concatenate(
            [
                query_t[...],
                key_acc[:, :, columns].reshape(part_width, block_rows),
                value_acc[:, :, columns].reshape(part_width, block_rows),
            ],
            axis=0,
        ).T
        mixed = mixed_low[...]
        joined = jnp.concatenate([mixed, later[...]], axis=0)
        next_one = pltpu.roll(joined, block_rows + 7, 0)[:block_rows]
        next_two = pltpu.roll(joined, block_rows + 6, 0)[:block_rows]
        later[...] = mixed[:8]
        before = pre_all[block].astype(F32)
        for at, moved in enumerate((mixed, next_one, next_two)):
            conv_acc[at : at + 1, :] += jnp.sum(before * moved, axis=0, keepdims=True)
        conv_acc[3:4, :] += jnp.sum(mixed, axis=0, keepdims=True)
        grad = (taps[0:1] * mixed + taps[1:2] * next_one + taps[2:3] * next_two).astype(BF)
        pre_grad[block] = grad
        fg_view(block, pl.ds(0, block_rows))[...] = mm(grad, wq[...], 1, 1)
        own_copy(block).start()

    smalls = [(early, early_xy, early_z), (late, late_xy, late_z)]

    def tp_copy(k):
        return remote(
            smalls[k][0].at[0], smalls[k][0].at[1], sm_send.at[k, 0], sm_recv.at[k, 0], partner
        )

    def xy_copy(k, at):
        view = smalls[k][1].at[f]
        return remote(
            view, view, sm_send.at[k, 1 + at], sm_recv.at[k, 1 + at], ((fx, fy, fd)[at], c, t)
        )

    def z_small(k, d):
        view = smalls[k][2].at[c]
        return remote(
            view, view, sm_send.at[k, 3 + d], sm_recv.at[k, 3 + d], (f, lax.rem(c + d, 4), t)
        )

    def small_tp(k):
        tp_copy(k).wait()
        mixed_rows = 2 if k == 0 else smalls[k][0].shape[1]
        total = smalls[k][0][0] + smalls[k][0][1]
        smalls[k][1][f] = smalls[k][0][0]
        smalls[k][1][f, 0:mixed_rows, :] = total[0:mixed_rows]
        for at in range(3):
            xy_copy(k, at).start()

    def small_xy(k):
        for at, owner in enumerate((fx, fy, fd)):
            xy_copy(k, at).wait_send()
            arrived(smalls[k][1].at[owner], sm_recv.at[k, 1 + at])
        own = smalls[k][1]
        smalls[k][2][c] = own[0] + own[1] + own[2] + own[3]
        for d in (1, 2, 3):
            z_small(k, d).start()

    def small_z(k, out):
        for d in (1, 2, 3):
            z_small(k, d).wait_send()
            arrived(smalls[k][2].at[lax.rem(c - d + 4, 4)], sm_recv.at[k, 3 + d])
        own = smalls[k][2]
        out[...] = own[0] + own[1] + own[2] + own[3]

    def small_start(k):
        if k == 0:
            for h in (0, 1):

                @pl.when(half == h)
                def _():
                    for tap in range(4):
                        for kind in range(3):
                            at = 3 * tap + kind
                            lane = (at % 2 * 2 + h) * part_width
                            channels = slice(kind * part_width, (kind + 1) * part_width)
                            early[0, 2 + at // 2 : 3 + at // 2, lane : lane + part_width] = (
                                conv_acc[tap : tap + 1, channels]
                            )

        tp_copy(k).start()

    def q_copy(stage, side, u):
        view = z_rows(QKV, side, u)
        if stage == 0:
            source, target, device = q_own.at[view], q_in.at[view], lax.rem(c + 2, 4)
        else:
            source = target = q_sum.at[half, view]
            device = c + 1 - 2 * half
        return remote(
            source, target, q_send.at[stage, side, u], q_recv.at[stage, side, u], (f, device, t)
        )

    def q_one(u):
        for side in (0, 1):
            q_own[z_rows(QKV, side, u), :] = own_sum(QKV, side, u).astype(BF)
            q_copy(0, side, u).start()

    def q_two(u):
        for side in (0, 1):
            q_copy(0, side, u).wait()
            at = z_rows(QKV, side, u)
            q_sum[half, at, :] = (q_own[at, :].astype(F32) + q_in[at, :]).astype(BF)
            q_copy(1, side, u).start()

    lane = late.shape[2]

    def norm_one_back(k):
        s = slot if k == 0 else 1 - slot
        if k == 0:
            late[0] = jnp.zeros(late.shape[1:], F32)
            grad = fg_own[...]
        else:
            arrived(fg_other, fg_recv.at[0])
            grad = fg_other[...].astype(F32)
        _, normed, recip = norm_rows(tok[s, mine, :].astype(F32), gain1[...], bias1[...])
        gain_sum = jnp.sum(grad * normed, axis=0, keepdims=True)
        bias_sum = jnp.sum(grad, axis=0, keepdims=True)
        for at in range(model // lane):
            lanes = slice(at * lane, (at + 1) * lane)
            late[0, at : at + 1, :] += gain_sum[:, lanes]
            late[0, 4 + at : 5 + at, :] += bias_sum[:, lanes]
        input_grad[s, mine, :] = middle_grad[s, mine, :] + norm_back(
            grad, normed, recip, gain1[...]
        )
        in_copy(k).start()

    def in_copy(k):
        view = input_grad.at[slot if k == 0 else 1 - slot, mine]
        return remote(view, view, in_send.at[k], in_recv.at[k], partner)

    send_out()
    send_direct(QKV)
    send_down()
    tokens(0)
    tokens(1)
    pass_on(QKV)
    send_up()
    own_norm()
    pass_down()
    tokens(2)
    tokens_passed()
    pass_on(OUT)
    projections()
    attention(3)
    attention(0)
    masks()
    attention(1)
    pass_on(UP)
    attention(2)
    pass_down_last()
    out_projection()
    feed_forward()
    feed_back(0)
    weight_grad(g_down, grad_low, act, 0)
    hop_one(DOWN, (1, 3), 0)
    hop_one(DOWN, (1, 3), 2)
    feed_back(1)
    norm_two_back(0)
    weight_grad(g_down, grad_low, act, 1)
    hop_one(DOWN, (1, 3), 1)
    norm_two_back(1)
    hop_one(DOWN, (0, 2), 0)
    hop_two(DOWN, 0)
    hop_two(DOWN, 2)
    weight_grad(g_up, second, up_grad, 0)
    for part in (0, 1):
        weight_grad(g_out, middle_low, low, part)
    hop_one(DOWN, (0, 2), 2)
    hop_two(DOWN, 1)
    hop_one(DOWN, (0, 2), 1)
    hop_one(OUT, (1, 3), 0)
    attention_back(3)
    z_one(DOWN, 0)
    attention_back(2)
    z_one(DOWN, 2)
    hop_one(UP, (1, 3), 1)
    attention_back(1)
    z_one(DOWN, 1)
    hop_one(UP, (1, 3), 0)
    hop_one(OUT, (0, 2), 0)
    z_two(DOWN, 0)
    attention_back(0)
    hand_over(2)
    hand_over(3)
    weight_grad(g_qkv, first_all, pre_grad, 0)
    hand_over(0)
    z_two(DOWN, 1)
    hop_one(QKV, (1, 3), 1)
    weight_grad(g_up, second, up_grad, 1)
    z_three(DOWN, 0)
    z_two(DOWN, 2)
    hop_one(UP, (1, 3), 2)
    feed_down()
    hop_two(OUT, 0)
    hop_one(UP, (0, 2), 1)
    hand_over(1)
    hop_one(QKV, (1, 3), 0)
    weight_grad(g_qkv, first_all, pre_grad, 1)
    collect(0)
    small_start(0)
    collect(3)
    collect(2)
    hop_one(QKV, (0, 2), 1)
    hop_two(UP, 0)
    small_tp(0)
    z_one(OUT, 0)
    collect(1)
    hop_two(QKV, 1)
    hop_two(UP, 1)
    hop_two(UP, 2)
    z_three(DOWN, 1)
    z_three(DOWN, 2)
    norm_one_back(0)
    hop_one(QKV, (0, 2), 0)
    q_one(1)
    norm_one_back(1)
    small_xy(0)
    hop_one(UP, (0, 2), 0)
    hop_one(UP, (0, 2), 2)
    z_one(UP, 1)
    z_one(UP, 0)
    z_two(UP, 1)
    q_two(1)
    z_two(UP, 0)
    small_z(0, early_out)
    z_three(UP, 1)
    z_two(OUT, 0)
    hop_two(QKV, 0)
    z_three(UP, 0)
    small_start(1)
    q_one(0)
    small_tp(1)
    z_three(OUT, 0)
    small_xy(1)
    z_one(UP, 2)
    q_two(0)
    z_two(UP, 2)
    put_result()
    small_z(1, late_out)
    z_three(UP, 2)
    for w in range(4):
        reduced(w)
        for kind in (0, 1):
            direct(w, kind).wait_send()
        for kind in (2, 3):
            relay(w, kind).wait_send()
    for side in (0, 1):
        for u in range(CUTS[QKV]):
            q_copy(1, side, u).wait_send()
            arrived(q_sum.at[1 - half, z_rows(QKV, side, u)], q_recv.at[1, side, u])
    for k in range(3):
        mate_copy(k).wait_send()
        tok_pass(k).wait_send()
        if k < 2:
            tok_copy(k).wait_send()

            @pl.when(inner == 1)
            def _():
                tok_relay(k).wait_send()

    for s in range(slots):
        in_copy(s).wait_send()
        view = input_grad.at[slot if s == 0 else 1 - slot, theirs]
        arrived(view, in_recv.at[s])
        for h in (0, 1):

            @pl.when(2 * s + h != c)
            def _():
                flat_copy(s, h).wait_send()

    for block in range(blocks):
        own_copy(block).wait_send()

        @pl.when(block != c)
        def _():
            att_copy(block).wait_send()

        @pl.when(jnp.logical_not(collects(block)))
        def _():
            pair_copy(block).wait_send()

        @pl.when(collects(block))
        def _():
            @pl.when(block != c)
            def _():
                fg_copy(block).wait_send()


def layer_call(
    lens, tok, cot, wq3, wo, wu, wd, gain1, bias1, gain2, bias2, taps3, shift3
):
    slots, block_rows, model = tok.shape
    share, units, channels = wu.shape[0], wu.shape[1], wo.shape[1]
    part = channels // 2
    width = 3 * part
    blocks = 4
    tall = (slots, block_rows, model)
    wide = (slots, block_rows, units)
    half = block_rows // 2
    columns = [units, units, channels, width]
    dma = pltpu.SemaphoreType.DMA

    def vmem(shape, kind=BF):
        return pltpu.VMEM(tuple(shape), kind)

    def struct(shape, kind=BF):
        return jax.ShapeDtypeStruct(tuple(shape), kind)

    return pl.pallas_call(
        layer_kernel,
        name="layer",
        out_shape=[
            struct(tall), struct(tall, F32), struct((share, units)), struct((share, units)),
            struct((share, channels)), struct((2, share, width)), struct((8, model), F32),
            struct((8, 256), F32),
        ],
        in_specs=[SMEM] + [ANY] * 6 + [VMEM] * 6,
        out_specs=[VMEM] * 8,
        scratch_shapes=[
            vmem(tall), vmem(tall), vmem(wq3.shape), vmem((model, width)),
            vmem((model, channels)), vmem((model, units)), vmem((model, units)),
            vmem((8, width), F32), vmem((8, width), F32), vmem((8, width), F32),
            vmem((blocks, block_rows, model)), vmem((blocks, block_rows, width)),
            vmem((width // HD, blocks * block_rows, HD)),
            vmem((blocks, part, block_rows)), vmem((blocks, part, block_rows)),
            vmem((slots, block_rows, channels)), vmem(tall, F32), vmem(tall, F32),
            vmem(tall, F32), vmem(tall, F32), vmem(wide, F32), vmem(tall, F32), vmem(tall, F32),
            vmem(tall), vmem(tall), vmem(wide), vmem(wide), vmem(tall),
            vmem((slots, 2, part, block_rows)), vmem((4, part, block_rows)),
            vmem((model, units)), vmem((model, units)), vmem((model, channels)),
            vmem((model, width)),
            [vmem((4, share // 2, n)) for n in columns],
            [vmem((2, share // 2, n)) for n in columns],
            [vmem((2, share // 2, n)) for n in columns],
            [vmem((share, n)) for n in columns[:3]],
            [vmem((2, share, n)) for n in columns[:3]],
            vmem((share, width)), vmem((share, width)),
            vmem((8, blocks * block_rows), F32),
            vmem((part // HD, HD, blocks * block_rows), F32),
            vmem((part // HD, HD, blocks * block_rows), F32),
            vmem((part, block_rows), F32), vmem((8, width), F32),
            vmem((block_rows, width), F32), vmem((blocks, block_rows, width)),
            vmem((8, width), F32),
            vmem((blocks, half, model), F32), vmem((blocks, half, model)),
            vmem((blocks, half, model)), vmem((half, model), F32), vmem((half, model)),
            vmem((2, 8, model), F32), vmem((4, 8, model), F32), vmem((4, 8, model), F32),
            vmem((2, 8, 256), F32), vmem((4, 8, 256), F32), vmem((4, 8, 256), F32),
            dma((6,)), dma((4,)), dma((4,)), dma((4,)), dma((4,)), dma((3,)), dma((3,)),
            dma((4, 4)), dma((4, 4)),
            dma((4,)), dma((4,)),
            dma((3, slots)), dma((3, slots)), dma((slots, 2)), dma((4,)),
            [dma((4, n)) for n in CUTS], [dma((4, n)) for n in CUTS],
            [dma((2, n)) for n in CUTS], [dma((2, n)) for n in CUTS],
            [dma((3, 2, n)) for n in CUTS[:3]], [dma((3, 2, n)) for n in CUTS[:3]],
            dma((2, 2, CUTS[QKV])), dma((2, 2, CUTS[QKV])),
            dma((4,)), dma((1,)), dma((4,)), dma((4,)), dma((4,)), dma((4,)), dma((slots,)),
            dma((slots,)),
            dma((2, 7)), dma((2, 7)),
        ],
        compiler_params=pltpu.CompilerParams(
            collective_id=0, has_side_effects=True, vmem_limit_bytes=67043328
        ),
    )(lens, tok, cot, wq3, wo, wu, wd, gain1, bias1, gain2, bias2, taps3, shift3)


def finish_kernel(
    result_in, grad_in, down_in, up_in, out_in, qkv_in, early, late,
    result, grad, gain1, bias1, qkv, taps, shift, out, gain2, bias2, up, down,
):
    result[...] = result_in[...]
    grad[...] = grad_in[...]
    down[...] = down_in[...].astype(F32)
    up[...] = up_in[...].astype(F32)
    out[...] = out_in[...].astype(F32)
    part = qkv_in.shape[2] // 3
    for kind in range(3):
        for h in (0, 1):
            qkv[kind, :, h * part : (h + 1) * part] = qkv_in[
                h, :, kind * part : (kind + 1) * part
            ].astype(F32)
    lane = late.shape[1]
    for at in range(gain1.shape[0] // lane):
        lanes = slice(at * lane, (at + 1) * lane)
        gain1[lanes] = late[at]
        bias1[lanes] = late[4 + at]
    gain2[...] = early[0]
    bias2[...] = early[1]
    for at in range(12):
        lane = at % 2 * 2 * part
        values = early[2 + at // 2 : 3 + at // 2, lane : lane + 2 * part]
        tap, kind = at // 3, at % 3
        if tap < 3:
            taps[tap, kind : kind + 1, :] = values
        else:
            shift[kind : kind + 1, :] = values


def finish_call(result, grad, down, up, out, qkv, early, late):
    channels, share, model = out.shape[1], out.shape[0], result.shape[2]

    def struct(shape, kind=F32):
        return jax.ShapeDtypeStruct(tuple(shape), kind)

    vector = struct((model,))
    steps = 4
    rows = share // steps
    cut = result.shape[1] * result.shape[0] // steps

    def tall(index):
        return index // 2, index % 2, 0

    def whole(shape):
        return pl.BlockSpec(shape, lambda index: (0,) * len(shape))

    def block(width):
        return pl.BlockSpec((rows, width), lambda index: (index, 0))

    def triple(count, width):
        return pl.BlockSpec((count, rows, width), lambda index: (0, index, 0))

    tall_spec = pl.BlockSpec((1, cut, model), tall)
    vector_spec = whole((model,))
    units = up.shape[1]
    return pl.pallas_call(
        finish_kernel,
        grid=(steps,),
        in_specs=[
            tall_spec, tall_spec, block(units), block(units), block(channels),
            triple(2, qkv.shape[2]), whole(early.shape), whole(late.shape),
        ],
        out_specs=[
            tall_spec, tall_spec, vector_spec, vector_spec, triple(3, channels),
            whole((3, 3, channels)), whole((3, channels)), block(channels), vector_spec,
            vector_spec, block(units), block(units),
        ],
        name="finish",
        out_shape=[
            struct(result.shape, BF), struct(grad.shape), vector, vector,
            struct((3, share, channels)), struct((3, 3, channels)), struct((3, channels)),
            struct(out.shape), vector, vector, struct(up.shape), struct(down.shape),
        ],
    )(result, grad, down, up, out, qkv, early, late)


def local(
    tokens,
    lengths,
    cotangent,
    ln1_gain,
    ln1_bias,
    qkv_weight,
    conv_kernel,
    conv_bias,
    out_weight,
    ln2_gain,
    ln2_bias,
    up_weight,
    down_weight,
):
    batches, block_rows, model_width = tokens.shape
    all_rows = batches * block_rows
    qkv_full, out_full, up_full_w, down_full_w = (
        lax.all_gather(qkv_weight, "fsdp", axis=0, tiled=True),
        lax.all_gather(out_weight, "fsdp", axis=1, tiled=True),
        lax.all_gather(up_weight, "fsdp", axis=0, tiled=True),
        lax.all_gather(down_weight, "fsdp", axis=1, tiled=True),
    )
    local_width = qkv_full.shape[2]
    local_heads = local_width // HD
    ctx_count = lax.axis_size("ctx")
    slot_span = block_rows * ctx_count
    group_blocks = 4
    key_span = block_rows * group_blocks
    ctx_index = lax.axis_index("ctx")
    positions = ctx_index * block_rows + jnp.arange(block_rows, dtype=jnp.int32)
    span_iota = jnp.arange(key_span, dtype=jnp.int32)
    block_count = (ctx_index * block_rows + block_rows + key_span - 1) // key_span
    token_valid = positions[None, :] < lengths[:, None]

    def span_slice(array_data, block, axis_pos):
        return lax.dynamic_slice_in_dim(array_data, block * key_span, key_span, axis_pos)

    inputs = tokens.astype(jnp.float32).reshape(all_rows, model_width)
    first_out, first_hat, first_recip = layer_norm(inputs, ln1_gain, ln1_bias)
    first_low = first_out.astype(jnp.bfloat16)
    pre_low = jnp.einsum(
        "td,dcn->tcn", first_low, qkv_full, preferred_element_type=jnp.float32
    ).astype(jnp.bfloat16)
    pre_low = pre_low.reshape(batches, block_rows, 3, local_width)
    earlier = shifted(pre_low[:, block_rows - 2 :], "ctx", 1)
    extended = jnp.concatenate([earlier, pre_low], axis=1).astype(jnp.float32)
    conv_out = (
        conv_bias
        + conv_kernel[0] * extended[:, 2:]
        + conv_kernel[1] * extended[:, 1:-1]
        + conv_kernel[2] * extended[:, :-2]
    ).astype(jnp.bfloat16)
    query_heads = conv_out[:, :, 0].reshape(batches, block_rows, local_heads, HD)
    own_pairs = conv_out[:, :, 1:]
    whole_pairs = lax.all_gather(own_pairs, "ctx", axis=1, tiled=True)
    key_heads = whole_pairs[:, :, 0].reshape(batches, slot_span, local_heads, HD)
    value_heads = whole_pairs[:, :, 1].reshape(batches, slot_span, local_heads, HD)

    def stat_step(block, carry):
        row_max, total = carry
        key_pos = block * key_span + span_iota
        scores = tile_scores(
            query_heads, span_slice(key_heads, block, 1), positions, key_pos, lengths
        )
        new_max = jnp.maximum(row_max, jnp.max(scores, axis=-1, keepdims=True))
        total = total * jnp.exp(row_max - new_max) + jnp.sum(
            jnp.exp(scores - new_max), axis=-1, keepdims=True
        )
        return (new_max, total)

    stat_shape = (batches, local_heads, block_rows, 1)
    row_max, total = lax.fori_loop(
        0,
        block_count,
        stat_step,
        (jnp.full(stat_shape, MASKED, jnp.float32), jnp.zeros(stat_shape, jnp.float32)),
    )
    log_total = row_max + jnp.log(total)

    def value_step(block, accum):
        key_pos = block * key_span + span_iota
        scores = tile_scores(
            query_heads, span_slice(key_heads, block, 1), positions, key_pos, lengths
        )
        probs_low = jnp.exp(scores - log_total).astype(jnp.bfloat16)
        return accum + jnp.einsum(
            "mhqk,mkhd->mqhd",
            probs_low,
            span_slice(value_heads, block, 1),
            preferred_element_type=jnp.float32,
        )

    attn_acc = lax.fori_loop(
        0, block_count, value_step, jnp.zeros((batches, block_rows, local_heads, HD), jnp.float32)
    )
    attn_low = attn_acc.reshape(all_rows, local_width).astype(jnp.bfloat16)
    attn_out = lax.psum(jnp.dot(attn_low, out_full, preferred_element_type=jnp.float32), "tp")
    middle = inputs + attn_out
    second_out, second_hat, second_recip = layer_norm(middle, ln2_gain, ln2_bias)
    second_low = second_out.astype(jnp.bfloat16)
    up_full = jnp.dot(second_low, up_full_w, preferred_element_type=jnp.float32)
    rectified = jnp.maximum(up_full, 0.0)
    act_low = (rectified * rectified).astype(jnp.bfloat16)
    ffn_out = lax.psum(jnp.dot(act_low, down_full_w, preferred_element_type=jnp.float32), "tp")
    result = (middle + ffn_out).reshape(batches, block_rows, model_width).astype(jnp.bfloat16)
    grad_out = (
        cotangent.astype(jnp.float32) * token_valid[:, :, None].astype(jnp.float32)
    ).reshape(all_rows, model_width)
    grad_low = grad_out.astype(jnp.bfloat16)
    down_wgrad = jnp.einsum("tf,td->fd", act_low, grad_low, preferred_element_type=jnp.float32)
    act_grad = jnp.einsum("td,fd->tf", grad_low, down_full_w, preferred_element_type=jnp.float32)
    up_grad_low = (act_grad * 2.0 * rectified).astype(jnp.bfloat16)
    up_wgrad = jnp.einsum("td,tf->df", second_low, up_grad_low, preferred_element_type=jnp.float32)
    second_grad = lax.psum(
        jnp.einsum("tf,df->td", up_grad_low, up_full_w, preferred_element_type=jnp.float32), "tp"
    )
    gain_two_grad = jnp.sum(second_grad * second_hat, axis=0)
    bias_two_grad = jnp.sum(second_grad, axis=0)
    middle_grad = grad_out + norm_back(second_grad, second_hat, second_recip, ln2_gain)
    middle_low = middle_grad.astype(jnp.bfloat16)
    out_wgrad = jnp.einsum("tn,td->nd", attn_low, middle_low, preferred_element_type=jnp.float32)
    attn_flat = jnp.einsum(
        "td,nd->tn", middle_low, out_full, preferred_element_type=jnp.float32
    ).astype(jnp.bfloat16)
    attn_grad = attn_flat.reshape(batches, block_rows, local_heads, HD)

    def delta_step(block, accum):
        key_pos = block * key_span + span_iota
        probs_full = jnp.exp(
            tile_scores(query_heads, span_slice(key_heads, block, 1), positions, key_pos, lengths)
            - log_total
        )
        prob_grad = jnp.einsum(
            "mqhd,mkhd->mhqk",
            attn_grad,
            span_slice(value_heads, block, 1),
            preferred_element_type=jnp.float32,
        )
        return accum + jnp.sum(probs_full * prob_grad, axis=-1, keepdims=True)

    delta = lax.fori_loop(0, block_count, delta_step, jnp.zeros(stat_shape, jnp.float32))
    query_zero = jnp.zeros((batches, block_rows, local_heads, HD), jnp.float32)

    def back_step(block, carry):
        accum, buffer = carry
        key_pos = block * key_span + span_iota
        key_part = span_slice(key_heads, block, 1)
        probs_full, prob_grad, score_grad = tile_grads(
            query_heads,
            key_part,
            span_slice(value_heads, block, 1),
            attn_grad,
            log_total,
            delta,
            positions,
            key_pos,
            lengths,
        )
        probs_again = probs_full.astype(jnp.bfloat16)
        accum = (
            accum
            + jnp.einsum(
                "mhqk,mkhd->mqhd", score_grad, key_part, preferred_element_type=jnp.float32
            )
            * SCALING
        )
        key_term = (
            jnp.einsum(
                "mhqk,mqhd->mkhd", score_grad, query_heads, preferred_element_type=jnp.float32
            )
            * SCALING
        )
        value_term = jnp.einsum(
            "mhqk,mqhd->mkhd", probs_again, attn_grad, preferred_element_type=jnp.float32
        )
        stacked = jnp.stack(
            [
                key_term.reshape(batches, key_span, local_width),
                value_term.reshape(batches, key_span, local_width),
            ],
            axis=2,
        )
        buffer = lax.dynamic_update_slice_in_dim(buffer, stacked, block * key_span, 1)
        return (accum, buffer)

    buffer_zero = jnp.zeros((batches, slot_span, 2, local_width), jnp.float32)
    query_grad, pair_terms = lax.fori_loop(0, block_count, back_step, (query_zero, buffer_zero))
    pair_grad = lax.psum_scatter(pair_terms, "ctx", scatter_dimension=1, tiled=True)
    mixed_grad = jnp.concatenate(
        [query_grad.reshape(batches, block_rows, 1, local_width), pair_grad], axis=2
    )
    later = shifted(mixed_grad[:, :2], "ctx", -1)
    ahead = jnp.concatenate([mixed_grad, later], axis=1)
    pre_grad = (
        conv_kernel[0] * ahead[:, :block_rows]
        + conv_kernel[1] * ahead[:, 1 : block_rows + 1]
        + conv_kernel[2] * ahead[:, 2:]
    ).astype(jnp.bfloat16)
    kernel_grad = jnp.stack(
        [
            jnp.sum(extended[:, 2 - offset : 2 - offset + block_rows] * mixed_grad, axis=(0, 1))
            for offset in range(3)
        ]
    )
    shift_grad = jnp.sum(mixed_grad, axis=(0, 1))
    pre_grad = pre_grad.reshape(all_rows, 3, local_width)
    qkv_wgrad = jnp.einsum("td,tcn->dcn", first_low, pre_grad, preferred_element_type=jnp.float32)
    first_grad = lax.psum(
        jnp.einsum("tcn,dcn->td", pre_grad, qkv_full, preferred_element_type=jnp.float32), "tp"
    )
    gain_one_grad = jnp.sum(first_grad * first_hat, axis=0)
    bias_one_grad = jnp.sum(first_grad, axis=0)
    input_grad = middle_grad + norm_back(first_grad, first_hat, first_recip, ln1_gain)
    input_grad = input_grad.reshape(batches, block_rows, model_width)
    summed = lax.psum(
        (
            qkv_wgrad,
            out_wgrad,
            up_wgrad,
            down_wgrad,
            gain_one_grad,
            bias_one_grad,
            kernel_grad,
            shift_grad,
            gain_two_grad,
            bias_two_grad,
        ),
        ("fsdp", "ctx"),
    )
    share_rows = model_width // lax.axis_size("fsdp")
    owner_start = lax.axis_index("fsdp") * share_rows
    qkv_share = lax.dynamic_slice_in_dim(summed[0], owner_start, share_rows, 0)
    out_share = lax.dynamic_slice_in_dim(summed[1], owner_start, share_rows, 1)
    up_share = lax.dynamic_slice_in_dim(summed[2], owner_start, share_rows, 0)
    down_share = lax.dynamic_slice_in_dim(summed[3], owner_start, share_rows, 1)
    small_sums = summed[4:]
    return (
        result,
        input_grad,
        small_sums[0],
        small_sums[1],
        qkv_share,
        small_sums[2],
        small_sums[3],
        out_share,
        small_sums[4],
        small_sums[5],
        up_share,
        down_share,
    )


def local_fast(
    tokens,
    lengths,
    cotangent,
    ln1_gain,
    ln1_bias,
    qkv_weight,
    conv_kernel,
    conv_bias,
    out_weight,
    ln2_gain,
    ln2_bias,
    up_weight,
    down_weight,
):
    parts = layer_call(
        lengths, tokens, cotangent, qkv_weight.transpose(1, 0, 2), out_weight.T, up_weight,
        down_weight.T, ln1_gain, ln1_bias, ln2_gain, ln2_bias, conv_kernel, conv_bias,
    )
    result, grad, gain1, bias1, qkv, taps, shift, out, gain2, bias2, up, down = finish_call(*parts)
    return (
        result, grad, gain1, bias1, qkv.transpose(1, 0, 2), taps, shift, out.T, gain2, bias2, up,
        down.T,
    )


def solution(mesh):
    placed = (
        P("fsdp", "ctx", None),
        P("fsdp"),
        P("fsdp", "ctx", None),
        P(),
        P(),
        P("fsdp", None, "tp"),
        P(None, None, "tp"),
        P(None, "tp"),
        P("tp", "fsdp"),
        P(),
        P(),
        P("fsdp", "tp"),
        P("tp", "fsdp"),
    )
    ctx, fsdp, tp = mesh.shape["ctx"], mesh.shape["fsdp"], mesh.shape["tp"]
    return jax.shard_map(
        local_fast if (fsdp, ctx, tp) == (4, 4, 2) else local,
        mesh=mesh,
        in_specs=placed,
        out_specs=(
            P("fsdp", "ctx", None),
            P("fsdp", "ctx", None),
            P(),
            P(),
            P("fsdp", None, "tp"),
            P(None, None, "tp"),
            P(None, "tp"),
            P("tp", "fsdp"),
            P(),
            P(),
            P("fsdp", "tp"),
            P("tp", "fsdp"),
        ),
        check_vma=False,
    )
```

```python
import jax
import jax.numpy as jnp
from jax import lax
from jax.experimental import pallas as pl
from jax.experimental.pallas import tpu as pltpu
from jax.sharding import PartitionSpec as P

HD = 64


EPSILON = 1e-05
SCALING = 0.125
MASKED = -1e30


def shifted(block, axis, distance):
    devices = range(lax.axis_size(axis))
    route = [(i - distance, i) for i in devices if i - distance in devices]
    return lax.ppermute(block, axis, route)


def layer_norm(row_data, norm_gain, shift_bias):
    centred = row_data - jnp.mean(row_data, axis=-1, keepdims=True)
    recip = lax.rsqrt(jnp.mean(centred * centred, axis=-1, keepdims=True) + EPSILON)
    normed = centred * recip
    return (normed * norm_gain + shift_bias, normed, recip)


def norm_back(grad_in, normed, recip, norm_gain):
    scaled = grad_in * norm_gain
    return recip * (
        scaled
        - jnp.mean(scaled, axis=-1, keepdims=True)
        - normed * jnp.mean(scaled * normed, axis=-1, keepdims=True)
    )


def tile_scores(query_part, key_part, query_pos, key_pos, lengths):
    scores = (
        jnp.einsum("mqhd,mkhd->mhqk", query_part, key_part, preferred_element_type=jnp.float32)
        * SCALING
    )
    allowed = (key_pos[None, None, :] <= query_pos[None, :, None]) & (
        key_pos[None, None, :] < lengths[:, None, None]
    )
    return jnp.where(allowed[:, None], scores, MASKED)


def tile_grads(
    query_part, key_part, value_part, grad_part, log_part, delta_part, query_pos, key_pos, lengths
):
    probs_full = jnp.exp(tile_scores(query_part, key_part, query_pos, key_pos, lengths) - log_part)
    prob_grad = jnp.einsum(
        "mqhd,mkhd->mhqk", grad_part, value_part, preferred_element_type=jnp.float32
    )
    score_grad = (probs_full * (prob_grad - delta_part)).astype(jnp.bfloat16)
    return (probs_full, prob_grad, score_grad)


def norm_rows(x, gain, bias):
    centred = x - jnp.mean(x, axis=-1, keepdims=True)
    recip = lax.rsqrt(jnp.mean(centred * centred, axis=-1, keepdims=True) + EPSILON)
    normed = centred * recip
    return normed * gain + bias, normed, recip


BF = jnp.bfloat16
F32 = jnp.float32
MESH = pl.DeviceIdType.MESH
ANY = pl.BlockSpec(memory_space=pl.ANY)
VMEM = pl.BlockSpec(memory_space=pltpu.VMEM)
SMEM = pl.BlockSpec(memory_space=pltpu.SMEM)
CUTS = (3, 3, 1, 2)
DOWN, UP, OUT, QKV = range(4)


def mm(left, right, left_dim, right_dim):
    return lax.dot_general(
        left, right, (((left_dim,), (right_dim,)), ((), ())), preferred_element_type=F32
    )


def remote(source, target, send_sem, recv_sem, device):
    return pltpu.make_async_remote_copy(
        src_ref=source,
        dst_ref=target,
        send_sem=send_sem,
        recv_sem=recv_sem,
        device_id=device,
        device_id_type=MESH,
    )


def span(start, size):
    return pl.ds(pl.multiple_of(start, 16), size)


def lanes_at(start, size):
    return pl.ds(pl.multiple_of(start, 128), size)


def layer_kernel(
    lens, tok_in, cot_in, wq_in, wo_in, wu_in, wd_in,
    gain1, bias1, gain2, bias2, taps3, shift3,
    result, input_grad, down_out, up_out, out_out, q_sum, early_out, late_out,
    tok, cot, wq_buf, wq, wo, wu, wd, taps, shift, prev,
    first_all, pre_all, heads, att, attn,
    low, part_a, part_a_in, part_b, part_b_in, wide_a, middle, middle_grad,
    second, grad_low, act, up_grad, middle_low, flat, flat_in,
    g_down, g_up, g_out, g_qkv, near, far_send, far, z_own, z_in, q_own, q_in,
    key_bias, key_acc, value_acc, query_t, later, mixed_low, pre_grad, conv_acc,
    fg_in, fg_low, pair_in, fg_own, fg_other, early, early_xy, early_z, late, late_xy, late_z,
    load_sem, tok_send, tok_recv, pass_send, pass_recv, mate_send, mate_recv, w_send, w_recv, att_send, att_recv,
    part_send, part_recv, flat_send, flat_recv,
    near_send, near_recv, far_ssem, far_recv, z_send, z_recv, q_send, q_recv,
    fg_ssem, fg_recv, pair_send, pair_recv, own_send, own_recv, in_send, in_recv, sm_send, sm_recv,
):
    f, c, t = lax.axis_index("fsdp"), lax.axis_index("ctx"), lax.axis_index("tp")
    fx = f + 1 - 2 * lax.rem(f, 2)
    fy = lax.rem(f + 2, 4)
    fd = lax.rem(fx + 2, 4)
    slot = lax.div(c, 2)
    half = lax.rem(c, 2)
    other = 1 - t
    partner = (f, c, other)
    barrier = pltpu.get_barrier_semaphore()
    peers = [(fx, c, t), (fy, c, t), (fd, c, t), partner]
    peers += [(f, lax.rem(c + d, 4), t) for d in (1, 2, 3)]
    for peer in peers:
        pl.semaphore_signal(barrier, inc=1, device_id=peer, device_id_type=MESH)

    slots, block_rows, model = tok.shape
    width = wq.shape[1]
    part_width = width // 3
    count = part_width // HD
    blocks = 4
    half_rows = block_rows // 2
    share = model // 4
    rows_half = share // 2
    mine = span(t * half_rows, half_rows)
    theirs = span(other * half_rows, half_rows)

    def arrived(view, sem):
        remote(view, view, tok_send.at[0], sem, partner).wait_recv()

    wholes = [wd, wu, wo, wq]
    shard_rows = span(f * share, share)
    loads = {}
    for at, (name, source, target) in enumerate(
        [
            ("wq", wq_in, wq_buf),
            ("tok", tok_in, tok),
            (OUT, wo_in, wo.at[shard_rows]),
            (UP, wu_in, wu.at[shard_rows]),
            (DOWN, wd_in, wd.at[shard_rows]),
            ("cot", cot_in, cot),
        ]
    ):
        loads[name] = pltpu.make_async_copy(source, target, load_sem.at[at])
        loads[name].start()
    pl.semaphore_wait(barrier, len(peers))

    inner = lax.rem(lax.div(c + 1, 2), 2)
    mate = c + 1 - 2 * half
    across = 2 - slot
    far_side = 3 - 3 * slot

    def tok_copy(k):
        return remote(
            tok_in.at[slot if k == 0 else 1 - slot, mine],
            first_all.at[c, mine],
            tok_send.at[k],
            tok_recv.at[c],
            (f, mate if k == 0 else across, t),
        )

    def tok_order(k):
        near_in, near_out = ((across, mate), (far_side, across), (mate, far_side))[k]
        return inner * near_in + (1 - inner) * near_out

    def tok_relay(k):
        view = first_all.at[tok_order(k), mine]
        return remote(
            view, view, tok_send.at[2 + k], tok_recv.at[tok_order(k)], (f, mate, t)
        )

    def tok_pass(k):
        view = first_all.at[tok_order(k), mine]
        return remote(view, view, pass_send.at[k], pass_recv.at[k], partner)

    for k in (0, 1):
        tok_copy(k).start()


    def shard_part(w, owner, kind):
        start, size = owner * share, share
        if w == DOWN:
            start, size = start + half * rows_half, rows_half
        if kind < 2:
            return span(start, size)
        return span(start + (kind - 2) * (size // 2), size // 2)

    def direct(w, kind):
        view = wholes[w].at[shard_part(w, f, 0)]
        target = (fx, c, t) if kind == 0 else (fy, c, t)
        return remote(view, view, w_send.at[w, kind], w_recv.at[w, kind], target)

    def relay(w, kind):
        origin, target = (fx, (fy, c, t)) if kind == 2 else (fy, (fx, c, t))
        view = wholes[w].at[shard_part(w, origin, kind)]
        return remote(view, view, w_send.at[w, kind], w_recv.at[w, kind], target)

    def landed(w, kind):
        owner = (fx, fy, fd, fd)[kind]
        arrived(wholes[w].at[shard_part(w, owner, kind)], w_recv.at[w, kind])

    def send_direct(w):
        direct(w, 0).start()
        direct(w, 1).start()

    def pass_on(w):
        landed(w, 0)
        relay(w, 2).start()
        landed(w, 1)
        relay(w, 3).start()

    def half_of(k, side):
        return wd.at[span((fx, fy, fd)[k] * share + side * rows_half, rows_half)]

    def mate_copy(k):
        view = half_of(k, half)
        return remote(view, view, mate_send.at[k], mate_recv.at[k], (f, mate, t))

    def pass_down():
        for k in (0, 1):
            landed(DOWN, k)
            relay(DOWN, 2 + k).start()
            mate_copy(k).start()

    def pass_down_last():
        landed(DOWN, 2)
        landed(DOWN, 3)
        mate_copy(2).start()

    loads["wq"].wait()
    for h in (0, 1):

        @pl.when(half == h)
        def _():
            lanes = slice(h * part_width, (h + 1) * part_width)
            for kind in range(3):
                target = slice(kind * part_width, (kind + 1) * part_width)
                wq[shard_rows, target] = wq_buf[kind, :, lanes]
                shift[0:1, target] = shift3[kind : kind + 1, lanes]
                for tap in range(3):
                    taps[tap : tap + 1, target] = taps3[tap, kind : kind + 1, lanes]

    def first_norm(x):
        return norm_rows(x.astype(F32), gain1[...], bias1[...])[0].astype(BF)

    def own_norm():
        loads["tok"].wait()
        first_all[c] = first_norm(tok[slot])

    def tokens(k):
        source = tok_order(k)
        arrived(first_all.at[source, mine], tok_recv.at[source])

        @pl.when((inner == 1) | (k == 0))
        def _():
            first_all[source, mine, :] = first_norm(first_all[source, mine, :])

        if k < 2:

            @pl.when(inner == 1)
            def _():
                tok_relay(k).start()

        tok_pass(k).start()

    def tokens_passed():
        for k in range(3):
            arrived(first_all.at[tok_order(k), theirs], pass_recv.at[k])

    def send_out():
        loads[OUT].wait()
        send_direct(OUT)

    def send_up():
        loads[UP].wait()
        send_direct(UP)

    def send_down():
        loads[DOWN].wait()
        send_direct(DOWN)

    def project(block, carry):
        pre = mm(first_all[block], wq[...], 1, 0).astype(BF)
        pre_all[block] = pre
        pre = pre.astype(F32)
        joined = jnp.concatenate([prev[...], pre], axis=0)
        prev[...] = pre[-8:]
        out = (
            shift[0:1]
            + taps[0:1] * pre
            + taps[1:2] * pltpu.roll(joined, 1, 0)[8:]
            + taps[2:3] * pltpu.roll(joined, 2, 0)[8:]
        ).astype(BF)
        at = span(block * block_rows, block_rows)
        for head in range(3 * count):
            piece = out[:, head * HD : (head + 1) * HD]
            if head < count:
                piece = (piece.astype(F32) * SCALING).astype(BF)
            heads[head, at, :] = piece
        return carry

    def projections():
        landed(QKV, 2)
        landed(QKV, 3)
        prev[...] = jnp.zeros_like(prev)
        lax.fori_loop(0, blocks, project, 0)
        at = lax.broadcasted_iota(jnp.int32, key_bias.shape, 1)
        key_bias[...] = jnp.where(at < lens[slot], 0.0, MASKED)

    def soft(head, block):
        at = block * block_rows
        query = heads[head, at : at + block_rows, :]
        key = heads[count + head, 0 : at + block_rows, :]
        scores = mm(query, key, 1, 1) + key_bias[0:1, 0 : at + block_rows]
        col = lax.broadcasted_iota(jnp.int32, (block_rows, block_rows), 1)
        row = lax.broadcasted_iota(jnp.int32, (block_rows, 1), 0)
        last = jnp.where(col <= row, scores[:, at:], MASKED)
        scores = jnp.concatenate([scores[:, :at], last], axis=1) if block else last
        powers = jnp.exp(scores - jnp.max(scores, axis=-1, keepdims=True))
        probs = powers * (1.0 / jnp.sum(powers, axis=-1, keepdims=True))
        return query, key, probs

    def att_copy(block):
        return remote(
            att.at[block],
            attn.at[c],
            att_send.at[block],
            att_recv.at[lax.rem(block - c + 4, 4)],
            (f, block, t),
        )

    def attention(block):
        keys = (block + 1) * block_rows

        def attend(head, carry, block=block, keys=keys):
            _, _, probs = soft(head, block)
            out = mm(probs.astype(BF), heads[2 * count + head, 0:keys, :], 1, 0)
            att[block, span(head * HD, HD), :] = out.T.astype(BF)
            return carry

        lax.fori_loop(0, count, attend, 0)

        @pl.when(block != c)
        def _():
            att_copy(block).start()

        @pl.when(block == c)
        def _():
            attn[c] = att[block]

    def mask_grad(s, carry):
        row = c * block_rows + lax.broadcasted_iota(jnp.int32, (block_rows, 1), 0)
        grad_low[s] = jnp.where(row < lens[s], cot[s].astype(F32), 0.0).astype(BF)
        return carry

    def masks():
        loads["cot"].wait()
        lax.fori_loop(0, slots, mask_grad, 0)

    def swap(source, target, kind, s):
        return remote(
            source.at[s], target.at[s], part_send.at[kind, s], part_recv.at[kind, s], partner
        )

    def attn_out(s, carry):
        rows = jnp.concatenate([attn[2 * s], attn[2 * s + 1]], axis=0).T
        low[s] = rows
        part_a[s] = mm(rows, wo[...], 1, 1)
        swap(part_a, part_a_in, 0, s).start()
        return carry

    def out_projection():
        for kind in (2, 3):
            landed(OUT, kind)
        for d in (1, 2, 3):
            arrived(attn.at[lax.rem(c - d + 4, 4)], att_recv.at[d])
        lax.fori_loop(0, slots, attn_out, 0)

    def feed(s, carry):
        swap(part_a, part_a_in, 0, s).wait()
        mid = tok[s].astype(F32) + (part_a[s] + part_a_in[s])
        middle[s] = mid
        low_out = norm_rows(mid, gain2[...], bias2[...])[0].astype(BF)
        second[s] = low_out
        rect = jnp.maximum(mm(low_out, wu[...], 1, 0), 0.0)
        wide_a[s] = rect
        act[s] = (rect * rect).astype(BF)
        return carry

    def feed_forward():
        for kind in (2, 3):
            landed(UP, kind)
        lax.fori_loop(0, slots, feed, 0)

    def weight_grad(target, left, right, part):
        chunks = model // 256
        first = chunks * lax.rem(lax.div(f, 2) + 1 - part, 2)

        def step(j, carry):
            at = lanes_at((first + j) * 128, 128)
            rows = left.shape[0] * left.shape[1]
            lhs = left[:, :, at].reshape(rows, 128)
            rhs = right[...].reshape(rows, right.shape[2])
            target[at, :] = mm(lhs, rhs, 0, 0).astype(BF)
            return carry

        lax.fori_loop(0, chunks, step, 0)

    grads = [g_down, g_up, g_out, g_qkv]
    finals = [down_out, up_out, out_out]
    z_outer = 3 * lax.div(c, 2)
    z_near = jnp.where(c == 0, 1, jnp.where(c == 3, 2, 3 - c))

    def size_of(w):
        return rows_half // CUTS[w]

    def rows_of(w, owner, side, u):
        return span(owner * share + side * rows_half + u * size_of(w), size_of(w))

    def cut(w, u):
        return pl.ds(u * size_of(w), size_of(w))

    def near_copy(w, kind, u):
        owner = (fx, fd, fy, fd)[kind]
        return remote(
            grads[w].at[rows_of(w, owner, kind // 2, u)],
            near[w].at[kind, cut(w, u)],
            near_send[w].at[kind, u],
            near_recv[w].at[kind, u],
            (fx, c, t) if kind < 2 else (fy, c, t),
        )

    def far_copy(w, side, u):
        return remote(
            far_send[w].at[side, cut(w, u)],
            far[w].at[side, cut(w, u)],
            far_ssem[w].at[side, u],
            far_recv[w].at[side, u],
            (fy, c, t) if side == 0 else (fx, c, t),
        )

    def hop_one(w, kinds, u):
        for kind in kinds:
            near_copy(w, kind, u).start()

    def hop_two(w, u):
        for side in (0, 1):
            kind = 1 + 2 * side
            near_copy(w, kind, u).wait_recv()
            owner = fy if side == 0 else fx
            own = grads[w][rows_of(w, owner, side, u), :].astype(F32)
            come = near[w][kind, cut(w, u), :].astype(F32)
            far_send[w][side, cut(w, u), :] = (own + come).astype(BF)
            far_copy(w, side, u).start()

    def own_sum(w, side, u):
        near_copy(w, 2 * side, u).wait_recv()
        far_copy(w, side, u).wait_recv()
        own = grads[w][rows_of(w, f, side, u), :].astype(F32)
        return own + near[w][2 * side, cut(w, u), :] + far[w][side, cut(w, u), :]

    def z_rows(w, side, u):
        return pl.ds(side * rows_half + u * size_of(w), size_of(w))

    def z_copy(w, stage, side, u):
        view = z_rows(w, side, u)
        source = (z_own[w], z_own[w], finals[w])[stage].at[view]
        target = (z_in[w].at[0, view], z_in[w].at[1, view], finals[w].at[view])[stage]
        return remote(
            source, target, z_send[w].at[stage, side, u], z_recv[w].at[stage, side, u],
            (f, (z_near, z_near, z_outer)[stage], t),
        )

    def z_one(w, u):
        for side in (0, 1):
            z_own[w][z_rows(w, side, u), :] = own_sum(w, side, u).astype(BF)

            @pl.when(inner == 0)
            def _():
                z_copy(w, 0, side, u).start()

    def z_two(w, u):
        @pl.when(inner == 1)
        def _():
            for side in (0, 1):
                z_copy(w, 0, side, u).wait_recv()
                at = z_rows(w, side, u)
                z_own[w][at, :] = (z_own[w][at, :].astype(F32) + z_in[w][0, at, :]).astype(BF)
                z_copy(w, 1, side, u).start()

    def z_three(w, u):
        @pl.when(inner == 1)
        def _():
            for side in (0, 1):
                z_copy(w, 1, side, u).wait_recv()
                at = z_rows(w, side, u)
                finals[w][at, :] = (z_own[w][at, :].astype(F32) + z_in[w][1, at, :]).astype(BF)
                z_copy(w, 2, side, u).start()

    def reduced(w):
        for u in range(CUTS[w]):
            for kind in range(4):
                near_copy(w, kind, u).wait_send()
            for side in (0, 1):
                far_copy(w, side, u).wait_send()
                if w == QKV:
                    continue

                @pl.when(inner == 1)
                def _():
                    z_copy(w, 1, side, u).wait_send()
                    z_copy(w, 2, side, u).wait_send()

                @pl.when(inner == 0)
                def _():
                    z_copy(w, 0, side, u).wait_send()
                    z_copy(w, 2, side, u).wait_recv()

    def feed_back(s):
        if s == 0:
            for k in range(3):
                arrived(half_of(k, 1 - half), mate_recv.at[k])
        grad = (mm(grad_low[s], wd[...], 1, 0) * 2.0 * wide_a[s]).astype(BF)
        up_grad[s] = grad
        part_b[s] = mm(grad, wu[...], 1, 1)
        swap(part_b, part_b_in, 1, s).start()

    def flat_copy(s, h):
        return remote(
            flat.at[s, h], flat_in.at[c], flat_send.at[s, h],
            flat_recv.at[lax.rem(2 * s + h - c + 4, 4)], (f, 2 * s + h, t),
        )

    in_half = (
        lax.div(lax.broadcasted_iota(jnp.int32, (block_rows, 1), 0), half_rows) == t
    ).astype(F32)

    def norm_two_back(s):
        if s == 0:
            early[0] = jnp.zeros(early.shape[1:], F32)
        swap(part_b, part_b_in, 1, s).wait()
        grad = part_b[s] + part_b_in[s]
        _, normed, recip = norm_rows(middle[s], gain2[...], bias2[...])
        kept = grad * in_half
        early[0, 0:1, :] += jnp.sum(kept * normed, axis=0, keepdims=True)
        early[0, 1:2, :] += jnp.sum(kept, axis=0, keepdims=True)
        back = grad_low[s].astype(F32) + norm_back(grad, normed, recip, gain2[...])
        middle_grad[s] = back
        back = back.astype(BF)
        middle_low[s] = back
        flat_rows = mm(back, wo[...], 1, 0).T.astype(BF)
        for h in (0, 1):
            flat[s, h] = flat_rows[h * part_width : (h + 1) * part_width]

            @pl.when(2 * s + h != c)
            def _():
                flat_copy(s, h).start()

            @pl.when(2 * s + h == c)
            def _():
                flat_in[c] = flat[s, h]

    def down(s, carry):
        part_a[s] = mm(act[s], wd[...], 1, 1)
        swap(part_a, part_a_in, 2, s).start()
        return carry

    def feed_down():
        lax.fori_loop(0, slots, down, 0)

    def put_result():
        for s in range(slots):
            swap(part_a, part_a_in, 2, s).wait()
            result[s] = (middle[s] + (part_a[s] + part_a_in[s])).astype(BF)

    def fg_view(block, rows):
        return wide_a.at[block // 2, rows, pl.ds(block % 2 * model, model)]

    def own_copy(block):
        return remote(
            fg_view(block, theirs), fg_in.at[block], own_send.at[block], own_recv.at[block],
            partner,
        )

    def pair_copy(block):
        return remote(
            fg_low.at[block], pair_in.at[block], pair_send.at[block], pair_recv.at[block],
            (f, mate, t),
        )

    def fg_copy(block):
        return remote(
            fg_low.at[block], fg_other, fg_ssem.at[block], fg_recv.at[0], (f, block, t)
        )

    def collects(block):
        return inner * (1 - (mate == block)) + (1 - inner) * (c == block) == 1

    def hand_over(block):
        own_copy(block).wait_recv()
        total = fg_view(block, mine)[...] + fg_in[block]
        fg_in[block] = total

        @pl.when(jnp.logical_not(collects(block)))
        def _():
            fg_low[block] = total.astype(BF)
            pair_copy(block).start()

    def collect(block):
        @pl.when(collects(block))
        def _():
            arrived(pair_in.at[block], pair_recv.at[block])
            total = fg_in[block] + pair_in[block]

            @pl.when(block == c)
            def _():
                fg_own[...] = total

            @pl.when(block != c)
            def _():
                fg_low[block] = total.astype(BF)
                fg_copy(block).start()

    def attention_back(block):
        if block == blocks - 1:
            key_acc[...] = jnp.zeros_like(key_acc)
            value_acc[...] = jnp.zeros_like(value_acc)
            later[...] = jnp.zeros_like(later)
            conv_acc[...] = jnp.zeros_like(conv_acc)

        @pl.when(block != c)
        def _():
            arrived(flat_in.at[block], flat_recv.at[lax.rem(c - block + 4, 4)])

        keys = (block + 1) * block_rows

        def attend_back(head, carry, block=block, keys=keys):
            query, key, probs = soft(head, block)
            channels = span(head * HD, HD)
            grad_t = flat_in[block, channels, :]
            prob_grad = mm(grad_t.T, heads[2 * count + head, 0:keys, :], 1, 1)
            delta = jnp.sum(probs * prob_grad, axis=-1, keepdims=True)
            score_grad = (probs * (prob_grad - delta)).astype(BF)
            query_t[channels, :] = (mm(score_grad, key, 1, 0) * SCALING).T
            key_acc[head, :, 0:keys] += mm(query.T, score_grad, 1, 0)
            value_acc[head, :, 0:keys] += mm(grad_t, probs.astype(BF), 1, 0)
            return carry

        lax.fori_loop(0, count, attend_back, 0)
        columns = slice(block * block_rows, (block + 1) * block_rows)
        mixed_low[...] = jnp.concatenate(
            [
                query_t[...],
                key_acc[:, :, columns].reshape(part_width, block_rows),
                value_acc[:, :, columns].reshape(part_width, block_rows),
            ],
            axis=0,
        ).T
        mixed = mixed_low[...]
        joined = jnp.concatenate([mixed, later[...]], axis=0)
        next_one = pltpu.roll(joined, block_rows + 7, 0)[:block_rows]
        next_two = pltpu.roll(joined, block_rows + 6, 0)[:block_rows]
        later[...] = mixed[:8]
        before = pre_all[block].astype(F32)
        for at, moved in enumerate((mixed, next_one, next_two)):
            conv_acc[at : at + 1, :] += jnp.sum(before * moved, axis=0, keepdims=True)
        conv_acc[3:4, :] += jnp.sum(mixed, axis=0, keepdims=True)
        grad = (taps[0:1] * mixed + taps[1:2] * next_one + taps[2:3] * next_two).astype(BF)
        pre_grad[block] = grad
        fg_view(block, pl.ds(0, block_rows))[...] = mm(grad, wq[...], 1, 1)
        own_copy(block).start()

    smalls = [(early, early_xy, early_z), (late, late_xy, late_z)]

    def tp_copy(k):
        return remote(
            smalls[k][0].at[0], smalls[k][0].at[1], sm_send.at[k, 0], sm_recv.at[k, 0], partner
        )

    def xy_copy(k, at):
        view = smalls[k][1].at[f]
        return remote(
            view, view, sm_send.at[k, 1 + at], sm_recv.at[k, 1 + at], ((fx, fy, fd)[at], c, t)
        )

    def z_small(k, d):
        view = smalls[k][2].at[c]
        return remote(
            view, view, sm_send.at[k, 3 + d], sm_recv.at[k, 3 + d], (f, lax.rem(c + d, 4), t)
        )

    def small_tp(k):
        tp_copy(k).wait()
        mixed_rows = 2 if k == 0 else smalls[k][0].shape[1]
        total = smalls[k][0][0] + smalls[k][0][1]
        smalls[k][1][f] = smalls[k][0][0]
        smalls[k][1][f, 0:mixed_rows, :] = total[0:mixed_rows]
        for at in range(3):
            xy_copy(k, at).start()

    def small_xy(k):
        for at, owner in enumerate((fx, fy, fd)):
            xy_copy(k, at).wait_send()
            arrived(smalls[k][1].at[owner], sm_recv.at[k, 1 + at])
        own = smalls[k][1]
        smalls[k][2][c] = own[0] + own[1] + own[2] + own[3]
        for d in (1, 2, 3):
            z_small(k, d).start()

    def small_z(k, out):
        for d in (1, 2, 3):
            z_small(k, d).wait_send()
            arrived(smalls[k][2].at[lax.rem(c - d + 4, 4)], sm_recv.at[k, 3 + d])
        own = smalls[k][2]
        out[...] = own[0] + own[1] + own[2] + own[3]

    def small_start(k):
        if k == 0:
            for h in (0, 1):

                @pl.when(half == h)
                def _():
                    for tap in range(4):
                        for kind in range(3):
                            at = 3 * tap + kind
                            lane = (at % 2 * 2 + h) * part_width
                            channels = slice(kind * part_width, (kind + 1) * part_width)
                            early[0, 2 + at // 2 : 3 + at // 2, lane : lane + part_width] = (
                                conv_acc[tap : tap + 1, channels]
                            )

        tp_copy(k).start()

    def q_copy(stage, side, u):
        view = z_rows(QKV, side, u)
        if stage == 0:
            source, target, device = q_own.at[view], q_in.at[view], lax.rem(c + 2, 4)
        else:
            source = target = q_sum.at[half, view]
            device = c + 1 - 2 * half
        return remote(
            source, target, q_send.at[stage, side, u], q_recv.at[stage, side, u], (f, device, t)
        )

    def q_one(u):
        for side in (0, 1):
            q_own[z_rows(QKV, side, u), :] = own_sum(QKV, side, u).astype(BF)
            q_copy(0, side, u).start()

    def q_two(u):
        for side in (0, 1):
            q_copy(0, side, u).wait()
            at = z_rows(QKV, side, u)
            q_sum[half, at, :] = (q_own[at, :].astype(F32) + q_in[at, :]).astype(BF)
            q_copy(1, side, u).start()

    lane = late.shape[2]

    def norm_one_back(k):
        s = slot if k == 0 else 1 - slot
        if k == 0:
            late[0] = jnp.zeros(late.shape[1:], F32)
            grad = fg_own[...]
        else:
            arrived(fg_other, fg_recv.at[0])
            grad = fg_other[...].astype(F32)
        _, normed, recip = norm_rows(tok[s, mine, :].astype(F32), gain1[...], bias1[...])
        gain_sum = jnp.sum(grad * normed, axis=0, keepdims=True)
        bias_sum = jnp.sum(grad, axis=0, keepdims=True)
        for at in range(model // lane):
            lanes = slice(at * lane, (at + 1) * lane)
            late[0, at : at + 1, :] += gain_sum[:, lanes]
            late[0, 4 + at : 5 + at, :] += bias_sum[:, lanes]
        input_grad[s, mine, :] = middle_grad[s, mine, :] + norm_back(
            grad, normed, recip, gain1[...]
        )
        in_copy(k).start()

    def in_copy(k):
        view = input_grad.at[slot if k == 0 else 1 - slot, mine]
        return remote(view, view, in_send.at[k], in_recv.at[k], partner)

    send_out()
    send_direct(QKV)
    tokens(0)
    send_down()
    pass_on(QKV)
    tokens(1)
    send_up()
    tokens(2)
    pass_down()
    own_norm()
    tokens_passed()
    pass_on(OUT)
    projections()
    attention(2)
    attention(1)
    attention(0)
    attention(3)
    pass_on(UP)
    masks()
    out_projection()
    pass_down_last()
    feed_forward()
    weight_grad(g_down, grad_low, act, 0)
    hop_one(DOWN, (1, 3), 2)
    hop_one(DOWN, (1, 3), 1)
    feed_back(0)
    weight_grad(g_down, grad_low, act, 1)
    hop_one(DOWN, (0, 2), 2)
    feed_back(1)
    norm_two_back(0)
    hop_two(DOWN, 2)
    hop_two(DOWN, 1)
    hop_one(DOWN, (1, 3), 0)
    hop_one(DOWN, (0, 2), 1)
    norm_two_back(1)
    weight_grad(g_up, second, up_grad, 0)
    weight_grad(g_up, second, up_grad, 1)
    hop_one(DOWN, (0, 2), 0)
    z_one(DOWN, 2)
    attention_back(3)
    hop_two(DOWN, 0)
    z_two(DOWN, 2)
    hop_one(UP, (1, 3), 1)
    z_one(DOWN, 1)
    attention_back(2)
    hop_one(UP, (1, 3), 2)
    hop_one(UP, (1, 3), 0)
    hop_one(UP, (0, 2), 0)
    hop_one(UP, (0, 2), 2)
    z_one(DOWN, 0)
    hand_over(3)
    z_two(DOWN, 1)
    attention_back(1)
    z_three(DOWN, 2)
    hand_over(2)
    attention_back(0)
    z_two(DOWN, 0)
    hop_two(UP, 0)
    hand_over(0)
    feed_down()
    collect(3)
    z_three(DOWN, 1)
    hand_over(1)
    hop_two(UP, 1)
    hop_two(UP, 2)
    collect(0)
    collect(2)
    small_start(0)
    z_one(UP, 0)
    weight_grad(g_qkv, first_all, pre_grad, 0)
    hop_one(UP, (0, 2), 1)
    put_result()
    for part in (0, 1):
        weight_grad(g_out, middle_low, low, part)
    collect(1)
    z_two(UP, 0)
    z_three(DOWN, 0)
    hop_one(QKV, (1, 3), 0)
    z_one(UP, 2)
    hop_one(OUT, (1, 3), 0)
    z_one(UP, 1)
    weight_grad(g_qkv, first_all, pre_grad, 1)
    hop_one(OUT, (0, 2), 0)
    norm_one_back(0)
    hop_one(QKV, (0, 2), 1)
    hop_one(QKV, (0, 2), 0)
    norm_one_back(1)
    z_two(UP, 2)
    z_three(UP, 0)
    hop_two(OUT, 0)
    hop_one(QKV, (1, 3), 1)
    z_two(UP, 1)
    z_three(UP, 2)
    z_one(OUT, 0)
    hop_two(QKV, 1)
    z_three(UP, 1)
    q_one(1)
    small_start(1)
    z_two(OUT, 0)
    small_tp(0)
    hop_two(QKV, 0)
    q_two(1)
    small_tp(1)
    small_xy(0)
    small_xy(1)
    q_one(0)
    z_three(OUT, 0)
    q_two(0)
    small_z(0, early_out)
    small_z(1, late_out)
    for w in range(4):
        reduced(w)
        for kind in (0, 1):
            direct(w, kind).wait_send()
        for kind in (2, 3):
            relay(w, kind).wait_send()
    for side in (0, 1):
        for u in range(CUTS[QKV]):
            q_copy(1, side, u).wait_send()
            arrived(q_sum.at[1 - half, z_rows(QKV, side, u)], q_recv.at[1, side, u])
    for k in range(3):
        mate_copy(k).wait_send()
        tok_pass(k).wait_send()
        if k < 2:
            tok_copy(k).wait_send()

            @pl.when(inner == 1)
            def _():
                tok_relay(k).wait_send()

    for s in range(slots):
        in_copy(s).wait_send()
        view = input_grad.at[slot if s == 0 else 1 - slot, theirs]
        arrived(view, in_recv.at[s])
        for h in (0, 1):

            @pl.when(2 * s + h != c)
            def _():
                flat_copy(s, h).wait_send()

    for block in range(blocks):
        own_copy(block).wait_send()

        @pl.when(block != c)
        def _():
            att_copy(block).wait_send()

        @pl.when(jnp.logical_not(collects(block)))
        def _():
            pair_copy(block).wait_send()

        @pl.when(collects(block))
        def _():
            @pl.when(block != c)
            def _():
                fg_copy(block).wait_send()


def layer_call(
    lens, tok, cot, wq3, wo, wu, wd, gain1, bias1, gain2, bias2, taps3, shift3
):
    slots, block_rows, model = tok.shape
    share, units, channels = wu.shape[0], wu.shape[1], wo.shape[1]
    part = channels // 2
    width = 3 * part
    blocks = 4
    tall = (slots, block_rows, model)
    wide = (slots, block_rows, units)
    half = block_rows // 2
    columns = [units, units, channels, width]
    dma = pltpu.SemaphoreType.DMA

    def vmem(shape, kind=BF):
        return pltpu.VMEM(tuple(shape), kind)

    def struct(shape, kind=BF):
        return jax.ShapeDtypeStruct(tuple(shape), kind)

    return pl.pallas_call(
        layer_kernel,
        name="layer",
        out_shape=[
            struct(tall), struct(tall, F32), struct((share, units)), struct((share, units)),
            struct((share, channels)), struct((2, share, width)), struct((8, model), F32),
            struct((8, 256), F32),
        ],
        in_specs=[SMEM] + [ANY] * 6 + [VMEM] * 6,
        out_specs=[VMEM] * 8,
        scratch_shapes=[
            vmem(tall), vmem(tall), vmem(wq3.shape), vmem((model, width)),
            vmem((model, channels)), vmem((model, units)), vmem((model, units)),
            vmem((8, width), F32), vmem((8, width), F32), vmem((8, width), F32),
            vmem((blocks, block_rows, model)), vmem((blocks, block_rows, width)),
            vmem((width // HD, blocks * block_rows, HD)),
            vmem((blocks, part, block_rows)), vmem((blocks, part, block_rows)),
            vmem((slots, block_rows, channels)), vmem(tall, F32), vmem(tall, F32),
            vmem(tall, F32), vmem(tall, F32), vmem(wide, F32), vmem(tall, F32), vmem(tall, F32),
            vmem(tall), vmem(tall), vmem(wide), vmem(wide), vmem(tall),
            vmem((slots, 2, part, block_rows)), vmem((4, part, block_rows)),
            vmem((model, units)), vmem((model, units)), vmem((model, channels)),
            vmem((model, width)),
            [vmem((4, share // 2, n)) for n in columns],
            [vmem((2, share // 2, n)) for n in columns],
            [vmem((2, share // 2, n)) for n in columns],
            [vmem((share, n)) for n in columns[:3]],
            [vmem((2, share, n)) for n in columns[:3]],
            vmem((share, width)), vmem((share, width)),
            vmem((8, blocks * block_rows), F32),
            vmem((part // HD, HD, blocks * block_rows), F32),
            vmem((part // HD, HD, blocks * block_rows), F32),
            vmem((part, block_rows), F32), vmem((8, width), F32),
            vmem((block_rows, width), F32), vmem((blocks, block_rows, width)),
            vmem((8, width), F32),
            vmem((blocks, half, model), F32), vmem((blocks, half, model)),
            vmem((blocks, half, model)), vmem((half, model), F32), vmem((half, model)),
            vmem((2, 8, model), F32), vmem((4, 8, model), F32), vmem((4, 8, model), F32),
            vmem((2, 8, 256), F32), vmem((4, 8, 256), F32), vmem((4, 8, 256), F32),
            dma((6,)), dma((4,)), dma((4,)), dma((4,)), dma((4,)), dma((3,)), dma((3,)),
            dma((4, 4)), dma((4, 4)),
            dma((4,)), dma((4,)),
            dma((3, slots)), dma((3, slots)), dma((slots, 2)), dma((4,)),
            [dma((4, n)) for n in CUTS], [dma((4, n)) for n in CUTS],
            [dma((2, n)) for n in CUTS], [dma((2, n)) for n in CUTS],
            [dma((3, 2, n)) for n in CUTS[:3]], [dma((3, 2, n)) for n in CUTS[:3]],
            dma((2, 2, CUTS[QKV])), dma((2, 2, CUTS[QKV])),
            dma((4,)), dma((1,)), dma((4,)), dma((4,)), dma((4,)), dma((4,)), dma((slots,)),
            dma((slots,)),
            dma((2, 7)), dma((2, 7)),
        ],
        compiler_params=pltpu.CompilerParams(
            collective_id=0, has_side_effects=True, vmem_limit_bytes=67043328
        ),
    )(lens, tok, cot, wq3, wo, wu, wd, gain1, bias1, gain2, bias2, taps3, shift3)


def finish_kernel(
    result_in, grad_in, down_in, up_in, out_in, qkv_in, early, late,
    result, grad, gain1, bias1, qkv, taps, shift, out, gain2, bias2, up, down,
):
    result[...] = result_in[...]
    grad[...] = grad_in[...]
    down[...] = down_in[...].astype(F32)
    up[...] = up_in[...].astype(F32)
    out[...] = out_in[...].astype(F32)
    part = qkv_in.shape[2] // 3
    for kind in range(3):
        for h in (0, 1):
            qkv[kind, :, h * part : (h + 1) * part] = qkv_in[
                h, :, kind * part : (kind + 1) * part
            ].astype(F32)
    lane = late.shape[1]
    for at in range(gain1.shape[0] // lane):
        lanes = slice(at * lane, (at + 1) * lane)
        gain1[lanes] = late[at]
        bias1[lanes] = late[4 + at]
    gain2[...] = early[0]
    bias2[...] = early[1]
    for at in range(12):
        lane = at % 2 * 2 * part
        values = early[2 + at // 2 : 3 + at // 2, lane : lane + 2 * part]
        tap, kind = at // 3, at % 3
        if tap < 3:
            taps[tap, kind : kind + 1, :] = values
        else:
            shift[kind : kind + 1, :] = values


def finish_call(result, grad, down, up, out, qkv, early, late):
    channels, share, model = out.shape[1], out.shape[0], result.shape[2]

    def struct(shape, kind=F32):
        return jax.ShapeDtypeStruct(tuple(shape), kind)

    vector = struct((model,))
    steps = 4
    rows = share // steps
    cut = result.shape[1] * result.shape[0] // steps

    def tall(index):
        return index // 2, index % 2, 0

    def whole(shape):
        return pl.BlockSpec(shape, lambda index: (0,) * len(shape))

    def block(width):
        return pl.BlockSpec((rows, width), lambda index: (index, 0))

    def triple(count, width):
        return pl.BlockSpec((count, rows, width), lambda index: (0, index, 0))

    tall_spec = pl.BlockSpec((1, cut, model), tall)
    vector_spec = whole((model,))
    units = up.shape[1]
    return pl.pallas_call(
        finish_kernel,
        grid=(steps,),
        in_specs=[
            tall_spec, tall_spec, block(units), block(units), block(channels),
            triple(2, qkv.shape[2]), whole(early.shape), whole(late.shape),
        ],
        out_specs=[
            tall_spec, tall_spec, vector_spec, vector_spec, triple(3, channels),
            whole((3, 3, channels)), whole((3, channels)), block(channels), vector_spec,
            vector_spec, block(units), block(units),
        ],
        name="finish",
        out_shape=[
            struct(result.shape, BF), struct(grad.shape), vector, vector,
            struct((3, share, channels)), struct((3, 3, channels)), struct((3, channels)),
            struct(out.shape), vector, vector, struct(up.shape), struct(down.shape),
        ],
    )(result, grad, down, up, out, qkv, early, late)


def local(
    tokens,
    lengths,
    cotangent,
    ln1_gain,
    ln1_bias,
    qkv_weight,
    conv_kernel,
    conv_bias,
    out_weight,
    ln2_gain,
    ln2_bias,
    up_weight,
    down_weight,
):
    batches, block_rows, model_width = tokens.shape
    all_rows = batches * block_rows
    qkv_full, out_full, up_full_w, down_full_w = (
        lax.all_gather(qkv_weight, "fsdp", axis=0, tiled=True),
        lax.all_gather(out_weight, "fsdp", axis=1, tiled=True),
        lax.all_gather(up_weight, "fsdp", axis=0, tiled=True),
        lax.all_gather(down_weight, "fsdp", axis=1, tiled=True),
    )
    local_width = qkv_full.shape[2]
    local_heads = local_width // HD
    ctx_count = lax.axis_size("ctx")
    slot_span = block_rows * ctx_count
    group_blocks = 4
    key_span = block_rows * group_blocks
    ctx_index = lax.axis_index("ctx")
    positions = ctx_index * block_rows + jnp.arange(block_rows, dtype=jnp.int32)
    span_iota = jnp.arange(key_span, dtype=jnp.int32)
    block_count = (ctx_index * block_rows + block_rows + key_span - 1) // key_span
    token_valid = positions[None, :] < lengths[:, None]

    def span_slice(array_data, block, axis_pos):
        return lax.dynamic_slice_in_dim(array_data, block * key_span, key_span, axis_pos)

    inputs = tokens.astype(jnp.float32).reshape(all_rows, model_width)
    first_out, first_hat, first_recip = layer_norm(inputs, ln1_gain, ln1_bias)
    first_low = first_out.astype(jnp.bfloat16)
    pre_low = jnp.einsum(
        "td,dcn->tcn", first_low, qkv_full, preferred_element_type=jnp.float32
    ).astype(jnp.bfloat16)
    pre_low = pre_low.reshape(batches, block_rows, 3, local_width)
    earlier = shifted(pre_low[:, block_rows - 2 :], "ctx", 1)
    extended = jnp.concatenate([earlier, pre_low], axis=1).astype(jnp.float32)
    conv_out = (
        conv_bias
        + conv_kernel[0] * extended[:, 2:]
        + conv_kernel[1] * extended[:, 1:-1]
        + conv_kernel[2] * extended[:, :-2]
    ).astype(jnp.bfloat16)
    query_heads = conv_out[:, :, 0].reshape(batches, block_rows, local_heads, HD)
    own_pairs = conv_out[:, :, 1:]
    whole_pairs = lax.all_gather(own_pairs, "ctx", axis=1, tiled=True)
    key_heads = whole_pairs[:, :, 0].reshape(batches, slot_span, local_heads, HD)
    value_heads = whole_pairs[:, :, 1].reshape(batches, slot_span, local_heads, HD)

    def stat_step(block, carry):
        row_max, total = carry
        key_pos = block * key_span + span_iota
        scores = tile_scores(
            query_heads, span_slice(key_heads, block, 1), positions, key_pos, lengths
        )
        new_max = jnp.maximum(row_max, jnp.max(scores, axis=-1, keepdims=True))
        total = total * jnp.exp(row_max - new_max) + jnp.sum(
            jnp.exp(scores - new_max), axis=-1, keepdims=True
        )
        return (new_max, total)

    stat_shape = (batches, local_heads, block_rows, 1)
    row_max, total = lax.fori_loop(
        0,
        block_count,
        stat_step,
        (jnp.full(stat_shape, MASKED, jnp.float32), jnp.zeros(stat_shape, jnp.float32)),
    )
    log_total = row_max + jnp.log(total)

    def value_step(block, accum):
        key_pos = block * key_span + span_iota
        scores = tile_scores(
            query_heads, span_slice(key_heads, block, 1), positions, key_pos, lengths
        )
        probs_low = jnp.exp(scores - log_total).astype(jnp.bfloat16)
        return accum + jnp.einsum(
            "mhqk,mkhd->mqhd",
            probs_low,
            span_slice(value_heads, block, 1),
            preferred_element_type=jnp.float32,
        )

    attn_acc = lax.fori_loop(
        0, block_count, value_step, jnp.zeros((batches, block_rows, local_heads, HD), jnp.float32)
    )
    attn_low = attn_acc.reshape(all_rows, local_width).astype(jnp.bfloat16)
    attn_out = lax.psum(jnp.dot(attn_low, out_full, preferred_element_type=jnp.float32), "tp")
    middle = inputs + attn_out
    second_out, second_hat, second_recip = layer_norm(middle, ln2_gain, ln2_bias)
    second_low = second_out.astype(jnp.bfloat16)
    up_full = jnp.dot(second_low, up_full_w, preferred_element_type=jnp.float32)
    rectified = jnp.maximum(up_full, 0.0)
    act_low = (rectified * rectified).astype(jnp.bfloat16)
    ffn_out = lax.psum(jnp.dot(act_low, down_full_w, preferred_element_type=jnp.float32), "tp")
    result = (middle + ffn_out).reshape(batches, block_rows, model_width).astype(jnp.bfloat16)
    grad_out = (
        cotangent.astype(jnp.float32) * token_valid[:, :, None].astype(jnp.float32)
    ).reshape(all_rows, model_width)
    grad_low = grad_out.astype(jnp.bfloat16)
    down_wgrad = jnp.einsum("tf,td->fd", act_low, grad_low, preferred_element_type=jnp.float32)
    act_grad = jnp.einsum("td,fd->tf", grad_low, down_full_w, preferred_element_type=jnp.float32)
    up_grad_low = (act_grad * 2.0 * rectified).astype(jnp.bfloat16)
    up_wgrad = jnp.einsum("td,tf->df", second_low, up_grad_low, preferred_element_type=jnp.float32)
    second_grad = lax.psum(
        jnp.einsum("tf,df->td", up_grad_low, up_full_w, preferred_element_type=jnp.float32), "tp"
    )
    gain_two_grad = jnp.sum(second_grad * second_hat, axis=0)
    bias_two_grad = jnp.sum(second_grad, axis=0)
    middle_grad = grad_out + norm_back(second_grad, second_hat, second_recip, ln2_gain)
    middle_low = middle_grad.astype(jnp.bfloat16)
    out_wgrad = jnp.einsum("tn,td->nd", attn_low, middle_low, preferred_element_type=jnp.float32)
    attn_flat = jnp.einsum(
        "td,nd->tn", middle_low, out_full, preferred_element_type=jnp.float32
    ).astype(jnp.bfloat16)
    attn_grad = attn_flat.reshape(batches, block_rows, local_heads, HD)

    def delta_step(block, accum):
        key_pos = block * key_span + span_iota
        probs_full = jnp.exp(
            tile_scores(query_heads, span_slice(key_heads, block, 1), positions, key_pos, lengths)
            - log_total
        )
        prob_grad = jnp.einsum(
            "mqhd,mkhd->mhqk",
            attn_grad,
            span_slice(value_heads, block, 1),
            preferred_element_type=jnp.float32,
        )
        return accum + jnp.sum(probs_full * prob_grad, axis=-1, keepdims=True)

    delta = lax.fori_loop(0, block_count, delta_step, jnp.zeros(stat_shape, jnp.float32))
    query_zero = jnp.zeros((batches, block_rows, local_heads, HD), jnp.float32)

    def back_step(block, carry):
        accum, buffer = carry
        key_pos = block * key_span + span_iota
        key_part = span_slice(key_heads, block, 1)
        probs_full, prob_grad, score_grad = tile_grads(
            query_heads,
            key_part,
            span_slice(value_heads, block, 1),
            attn_grad,
            log_total,
            delta,
            positions,
            key_pos,
            lengths,
        )
        probs_again = probs_full.astype(jnp.bfloat16)
        accum = (
            accum
            + jnp.einsum(
                "mhqk,mkhd->mqhd", score_grad, key_part, preferred_element_type=jnp.float32
            )
            * SCALING
        )
        key_term = (
            jnp.einsum(
                "mhqk,mqhd->mkhd", score_grad, query_heads, preferred_element_type=jnp.float32
            )
            * SCALING
        )
        value_term = jnp.einsum(
            "mhqk,mqhd->mkhd", probs_again, attn_grad, preferred_element_type=jnp.float32
        )
        stacked = jnp.stack(
            [
                key_term.reshape(batches, key_span, local_width),
                value_term.reshape(batches, key_span, local_width),
            ],
            axis=2,
        )
        buffer = lax.dynamic_update_slice_in_dim(buffer, stacked, block * key_span, 1)
        return (accum, buffer)

    buffer_zero = jnp.zeros((batches, slot_span, 2, local_width), jnp.float32)
    query_grad, pair_terms = lax.fori_loop(0, block_count, back_step, (query_zero, buffer_zero))
    pair_grad = lax.psum_scatter(pair_terms, "ctx", scatter_dimension=1, tiled=True)
    mixed_grad = jnp.concatenate(
        [query_grad.reshape(batches, block_rows, 1, local_width), pair_grad], axis=2
    )
    later = shifted(mixed_grad[:, :2], "ctx", -1)
    ahead = jnp.concatenate([mixed_grad, later], axis=1)
    pre_grad = (
        conv_kernel[0] * ahead[:, :block_rows]
        + conv_kernel[1] * ahead[:, 1 : block_rows + 1]
        + conv_kernel[2] * ahead[:, 2:]
    ).astype(jnp.bfloat16)
    kernel_grad = jnp.stack(
        [
            jnp.sum(extended[:, 2 - offset : 2 - offset + block_rows] * mixed_grad, axis=(0, 1))
            for offset in range(3)
        ]
    )
    shift_grad = jnp.sum(mixed_grad, axis=(0, 1))
    pre_grad = pre_grad.reshape(all_rows, 3, local_width)
    qkv_wgrad = jnp.einsum("td,tcn->dcn", first_low, pre_grad, preferred_element_type=jnp.float32)
    first_grad = lax.psum(
        jnp.einsum("tcn,dcn->td", pre_grad, qkv_full, preferred_element_type=jnp.float32), "tp"
    )
    gain_one_grad = jnp.sum(first_grad * first_hat, axis=0)
    bias_one_grad = jnp.sum(first_grad, axis=0)
    input_grad = middle_grad + norm_back(first_grad, first_hat, first_recip, ln1_gain)
    input_grad = input_grad.reshape(batches, block_rows, model_width)
    summed = lax.psum(
        (
            qkv_wgrad,
            out_wgrad,
            up_wgrad,
            down_wgrad,
            gain_one_grad,
            bias_one_grad,
            kernel_grad,
            shift_grad,
            gain_two_grad,
            bias_two_grad,
        ),
        ("fsdp", "ctx"),
    )
    share_rows = model_width // lax.axis_size("fsdp")
    owner_start = lax.axis_index("fsdp") * share_rows
    qkv_share = lax.dynamic_slice_in_dim(summed[0], owner_start, share_rows, 0)
    out_share = lax.dynamic_slice_in_dim(summed[1], owner_start, share_rows, 1)
    up_share = lax.dynamic_slice_in_dim(summed[2], owner_start, share_rows, 0)
    down_share = lax.dynamic_slice_in_dim(summed[3], owner_start, share_rows, 1)
    small_sums = summed[4:]
    return (
        result,
        input_grad,
        small_sums[0],
        small_sums[1],
        qkv_share,
        small_sums[2],
        small_sums[3],
        out_share,
        small_sums[4],
        small_sums[5],
        up_share,
        down_share,
    )


def local_fast(
    tokens,
    lengths,
    cotangent,
    ln1_gain,
    ln1_bias,
    qkv_weight,
    conv_kernel,
    conv_bias,
    out_weight,
    ln2_gain,
    ln2_bias,
    up_weight,
    down_weight,
):
    parts = layer_call(
        lengths, tokens, cotangent, qkv_weight.transpose(1, 0, 2), out_weight.T, up_weight,
        down_weight.T, ln1_gain, ln1_bias, ln2_gain, ln2_bias, conv_kernel, conv_bias,
    )
    result, grad, gain1, bias1, qkv, taps, shift, out, gain2, bias2, up, down = finish_call(*parts)
    return (
        result, grad, gain1, bias1, qkv.transpose(1, 0, 2), taps, shift, out.T, gain2, bias2, up,
        down.T,
    )


def solution(mesh):
    placed = (
        P("fsdp", "ctx", None),
        P("fsdp"),
        P("fsdp", "ctx", None),
        P(),
        P(),
        P("fsdp", None, "tp"),
        P(None, None, "tp"),
        P(None, "tp"),
        P("tp", "fsdp"),
        P(),
        P(),
        P("fsdp", "tp"),
        P("tp", "fsdp"),
    )
    ctx, fsdp, tp = mesh.shape["ctx"], mesh.shape["fsdp"], mesh.shape["tp"]
    return jax.shard_map(
        local_fast if (fsdp, ctx, tp) == (4, 4, 2) else local,
        mesh=mesh,
        in_specs=placed,
        out_specs=(
            P("fsdp", "ctx", None),
            P("fsdp", "ctx", None),
            P(),
            P(),
            P("fsdp", None, "tp"),
            P(None, None, "tp"),
            P(None, "tp"),
            P("tp", "fsdp"),
            P(),
            P(),
            P("fsdp", "tp"),
            P("tp", "fsdp"),
        ),
        check_vma=False,
    )
```

```python
import jax
import jax.numpy as jnp
from jax import lax
from jax.experimental import pallas as pl
from jax.experimental.pallas import tpu as pltpu
from jax.sharding import PartitionSpec as P

HD = 64


EPSILON = 1e-05
SCALING = 0.125
MASKED = -1e30


def shifted(block, axis, distance):
    devices = range(lax.axis_size(axis))
    route = [(i - distance, i) for i in devices if i - distance in devices]
    return lax.ppermute(block, axis, route)


def layer_norm(row_data, norm_gain, shift_bias):
    centred = row_data - jnp.mean(row_data, axis=-1, keepdims=True)
    recip = lax.rsqrt(jnp.mean(centred * centred, axis=-1, keepdims=True) + EPSILON)
    normed = centred * recip
    return (normed * norm_gain + shift_bias, normed, recip)


def norm_back(grad_in, normed, recip, norm_gain):
    scaled = grad_in * norm_gain
    return recip * (
        scaled
        - jnp.mean(scaled, axis=-1, keepdims=True)
        - normed * jnp.mean(scaled * normed, axis=-1, keepdims=True)
    )


def tile_scores(query_part, key_part, query_pos, key_pos, lengths):
    scores = (
        jnp.einsum("mqhd,mkhd->mhqk", query_part, key_part, preferred_element_type=jnp.float32)
        * SCALING
    )
    allowed = (key_pos[None, None, :] <= query_pos[None, :, None]) & (
        key_pos[None, None, :] < lengths[:, None, None]
    )
    return jnp.where(allowed[:, None], scores, MASKED)


def tile_grads(
    query_part, key_part, value_part, grad_part, log_part, delta_part, query_pos, key_pos, lengths
):
    probs_full = jnp.exp(tile_scores(query_part, key_part, query_pos, key_pos, lengths) - log_part)
    prob_grad = jnp.einsum(
        "mqhd,mkhd->mhqk", grad_part, value_part, preferred_element_type=jnp.float32
    )
    score_grad = (probs_full * (prob_grad - delta_part)).astype(jnp.bfloat16)
    return (probs_full, prob_grad, score_grad)


def norm_rows(x, gain, bias):
    centred = x - jnp.mean(x, axis=-1, keepdims=True)
    recip = lax.rsqrt(jnp.mean(centred * centred, axis=-1, keepdims=True) + EPSILON)
    normed = centred * recip
    return normed * gain + bias, normed, recip


BF = jnp.bfloat16
F32 = jnp.float32
MESH = pl.DeviceIdType.MESH
ANY = pl.BlockSpec(memory_space=pl.ANY)
VMEM = pl.BlockSpec(memory_space=pltpu.VMEM)
SMEM = pl.BlockSpec(memory_space=pltpu.SMEM)
CUTS = (3, 3, 1, 2)
DOWN, UP, OUT, QKV = range(4)


def mm(left, right, left_dim, right_dim):
    return lax.dot_general(
        left, right, (((left_dim,), (right_dim,)), ((), ())), preferred_element_type=F32
    )


def remote(source, target, send_sem, recv_sem, device):
    return pltpu.make_async_remote_copy(
        src_ref=source,
        dst_ref=target,
        send_sem=send_sem,
        recv_sem=recv_sem,
        device_id=device,
        device_id_type=MESH,
    )


def span(start, size):
    return pl.ds(pl.multiple_of(start, 16), size)


def lanes_at(start, size):
    return pl.ds(pl.multiple_of(start, 128), size)


def layer_kernel(
    lens, tok_in, cot_in, wq_in, wo_in, wu_in, wd_in,
    gain1, bias1, gain2, bias2, taps3, shift3,
    result, input_grad, down_out, up_out, out_out, q_sum, early_out, late_out,
    tok, cot, wq_buf, wq, wo, wu, wd, taps, shift, prev,
    first_all, pre_all, heads, att, attn,
    low, part_a, part_a_in, part_b, part_b_in, wide_a, middle, middle_grad,
    second, grad_low, act, up_grad, middle_low, flat, flat_in,
    g_down, g_up, g_out, g_qkv, near, far_send, far, z_own, z_in, q_own, q_in,
    key_bias, key_acc, value_acc, query_t, later, mixed_low, pre_grad, conv_acc,
    fg_in, fg_low, pair_in, fg_own, fg_other, early, early_xy, early_z, late, late_xy, late_z,
    load_sem, tok_send, tok_recv, pass_send, pass_recv, mate_send, mate_recv, w_send, w_recv, att_send, att_recv,
    part_send, part_recv, flat_send, flat_recv,
    near_send, near_recv, far_ssem, far_recv, z_send, z_recv, q_send, q_recv,
    fg_ssem, fg_recv, pair_send, pair_recv, own_send, own_recv, in_send, in_recv, sm_send, sm_recv,
):
    f, c, t = lax.axis_index("fsdp"), lax.axis_index("ctx"), lax.axis_index("tp")
    fx = f + 1 - 2 * lax.rem(f, 2)
    fy = lax.rem(f + 2, 4)
    fd = lax.rem(fx + 2, 4)
    slot = lax.div(c, 2)
    half = lax.rem(c, 2)
    other = 1 - t
    partner = (f, c, other)
    barrier = pltpu.get_barrier_semaphore()
    peers = [(fx, c, t), (fy, c, t), (fd, c, t), partner]
    peers += [(f, lax.rem(c + d, 4), t) for d in (1, 2, 3)]
    for peer in peers:
        pl.semaphore_signal(barrier, inc=1, device_id=peer, device_id_type=MESH)

    slots, block_rows, model = tok.shape
    width = wq.shape[1]
    part_width = width // 3
    count = part_width // HD
    blocks = 4
    half_rows = block_rows // 2
    share = model // 4
    rows_half = share // 2
    mine = span(t * half_rows, half_rows)
    theirs = span(other * half_rows, half_rows)

    def arrived(view, sem):
        remote(view, view, tok_send.at[0], sem, partner).wait_recv()

    wholes = [wd, wu, wo, wq]
    shard_rows = span(f * share, share)
    loads = {}
    for at, (name, source, target) in enumerate(
        [
            ("wq", wq_in, wq_buf),
            ("tok", tok_in, tok),
            (OUT, wo_in, wo.at[shard_rows]),
            (UP, wu_in, wu.at[shard_rows]),
            (DOWN, wd_in, wd.at[shard_rows]),
            ("cot", cot_in, cot),
        ]
    ):
        loads[name] = pltpu.make_async_copy(source, target, load_sem.at[at])
        loads[name].start()
    pl.semaphore_wait(barrier, len(peers))

    inner = lax.rem(lax.div(c + 1, 2), 2)
    mate = c + 1 - 2 * half
    across = 2 - slot
    far_side = 3 - 3 * slot

    def tok_copy(k):
        return remote(
            tok_in.at[slot if k == 0 else 1 - slot, mine],
            first_all.at[c, mine],
            tok_send.at[k],
            tok_recv.at[c],
            (f, mate if k == 0 else across, t),
        )

    def tok_order(k):
        near_in, near_out = ((across, mate), (far_side, across), (mate, far_side))[k]
        return inner * near_in + (1 - inner) * near_out

    def tok_relay(k):
        view = first_all.at[tok_order(k), mine]
        return remote(
            view, view, tok_send.at[2 + k], tok_recv.at[tok_order(k)], (f, mate, t)
        )

    def tok_pass(k):
        view = first_all.at[tok_order(k), mine]
        return remote(view, view, pass_send.at[k], pass_recv.at[k], partner)

    for k in (0, 1):
        tok_copy(k).start()


    def shard_part(w, owner, kind):
        start, size = owner * share, share
        if w == DOWN:
            start, size = start + half * rows_half, rows_half
        if kind < 2:
            return span(start, size)
        return span(start + (kind - 2) * (size // 2), size // 2)

    def direct(w, kind):
        view = wholes[w].at[shard_part(w, f, 0)]
        target = (fx, c, t) if kind == 0 else (fy, c, t)
        return remote(view, view, w_send.at[w, kind], w_recv.at[w, kind], target)

    def relay(w, kind):
        origin, target = (fx, (fy, c, t)) if kind == 2 else (fy, (fx, c, t))
        view = wholes[w].at[shard_part(w, origin, kind)]
        return remote(view, view, w_send.at[w, kind], w_recv.at[w, kind], target)

    def landed(w, kind):
        owner = (fx, fy, fd, fd)[kind]
        arrived(wholes[w].at[shard_part(w, owner, kind)], w_recv.at[w, kind])

    def send_direct(w):
        direct(w, 0).start()
        direct(w, 1).start()

    def pass_on(w):
        landed(w, 0)
        relay(w, 2).start()
        landed(w, 1)
        relay(w, 3).start()

    def half_of(k, side):
        return wd.at[span((fx, fy, fd)[k] * share + side * rows_half, rows_half)]

    def mate_copy(k):
        view = half_of(k, half)
        return remote(view, view, mate_send.at[k], mate_recv.at[k], (f, mate, t))

    def pass_down():
        for k in (0, 1):
            landed(DOWN, k)
            relay(DOWN, 2 + k).start()
            mate_copy(k).start()

    def pass_down_last():
        landed(DOWN, 2)
        landed(DOWN, 3)
        mate_copy(2).start()

    loads["wq"].wait()
    for h in (0, 1):

        @pl.when(half == h)
        def _():
            lanes = slice(h * part_width, (h + 1) * part_width)
            for kind in range(3):
                target = slice(kind * part_width, (kind + 1) * part_width)
                wq[shard_rows, target] = wq_buf[kind, :, lanes]
                shift[0:1, target] = shift3[kind : kind + 1, lanes]
                for tap in range(3):
                    taps[tap : tap + 1, target] = taps3[tap, kind : kind + 1, lanes]

    def first_norm(x):
        return norm_rows(x.astype(F32), gain1[...], bias1[...])[0].astype(BF)

    def own_norm():
        loads["tok"].wait()
        first_all[c] = first_norm(tok[slot])

    def tokens(k):
        source = tok_order(k)
        arrived(first_all.at[source, mine], tok_recv.at[source])

        @pl.when((inner == 1) | (k == 0))
        def _():
            first_all[source, mine, :] = first_norm(first_all[source, mine, :])

        if k < 2:

            @pl.when(inner == 1)
            def _():
                tok_relay(k).start()

        tok_pass(k).start()

    def tokens_passed():
        for k in range(3):
            arrived(first_all.at[tok_order(k), theirs], pass_recv.at[k])

    def send_out():
        loads[OUT].wait()
        send_direct(OUT)

    def send_up():
        loads[UP].wait()
        send_direct(UP)

    def send_down():
        loads[DOWN].wait()
        send_direct(DOWN)

    def project(block, carry):
        pre = mm(first_all[block], wq[...], 1, 0).astype(BF)
        pre_all[block] = pre
        pre = pre.astype(F32)
        joined = jnp.concatenate([prev[...], pre], axis=0)
        prev[...] = pre[-8:]
        out = (
            shift[0:1]
            + taps[0:1] * pre
            + taps[1:2] * pltpu.roll(joined, 1, 0)[8:]
            + taps[2:3] * pltpu.roll(joined, 2, 0)[8:]
        ).astype(BF)
        at = span(block * block_rows, block_rows)
        for head in range(3 * count):
            piece = out[:, head * HD : (head + 1) * HD]
            if head < count:
                piece = (piece.astype(F32) * SCALING).astype(BF)
            heads[head, at, :] = piece
        return carry

    def projections():
        landed(QKV, 2)
        landed(QKV, 3)
        prev[...] = jnp.zeros_like(prev)
        lax.fori_loop(0, blocks, project, 0)
        at = lax.broadcasted_iota(jnp.int32, key_bias.shape, 1)
        key_bias[...] = jnp.where(at < lens[slot], 0.0, MASKED)

    def soft(head, block):
        at = block * block_rows
        query = heads[head, at : at + block_rows, :]
        key = heads[count + head, 0 : at + block_rows, :]
        scores = mm(query, key, 1, 1) + key_bias[0:1, 0 : at + block_rows]
        col = lax.broadcasted_iota(jnp.int32, (block_rows, block_rows), 1)
        row = lax.broadcasted_iota(jnp.int32, (block_rows, 1), 0)
        last = jnp.where(col <= row, scores[:, at:], MASKED)
        scores = jnp.concatenate([scores[:, :at], last], axis=1) if block else last
        powers = jnp.exp(scores - jnp.max(scores, axis=-1, keepdims=True))
        probs = powers * (1.0 / jnp.sum(powers, axis=-1, keepdims=True))
        return query, key, probs

    def att_copy(block):
        return remote(
            att.at[block],
            attn.at[c],
            att_send.at[block],
            att_recv.at[lax.rem(block - c + 4, 4)],
            (f, block, t),
        )

    def attention(block):
        keys = (block + 1) * block_rows

        def attend(head, carry, block=block, keys=keys):
            _, _, probs = soft(head, block)
            out = mm(probs.astype(BF), heads[2 * count + head, 0:keys, :], 1, 0)
            att[block, span(head * HD, HD), :] = out.T.astype(BF)
            return carry

        lax.fori_loop(0, count, attend, 0)

        @pl.when(block != c)
        def _():
            att_copy(block).start()

        @pl.when(block == c)
        def _():
            attn[c] = att[block]

    def mask_grad(s, carry):
        row = c * block_rows + lax.broadcasted_iota(jnp.int32, (block_rows, 1), 0)
        grad_low[s] = jnp.where(row < lens[s], cot[s].astype(F32), 0.0).astype(BF)
        return carry

    def masks():
        loads["cot"].wait()
        lax.fori_loop(0, slots, mask_grad, 0)

    def swap(source, target, kind, s):
        return remote(
            source.at[s], target.at[s], part_send.at[kind, s], part_recv.at[kind, s], partner
        )

    def attn_out(s, carry):
        rows = jnp.concatenate([attn[2 * s], attn[2 * s + 1]], axis=0).T
        low[s] = rows
        part_a[s] = mm(rows, wo[...], 1, 1)
        swap(part_a, part_a_in, 0, s).start()
        return carry

    def out_projection():
        for kind in (2, 3):
            landed(OUT, kind)
        for d in (1, 2, 3):
            arrived(attn.at[lax.rem(c - d + 4, 4)], att_recv.at[d])
        lax.fori_loop(0, slots, attn_out, 0)

    def feed(s, carry):
        swap(part_a, part_a_in, 0, s).wait()
        mid = tok[s].astype(F32) + (part_a[s] + part_a_in[s])
        middle[s] = mid
        low_out = norm_rows(mid, gain2[...], bias2[...])[0].astype(BF)
        second[s] = low_out
        rect = jnp.maximum(mm(low_out, wu[...], 1, 0), 0.0)
        wide_a[s] = rect
        act[s] = (rect * rect).astype(BF)
        return carry

    def feed_forward():
        for kind in (2, 3):
            landed(UP, kind)
        lax.fori_loop(0, slots, feed, 0)

    def weight_grad(target, left, right, part):
        chunks = model // 256
        first = chunks * lax.rem(lax.div(f, 2) + 1 - part, 2)

        def step(j, carry):
            at = lanes_at((first + j) * 128, 128)
            rows = left.shape[0] * left.shape[1]
            lhs = left[:, :, at].reshape(rows, 128)
            rhs = right[...].reshape(rows, right.shape[2])
            target[at, :] = mm(lhs, rhs, 0, 0).astype(BF)
            return carry

        lax.fori_loop(0, chunks, step, 0)

    grads = [g_down, g_up, g_out, g_qkv]
    finals = [down_out, up_out, out_out]
    z_outer = 3 * lax.div(c, 2)
    z_near = jnp.where(c == 0, 1, jnp.where(c == 3, 2, 3 - c))

    def size_of(w):
        return rows_half // CUTS[w]

    def rows_of(w, owner, side, u):
        return span(owner * share + side * rows_half + u * size_of(w), size_of(w))

    def cut(w, u):
        return pl.ds(u * size_of(w), size_of(w))

    def near_copy(w, kind, u):
        owner = (fx, fd, fy, fd)[kind]
        return remote(
            grads[w].at[rows_of(w, owner, kind // 2, u)],
            near[w].at[kind, cut(w, u)],
            near_send[w].at[kind, u],
            near_recv[w].at[kind, u],
            (fx, c, t) if kind < 2 else (fy, c, t),
        )

    def far_copy(w, side, u):
        return remote(
            far_send[w].at[side, cut(w, u)],
            far[w].at[side, cut(w, u)],
            far_ssem[w].at[side, u],
            far_recv[w].at[side, u],
            (fy, c, t) if side == 0 else (fx, c, t),
        )

    def hop_one(w, kinds, u):
        for kind in kinds:
            near_copy(w, kind, u).start()

    def hop_two(w, u):
        for side in (0, 1):
            kind = 1 + 2 * side
            near_copy(w, kind, u).wait_recv()
            owner = fy if side == 0 else fx
            own = grads[w][rows_of(w, owner, side, u), :].astype(F32)
            come = near[w][kind, cut(w, u), :].astype(F32)
            far_send[w][side, cut(w, u), :] = (own + come).astype(BF)
            far_copy(w, side, u).start()

    def own_sum(w, side, u):
        near_copy(w, 2 * side, u).wait_recv()
        far_copy(w, side, u).wait_recv()
        own = grads[w][rows_of(w, f, side, u), :].astype(F32)
        return own + near[w][2 * side, cut(w, u), :] + far[w][side, cut(w, u), :]

    def z_rows(w, side, u):
        return pl.ds(side * rows_half + u * size_of(w), size_of(w))

    def z_copy(w, stage, side, u):
        view = z_rows(w, side, u)
        source = (z_own[w], z_own[w], finals[w])[stage].at[view]
        target = (z_in[w].at[0, view], z_in[w].at[1, view], finals[w].at[view])[stage]
        return remote(
            source, target, z_send[w].at[stage, side, u], z_recv[w].at[stage, side, u],
            (f, (z_near, z_near, z_outer)[stage], t),
        )

    def z_one(w, u):
        for side in (0, 1):
            z_own[w][z_rows(w, side, u), :] = own_sum(w, side, u).astype(BF)

            @pl.when(inner == 0)
            def _():
                z_copy(w, 0, side, u).start()

    def z_two(w, u):
        @pl.when(inner == 1)
        def _():
            for side in (0, 1):
                z_copy(w, 0, side, u).wait_recv()
                at = z_rows(w, side, u)
                z_own[w][at, :] = (z_own[w][at, :].astype(F32) + z_in[w][0, at, :]).astype(BF)
                z_copy(w, 1, side, u).start()

    def z_three(w, u):
        @pl.when(inner == 1)
        def _():
            for side in (0, 1):
                z_copy(w, 1, side, u).wait_recv()
                at = z_rows(w, side, u)
                finals[w][at, :] = (z_own[w][at, :].astype(F32) + z_in[w][1, at, :]).astype(BF)
                z_copy(w, 2, side, u).start()

    def reduced(w):
        for u in range(CUTS[w]):
            for kind in range(4):
                near_copy(w, kind, u).wait_send()
            for side in (0, 1):
                far_copy(w, side, u).wait_send()
                if w == QKV:
                    continue

                @pl.when(inner == 1)
                def _():
                    z_copy(w, 1, side, u).wait_send()
                    z_copy(w, 2, side, u).wait_send()

                @pl.when(inner == 0)
                def _():
                    z_copy(w, 0, side, u).wait_send()
                    z_copy(w, 2, side, u).wait_recv()

    def feed_back(s):
        if s == 0:
            for k in range(3):
                arrived(half_of(k, 1 - half), mate_recv.at[k])
        grad = (mm(grad_low[s], wd[...], 1, 0) * 2.0 * wide_a[s]).astype(BF)
        up_grad[s] = grad
        part_b[s] = mm(grad, wu[...], 1, 1)
        swap(part_b, part_b_in, 1, s).start()

    def flat_copy(s, h):
        return remote(
            flat.at[s, h], flat_in.at[c], flat_send.at[s, h],
            flat_recv.at[lax.rem(2 * s + h - c + 4, 4)], (f, 2 * s + h, t),
        )

    in_half = (
        lax.div(lax.broadcasted_iota(jnp.int32, (block_rows, 1), 0), half_rows) == t
    ).astype(F32)

    def norm_two_back(s):
        if s == 0:
            early[0] = jnp.zeros(early.shape[1:], F32)
        swap(part_b, part_b_in, 1, s).wait()
        grad = part_b[s] + part_b_in[s]
        _, normed, recip = norm_rows(middle[s], gain2[...], bias2[...])
        kept = grad * in_half
        early[0, 0:1, :] += jnp.sum(kept * normed, axis=0, keepdims=True)
        early[0, 1:2, :] += jnp.sum(kept, axis=0, keepdims=True)
        back = grad_low[s].astype(F32) + norm_back(grad, normed, recip, gain2[...])
        middle_grad[s] = back
        back = back.astype(BF)
        middle_low[s] = back
        flat_rows = mm(back, wo[...], 1, 0).T.astype(BF)
        for h in (0, 1):
            flat[s, h] = flat_rows[h * part_width : (h + 1) * part_width]

            @pl.when(2 * s + h != c)
            def _():
                flat_copy(s, h).start()

            @pl.when(2 * s + h == c)
            def _():
                flat_in[c] = flat[s, h]

    def down(s, carry):
        part_a[s] = mm(act[s], wd[...], 1, 1)
        swap(part_a, part_a_in, 2, s).start()
        return carry

    def feed_down():
        lax.fori_loop(0, slots, down, 0)

    def put_result():
        for s in range(slots):
            swap(part_a, part_a_in, 2, s).wait()
            result[s] = (middle[s] + (part_a[s] + part_a_in[s])).astype(BF)

    def fg_view(block, rows):
        return wide_a.at[block // 2, rows, pl.ds(block % 2 * model, model)]

    def own_copy(block):
        return remote(
            fg_view(block, theirs), fg_in.at[block], own_send.at[block], own_recv.at[block],
            partner,
        )

    def pair_copy(block):
        return remote(
            fg_low.at[block], pair_in.at[block], pair_send.at[block], pair_recv.at[block],
            (f, mate, t),
        )

    def fg_copy(block):
        return remote(
            fg_low.at[block], fg_other, fg_ssem.at[block], fg_recv.at[0], (f, block, t)
        )

    def collects(block):
        return inner * (1 - (mate == block)) + (1 - inner) * (c == block) == 1

    def hand_over(block):
        own_copy(block).wait_recv()
        total = fg_view(block, mine)[...] + fg_in[block]
        fg_in[block] = total

        @pl.when(jnp.logical_not(collects(block)))
        def _():
            fg_low[block] = total.astype(BF)
            pair_copy(block).start()

    def collect(block):
        @pl.when(collects(block))
        def _():
            arrived(pair_in.at[block], pair_recv.at[block])
            total = fg_in[block] + pair_in[block]

            @pl.when(block == c)
            def _():
                fg_own[...] = total

            @pl.when(block != c)
            def _():
                fg_low[block] = total.astype(BF)
                fg_copy(block).start()

    def attention_back(block):
        if block == blocks - 1:
            key_acc[...] = jnp.zeros_like(key_acc)
            value_acc[...] = jnp.zeros_like(value_acc)
            later[...] = jnp.zeros_like(later)
            conv_acc[...] = jnp.zeros_like(conv_acc)

        @pl.when(block != c)
        def _():
            arrived(flat_in.at[block], flat_recv.at[lax.rem(c - block + 4, 4)])

        keys = (block + 1) * block_rows

        def attend_back(head, carry, block=block, keys=keys):
            query, key, probs = soft(head, block)
            channels = span(head * HD, HD)
            grad_t = flat_in[block, channels, :]
            prob_grad = mm(grad_t.T, heads[2 * count + head, 0:keys, :], 1, 1)
            delta = jnp.sum(probs * prob_grad, axis=-1, keepdims=True)
            score_grad = (probs * (prob_grad - delta)).astype(BF)
            query_t[channels, :] = (mm(score_grad, key, 1, 0) * SCALING).T
            key_acc[head, :, 0:keys] += mm(query.T, score_grad, 1, 0)
            value_acc[head, :, 0:keys] += mm(grad_t, probs.astype(BF), 1, 0)
            return carry

        lax.fori_loop(0, count, attend_back, 0)
        columns = slice(block * block_rows, (block + 1) * block_rows)
        mixed_low[...] = jnp.concatenate(
            [
                query_t[...],
                key_acc[:, :, columns].reshape(part_width, block_rows),
                value_acc[:, :, columns].reshape(part_width, block_rows),
            ],
            axis=0,
        ).T
        mixed = mixed_low[...]
        joined = jnp.concatenate([mixed, later[...]], axis=0)
        next_one = pltpu.roll(joined, block_rows + 7, 0)[:block_rows]
        next_two = pltpu.roll(joined, block_rows + 6, 0)[:block_rows]
        later[...] = mixed[:8]
        before = pre_all[block].astype(F32)
        for at, moved in enumerate((mixed, next_one, next_two)):
            conv_acc[at : at + 1, :] += jnp.sum(before * moved, axis=0, keepdims=True)
        conv_acc[3:4, :] += jnp.sum(mixed, axis=0, keepdims=True)
        grad = (taps[0:1] * mixed + taps[1:2] * next_one + taps[2:3] * next_two).astype(BF)
        pre_grad[block] = grad
        fg_view(block, pl.ds(0, block_rows))[...] = mm(grad, wq[...], 1, 1)
        own_copy(block).start()

    smalls = [(early, early_xy, early_z), (late, late_xy, late_z)]

    def tp_copy(k):
        return remote(
            smalls[k][0].at[0], smalls[k][0].at[1], sm_send.at[k, 0], sm_recv.at[k, 0], partner
        )

    def xy_copy(k, at):
        view = smalls[k][1].at[f]
        return remote(
            view, view, sm_send.at[k, 1 + at], sm_recv.at[k, 1 + at], ((fx, fy, fd)[at], c, t)
        )

    def z_small(k, d):
        view = smalls[k][2].at[c]
        return remote(
            view, view, sm_send.at[k, 3 + d], sm_recv.at[k, 3 + d], (f, lax.rem(c + d, 4), t)
        )

    def small_tp(k):
        tp_copy(k).wait()
        mixed_rows = 2 if k == 0 else smalls[k][0].shape[1]
        total = smalls[k][0][0] + smalls[k][0][1]
        smalls[k][1][f] = smalls[k][0][0]
        smalls[k][1][f, 0:mixed_rows, :] = total[0:mixed_rows]
        for at in range(3):
            xy_copy(k, at).start()

    def small_xy(k):
        for at, owner in enumerate((fx, fy, fd)):
            xy_copy(k, at).wait_send()
            arrived(smalls[k][1].at[owner], sm_recv.at[k, 1 + at])
        own = smalls[k][1]
        smalls[k][2][c] = own[0] + own[1] + own[2] + own[3]
        for d in (1, 2, 3):
            z_small(k, d).start()

    def small_z(k, out):
        for d in (1, 2, 3):
            z_small(k, d).wait_send()
            arrived(smalls[k][2].at[lax.rem(c - d + 4, 4)], sm_recv.at[k, 3 + d])
        own = smalls[k][2]
        out[...] = own[0] + own[1] + own[2] + own[3]

    def small_start(k):
        if k == 0:
            for h in (0, 1):

                @pl.when(half == h)
                def _():
                    for tap in range(4):
                        for kind in range(3):
                            at = 3 * tap + kind
                            lane = (at % 2 * 2 + h) * part_width
                            channels = slice(kind * part_width, (kind + 1) * part_width)
                            early[0, 2 + at // 2 : 3 + at // 2, lane : lane + part_width] = (
                                conv_acc[tap : tap + 1, channels]
                            )

        tp_copy(k).start()

    def q_copy(stage, side, u):
        view = z_rows(QKV, side, u)
        if stage == 0:
            source, target, device = q_own.at[view], q_in.at[view], lax.rem(c + 2, 4)
        else:
            source = target = q_sum.at[half, view]
            device = c + 1 - 2 * half
        return remote(
            source, target, q_send.at[stage, side, u], q_recv.at[stage, side, u], (f, device, t)
        )

    def q_one(u):
        for side in (0, 1):
            q_own[z_rows(QKV, side, u), :] = own_sum(QKV, side, u).astype(BF)
            q_copy(0, side, u).start()

    def q_two(u):
        for side in (0, 1):
            q_copy(0, side, u).wait()
            at = z_rows(QKV, side, u)
            q_sum[half, at, :] = (q_own[at, :].astype(F32) + q_in[at, :]).astype(BF)
            q_copy(1, side, u).start()

    lane = late.shape[2]

    def norm_one_back(k):
        s = slot if k == 0 else 1 - slot
        if k == 0:
            late[0] = jnp.zeros(late.shape[1:], F32)
            grad = fg_own[...]
        else:
            arrived(fg_other, fg_recv.at[0])
            grad = fg_other[...].astype(F32)
        _, normed, recip = norm_rows(tok[s, mine, :].astype(F32), gain1[...], bias1[...])
        gain_sum = jnp.sum(grad * normed, axis=0, keepdims=True)
        bias_sum = jnp.sum(grad, axis=0, keepdims=True)
        for at in range(model // lane):
            lanes = slice(at * lane, (at + 1) * lane)
            late[0, at : at + 1, :] += gain_sum[:, lanes]
            late[0, 4 + at : 5 + at, :] += bias_sum[:, lanes]
        input_grad[s, mine, :] = middle_grad[s, mine, :] + norm_back(
            grad, normed, recip, gain1[...]
        )
        in_copy(k).start()

    def in_copy(k):
        view = input_grad.at[slot if k == 0 else 1 - slot, mine]
        return remote(view, view, in_send.at[k], in_recv.at[k], partner)

    send_out()
    send_direct(QKV)
    tokens(0)
    send_down()
    pass_on(QKV)
    tokens(1)
    send_up()
    tokens(2)
    pass_down()
    own_norm()
    tokens_passed()
    pass_on(OUT)
    projections()
    attention(2)
    attention(1)
    attention(0)
    attention(3)
    pass_on(UP)
    masks()
    out_projection()
    pass_down_last()
    feed_forward()
    weight_grad(g_down, grad_low, act, 0)
    hop_one(DOWN, (1, 3), 2)
    hop_one(DOWN, (1, 3), 1)
    feed_back(0)
    weight_grad(g_down, grad_low, act, 1)
    hop_one(DOWN, (0, 2), 2)
    feed_back(1)
    norm_two_back(0)
    hop_two(DOWN, 2)
    hop_two(DOWN, 1)
    hop_one(DOWN, (1, 3), 0)
    hop_one(DOWN, (0, 2), 1)
    norm_two_back(1)
    weight_grad(g_up, second, up_grad, 0)
    weight_grad(g_up, second, up_grad, 1)
    hop_one(DOWN, (0, 2), 0)
    z_one(DOWN, 2)
    attention_back(3)
    hop_two(DOWN, 0)
    z_two(DOWN, 2)
    hop_one(UP, (1, 3), 1)
    z_one(DOWN, 1)
    attention_back(2)
    hop_one(UP, (1, 3), 2)
    hop_one(UP, (1, 3), 0)
    hop_one(UP, (0, 2), 0)
    hop_one(UP, (0, 2), 2)
    z_one(DOWN, 0)
    hand_over(3)
    z_two(DOWN, 1)
    attention_back(1)
    z_three(DOWN, 2)
    hand_over(2)
    attention_back(0)
    z_two(DOWN, 0)
    hop_two(UP, 0)
    hand_over(0)
    feed_down()
    collect(3)
    z_three(DOWN, 1)
    hand_over(1)
    hop_two(UP, 1)
    hop_two(UP, 2)
    collect(0)
    collect(2)
    small_start(0)
    z_one(UP, 0)
    weight_grad(g_qkv, first_all, pre_grad, 0)
    hop_one(UP, (0, 2), 1)
    put_result()
    for part in (0, 1):
        weight_grad(g_out, middle_low, low, part)
    collect(1)
    z_two(UP, 0)
    z_three(DOWN, 0)
    hop_one(QKV, (1, 3), 0)
    z_one(UP, 2)
    hop_one(OUT, (1, 3), 0)
    z_one(UP, 1)
    weight_grad(g_qkv, first_all, pre_grad, 1)
    hop_one(OUT, (0, 2), 0)
    norm_one_back(0)
    hop_one(QKV, (0, 2), 1)
    hop_one(QKV, (0, 2), 0)
    norm_one_back(1)
    z_two(UP, 2)
    z_three(UP, 0)
    hop_two(OUT, 0)
    hop_one(QKV, (1, 3), 1)
    z_two(UP, 1)
    z_three(UP, 2)
    z_one(OUT, 0)
    hop_two(QKV, 1)
    z_three(UP, 1)
    q_one(1)
    small_start(1)
    z_two(OUT, 0)
    small_tp(0)
    hop_two(QKV, 0)
    q_two(1)
    small_tp(1)
    small_xy(0)
    small_xy(1)
    q_one(0)
    z_three(OUT, 0)
    q_two(0)
    small_z(0, early_out)
    small_z(1, late_out)
    for w in range(4):
        reduced(w)
        for kind in (0, 1):
            direct(w, kind).wait_send()
        for kind in (2, 3):
            relay(w, kind).wait_send()
    for side in (0, 1):
        for u in range(CUTS[QKV]):
            q_copy(1, side, u).wait_send()
            arrived(q_sum.at[1 - half, z_rows(QKV, side, u)], q_recv.at[1, side, u])
    for k in range(3):
        mate_copy(k).wait_send()
        tok_pass(k).wait_send()
        if k < 2:
            tok_copy(k).wait_send()

            @pl.when(inner == 1)
            def _():
                tok_relay(k).wait_send()

    for s in range(slots):
        in_copy(s).wait_send()
        view = input_grad.at[slot if s == 0 else 1 - slot, theirs]
        arrived(view, in_recv.at[s])
        for h in (0, 1):

            @pl.when(2 * s + h != c)
            def _():
                flat_copy(s, h).wait_send()

    for block in range(blocks):
        own_copy(block).wait_send()

        @pl.when(block != c)
        def _():
            att_copy(block).wait_send()

        @pl.when(jnp.logical_not(collects(block)))
        def _():
            pair_copy(block).wait_send()

        @pl.when(collects(block))
        def _():
            @pl.when(block != c)
            def _():
                fg_copy(block).wait_send()


def layer_call(
    lens, tok, cot, wq3, wo, wu, wd, gain1, bias1, gain2, bias2, taps3, shift3
):
    slots, block_rows, model = tok.shape
    share, units, channels = wu.shape[0], wu.shape[1], wo.shape[1]
    part = channels // 2
    width = 3 * part
    blocks = 4
    tall = (slots, block_rows, model)
    wide = (slots, block_rows, units)
    half = block_rows // 2
    columns = [units, units, channels, width]
    dma = pltpu.SemaphoreType.DMA

    def vmem(shape, kind=BF):
        return pltpu.VMEM(tuple(shape), kind)

    def struct(shape, kind=BF):
        return jax.ShapeDtypeStruct(tuple(shape), kind)

    return pl.pallas_call(
        layer_kernel,
        name="layer",
        out_shape=[
            struct(tall), struct(tall, F32), struct((share, units)), struct((share, units)),
            struct((share, channels)), struct((2, share, width)), struct((8, model), F32),
            struct((8, 256), F32),
        ],
        in_specs=[SMEM] + [ANY] * 6 + [VMEM] * 6,
        out_specs=[VMEM] * 8,
        scratch_shapes=[
            vmem(tall), vmem(tall), vmem(wq3.shape), vmem((model, width)),
            vmem((model, channels)), vmem((model, units)), vmem((model, units)),
            vmem((8, width), F32), vmem((8, width), F32), vmem((8, width), F32),
            vmem((blocks, block_rows, model)), vmem((blocks, block_rows, width)),
            vmem((width // HD, blocks * block_rows, HD)),
            vmem((blocks, part, block_rows)), vmem((blocks, part, block_rows)),
            vmem((slots, block_rows, channels)), vmem(tall, F32), vmem(tall, F32),
            vmem(tall, F32), vmem(tall, F32), vmem(wide, F32), vmem(tall, F32), vmem(tall, F32),
            vmem(tall), vmem(tall), vmem(wide), vmem(wide), vmem(tall),
            vmem((slots, 2, part, block_rows)), vmem((4, part, block_rows)),
            vmem((model, units)), vmem((model, units)), vmem((model, channels)),
            vmem((model, width)),
            [vmem((4, share // 2, n)) for n in columns],
            [vmem((2, share // 2, n)) for n in columns],
            [vmem((2, share // 2, n)) for n in columns],
            [vmem((share, n)) for n in columns[:3]],
            [vmem((2, share, n)) for n in columns[:3]],
            vmem((share, width)), vmem((share, width)),
            vmem((8, blocks * block_rows), F32),
            vmem((part // HD, HD, blocks * block_rows), F32),
            vmem((part // HD, HD, blocks * block_rows), F32),
            vmem((part, block_rows), F32), vmem((8, width), F32),
            vmem((block_rows, width), F32), vmem((blocks, block_rows, width)),
            vmem((8, width), F32),
            vmem((blocks, half, model), F32), vmem((blocks, half, model)),
            vmem((blocks, half, model)), vmem((half, model), F32), vmem((half, model)),
            vmem((2, 8, model), F32), vmem((4, 8, model), F32), vmem((4, 8, model), F32),
            vmem((2, 8, 256), F32), vmem((4, 8, 256), F32), vmem((4, 8, 256), F32),
            dma((6,)), dma((4,)), dma((4,)), dma((4,)), dma((4,)), dma((3,)), dma((3,)),
            dma((4, 4)), dma((4, 4)),
            dma((4,)), dma((4,)),
            dma((3, slots)), dma((3, slots)), dma((slots, 2)), dma((4,)),
            [dma((4, n)) for n in CUTS], [dma((4, n)) for n in CUTS],
            [dma((2, n)) for n in CUTS], [dma((2, n)) for n in CUTS],
            [dma((3, 2, n)) for n in CUTS[:3]], [dma((3, 2, n)) for n in CUTS[:3]],
            dma((2, 2, CUTS[QKV])), dma((2, 2, CUTS[QKV])),
            dma((4,)), dma((1,)), dma((4,)), dma((4,)), dma((4,)), dma((4,)), dma((slots,)),
            dma((slots,)),
            dma((2, 7)), dma((2, 7)),
        ],
        compiler_params=pltpu.CompilerParams(
            collective_id=0, has_side_effects=True, vmem_limit_bytes=67043328
        ),
    )(lens, tok, cot, wq3, wo, wu, wd, gain1, bias1, gain2, bias2, taps3, shift3)


def finish_kernel(
    result_in, grad_in, down_in, up_in, out_in, qkv_in, early, late,
    result, grad, gain1, bias1, qkv, taps, shift, out, gain2, bias2, up, down,
):
    result[...] = result_in[...]
    grad[...] = grad_in[...]
    down[...] = down_in[...].astype(F32)
    up[...] = up_in[...].astype(F32)
    out[...] = out_in[...].astype(F32)
    part = qkv_in.shape[2] // 3
    for kind in range(3):
        for h in (0, 1):
            qkv[kind, :, h * part : (h + 1) * part] = qkv_in[
                h, :, kind * part : (kind + 1) * part
            ].astype(F32)
    lane = late.shape[1]
    for at in range(gain1.shape[0] // lane):
        lanes = slice(at * lane, (at + 1) * lane)
        gain1[lanes] = late[at]
        bias1[lanes] = late[4 + at]
    gain2[...] = early[0]
    bias2[...] = early[1]
    for at in range(12):
        lane = at % 2 * 2 * part
        values = early[2 + at // 2 : 3 + at // 2, lane : lane + 2 * part]
        tap, kind = at // 3, at % 3
        if tap < 3:
            taps[tap, kind : kind + 1, :] = values
        else:
            shift[kind : kind + 1, :] = values


def finish_call(result, grad, down, up, out, qkv, early, late):
    channels, share, model = out.shape[1], out.shape[0], result.shape[2]

    def struct(shape, kind=F32):
        return jax.ShapeDtypeStruct(tuple(shape), kind)

    vector = struct((model,))
    steps = result.shape[0]
    rows = share // steps
    cut = result.shape[1] * result.shape[0] // steps

    def tall(index):
        return index, 0, 0

    def whole(shape):
        return pl.BlockSpec(shape, lambda index: (0,) * len(shape))

    def block(width):
        return pl.BlockSpec((rows, width), lambda index: (index, 0))

    def triple(count, width):
        return pl.BlockSpec((count, rows, width), lambda index: (0, index, 0))

    tall_spec = pl.BlockSpec((1, cut, model), tall)
    vector_spec = whole((model,))
    units = up.shape[1]
    return pl.pallas_call(
        finish_kernel,
        grid=(steps,),
        in_specs=[
            tall_spec, tall_spec, block(units), block(units), block(channels),
            triple(2, qkv.shape[2]), whole(early.shape), whole(late.shape),
        ],
        out_specs=[
            tall_spec, tall_spec, vector_spec, vector_spec, triple(3, channels),
            whole((3, 3, channels)), whole((3, channels)), block(channels), vector_spec,
            vector_spec, block(units), block(units),
        ],
        name="finish",
        out_shape=[
            struct(result.shape, BF), struct(grad.shape), vector, vector,
            struct((3, share, channels)), struct((3, 3, channels)), struct((3, channels)),
            struct(out.shape), vector, vector, struct(up.shape), struct(down.shape),
        ],
    )(result, grad, down, up, out, qkv, early, late)


def local(
    tokens,
    lengths,
    cotangent,
    ln1_gain,
    ln1_bias,
    qkv_weight,
    conv_kernel,
    conv_bias,
    out_weight,
    ln2_gain,
    ln2_bias,
    up_weight,
    down_weight,
):
    batches, block_rows, model_width = tokens.shape
    all_rows = batches * block_rows
    qkv_full, out_full, up_full_w, down_full_w = (
        lax.all_gather(qkv_weight, "fsdp", axis=0, tiled=True),
        lax.all_gather(out_weight, "fsdp", axis=1, tiled=True),
        lax.all_gather(up_weight, "fsdp", axis=0, tiled=True),
        lax.all_gather(down_weight, "fsdp", axis=1, tiled=True),
    )
    local_width = qkv_full.shape[2]
    local_heads = local_width // HD
    ctx_count = lax.axis_size("ctx")
    slot_span = block_rows * ctx_count
    group_blocks = 4
    key_span = block_rows * group_blocks
    ctx_index = lax.axis_index("ctx")
    positions = ctx_index * block_rows + jnp.arange(block_rows, dtype=jnp.int32)
    span_iota = jnp.arange(key_span, dtype=jnp.int32)
    block_count = (ctx_index * block_rows + block_rows + key_span - 1) // key_span
    token_valid = positions[None, :] < lengths[:, None]

    def span_slice(array_data, block, axis_pos):
        return lax.dynamic_slice_in_dim(array_data, block * key_span, key_span, axis_pos)

    inputs = tokens.astype(jnp.float32).reshape(all_rows, model_width)
    first_out, first_hat, first_recip = layer_norm(inputs, ln1_gain, ln1_bias)
    first_low = first_out.astype(jnp.bfloat16)
    pre_low = jnp.einsum(
        "td,dcn->tcn", first_low, qkv_full, preferred_element_type=jnp.float32
    ).astype(jnp.bfloat16)
    pre_low = pre_low.reshape(batches, block_rows, 3, local_width)
    earlier = shifted(pre_low[:, block_rows - 2 :], "ctx", 1)
    extended = jnp.concatenate([earlier, pre_low], axis=1).astype(jnp.float32)
    conv_out = (
        conv_bias
        + conv_kernel[0] * extended[:, 2:]
        + conv_kernel[1] * extended[:, 1:-1]
        + conv_kernel[2] * extended[:, :-2]
    ).astype(jnp.bfloat16)
    query_heads = conv_out[:, :, 0].reshape(batches, block_rows, local_heads, HD)
    own_pairs = conv_out[:, :, 1:]
    whole_pairs = lax.all_gather(own_pairs, "ctx", axis=1, tiled=True)
    key_heads = whole_pairs[:, :, 0].reshape(batches, slot_span, local_heads, HD)
    value_heads = whole_pairs[:, :, 1].reshape(batches, slot_span, local_heads, HD)

    def stat_step(block, carry):
        row_max, total = carry
        key_pos = block * key_span + span_iota
        scores = tile_scores(
            query_heads, span_slice(key_heads, block, 1), positions, key_pos, lengths
        )
        new_max = jnp.maximum(row_max, jnp.max(scores, axis=-1, keepdims=True))
        total = total * jnp.exp(row_max - new_max) + jnp.sum(
            jnp.exp(scores - new_max), axis=-1, keepdims=True
        )
        return (new_max, total)

    stat_shape = (batches, local_heads, block_rows, 1)
    row_max, total = lax.fori_loop(
        0,
        block_count,
        stat_step,
        (jnp.full(stat_shape, MASKED, jnp.float32), jnp.zeros(stat_shape, jnp.float32)),
    )
    log_total = row_max + jnp.log(total)

    def value_step(block, accum):
        key_pos = block * key_span + span_iota
        scores = tile_scores(
            query_heads, span_slice(key_heads, block, 1), positions, key_pos, lengths
        )
        probs_low = jnp.exp(scores - log_total).astype(jnp.bfloat16)
        return accum + jnp.einsum(
            "mhqk,mkhd->mqhd",
            probs_low,
            span_slice(value_heads, block, 1),
            preferred_element_type=jnp.float32,
        )

    attn_acc = lax.fori_loop(
        0, block_count, value_step, jnp.zeros((batches, block_rows, local_heads, HD), jnp.float32)
    )
    attn_low = attn_acc.reshape(all_rows, local_width).astype(jnp.bfloat16)
    attn_out = lax.psum(jnp.dot(attn_low, out_full, preferred_element_type=jnp.float32), "tp")
    middle = inputs + attn_out
    second_out, second_hat, second_recip = layer_norm(middle, ln2_gain, ln2_bias)
    second_low = second_out.astype(jnp.bfloat16)
    up_full = jnp.dot(second_low, up_full_w, preferred_element_type=jnp.float32)
    rectified = jnp.maximum(up_full, 0.0)
    act_low = (rectified * rectified).astype(jnp.bfloat16)
    ffn_out = lax.psum(jnp.dot(act_low, down_full_w, preferred_element_type=jnp.float32), "tp")
    result = (middle + ffn_out).reshape(batches, block_rows, model_width).astype(jnp.bfloat16)
    grad_out = (
        cotangent.astype(jnp.float32) * token_valid[:, :, None].astype(jnp.float32)
    ).reshape(all_rows, model_width)
    grad_low = grad_out.astype(jnp.bfloat16)
    down_wgrad = jnp.einsum("tf,td->fd", act_low, grad_low, preferred_element_type=jnp.float32)
    act_grad = jnp.einsum("td,fd->tf", grad_low, down_full_w, preferred_element_type=jnp.float32)
    up_grad_low = (act_grad * 2.0 * rectified).astype(jnp.bfloat16)
    up_wgrad = jnp.einsum("td,tf->df", second_low, up_grad_low, preferred_element_type=jnp.float32)
    second_grad = lax.psum(
        jnp.einsum("tf,df->td", up_grad_low, up_full_w, preferred_element_type=jnp.float32), "tp"
    )
    gain_two_grad = jnp.sum(second_grad * second_hat, axis=0)
    bias_two_grad = jnp.sum(second_grad, axis=0)
    middle_grad = grad_out + norm_back(second_grad, second_hat, second_recip, ln2_gain)
    middle_low = middle_grad.astype(jnp.bfloat16)
    out_wgrad = jnp.einsum("tn,td->nd", attn_low, middle_low, preferred_element_type=jnp.float32)
    attn_flat = jnp.einsum(
        "td,nd->tn", middle_low, out_full, preferred_element_type=jnp.float32
    ).astype(jnp.bfloat16)
    attn_grad = attn_flat.reshape(batches, block_rows, local_heads, HD)

    def delta_step(block, accum):
        key_pos = block * key_span + span_iota
        probs_full = jnp.exp(
            tile_scores(query_heads, span_slice(key_heads, block, 1), positions, key_pos, lengths)
            - log_total
        )
        prob_grad = jnp.einsum(
            "mqhd,mkhd->mhqk",
            attn_grad,
            span_slice(value_heads, block, 1),
            preferred_element_type=jnp.float32,
        )
        return accum + jnp.sum(probs_full * prob_grad, axis=-1, keepdims=True)

    delta = lax.fori_loop(0, block_count, delta_step, jnp.zeros(stat_shape, jnp.float32))
    query_zero = jnp.zeros((batches, block_rows, local_heads, HD), jnp.float32)

    def back_step(block, carry):
        accum, buffer = carry
        key_pos = block * key_span + span_iota
        key_part = span_slice(key_heads, block, 1)
        probs_full, prob_grad, score_grad = tile_grads(
            query_heads,
            key_part,
            span_slice(value_heads, block, 1),
            attn_grad,
            log_total,
            delta,
            positions,
            key_pos,
            lengths,
        )
        probs_again = probs_full.astype(jnp.bfloat16)
        accum = (
            accum
            + jnp.einsum(
                "mhqk,mkhd->mqhd", score_grad, key_part, preferred_element_type=jnp.float32
            )
            * SCALING
        )
        key_term = (
            jnp.einsum(
                "mhqk,mqhd->mkhd", score_grad, query_heads, preferred_element_type=jnp.float32
            )
            * SCALING
        )
        value_term = jnp.einsum(
            "mhqk,mqhd->mkhd", probs_again, attn_grad, preferred_element_type=jnp.float32
        )
        stacked = jnp.stack(
            [
                key_term.reshape(batches, key_span, local_width),
                value_term.reshape(batches, key_span, local_width),
            ],
            axis=2,
        )
        buffer = lax.dynamic_update_slice_in_dim(buffer, stacked, block * key_span, 1)
        return (accum, buffer)

    buffer_zero = jnp.zeros((batches, slot_span, 2, local_width), jnp.float32)
    query_grad, pair_terms = lax.fori_loop(0, block_count, back_step, (query_zero, buffer_zero))
    pair_grad = lax.psum_scatter(pair_terms, "ctx", scatter_dimension=1, tiled=True)
    mixed_grad = jnp.concatenate(
        [query_grad.reshape(batches, block_rows, 1, local_width), pair_grad], axis=2
    )
    later = shifted(mixed_grad[:, :2], "ctx", -1)
    ahead = jnp.concatenate([mixed_grad, later], axis=1)
    pre_grad = (
        conv_kernel[0] * ahead[:, :block_rows]
        + conv_kernel[1] * ahead[:, 1 : block_rows + 1]
        + conv_kernel[2] * ahead[:, 2:]
    ).astype(jnp.bfloat16)
    kernel_grad = jnp.stack(
        [
            jnp.sum(extended[:, 2 - offset : 2 - offset + block_rows] * mixed_grad, axis=(0, 1))
            for offset in range(3)
        ]
    )
    shift_grad = jnp.sum(mixed_grad, axis=(0, 1))
    pre_grad = pre_grad.reshape(all_rows, 3, local_width)
    qkv_wgrad = jnp.einsum("td,tcn->dcn", first_low, pre_grad, preferred_element_type=jnp.float32)
    first_grad = lax.psum(
        jnp.einsum("tcn,dcn->td", pre_grad, qkv_full, preferred_element_type=jnp.float32), "tp"
    )
    gain_one_grad = jnp.sum(first_grad * first_hat, axis=0)
    bias_one_grad = jnp.sum(first_grad, axis=0)
    input_grad = middle_grad + norm_back(first_grad, first_hat, first_recip, ln1_gain)
    input_grad = input_grad.reshape(batches, block_rows, model_width)
    summed = lax.psum(
        (
            qkv_wgrad,
            out_wgrad,
            up_wgrad,
            down_wgrad,
            gain_one_grad,
            bias_one_grad,
            kernel_grad,
            shift_grad,
            gain_two_grad,
            bias_two_grad,
        ),
        ("fsdp", "ctx"),
    )
    share_rows = model_width // lax.axis_size("fsdp")
    owner_start = lax.axis_index("fsdp") * share_rows
    qkv_share = lax.dynamic_slice_in_dim(summed[0], owner_start, share_rows, 0)
    out_share = lax.dynamic_slice_in_dim(summed[1], owner_start, share_rows, 1)
    up_share = lax.dynamic_slice_in_dim(summed[2], owner_start, share_rows, 0)
    down_share = lax.dynamic_slice_in_dim(summed[3], owner_start, share_rows, 1)
    small_sums = summed[4:]
    return (
        result,
        input_grad,
        small_sums[0],
        small_sums[1],
        qkv_share,
        small_sums[2],
        small_sums[3],
        out_share,
        small_sums[4],
        small_sums[5],
        up_share,
        down_share,
    )


def local_fast(
    tokens,
    lengths,
    cotangent,
    ln1_gain,
    ln1_bias,
    qkv_weight,
    conv_kernel,
    conv_bias,
    out_weight,
    ln2_gain,
    ln2_bias,
    up_weight,
    down_weight,
):
    parts = layer_call(
        lengths, tokens, cotangent, qkv_weight.transpose(1, 0, 2), out_weight.T, up_weight,
        down_weight.T, ln1_gain, ln1_bias, ln2_gain, ln2_bias, conv_kernel, conv_bias,
    )
    result, grad, gain1, bias1, qkv, taps, shift, out, gain2, bias2, up, down = finish_call(*parts)
    return (
        result, grad, gain1, bias1, qkv.transpose(1, 0, 2), taps, shift, out.T, gain2, bias2, up,
        down.T,
    )


def solution(mesh):
    placed = (
        P("fsdp", "ctx", None),
        P("fsdp"),
        P("fsdp", "ctx", None),
        P(),
        P(),
        P("fsdp", None, "tp"),
        P(None, None, "tp"),
        P(None, "tp"),
        P("tp", "fsdp"),
        P(),
        P(),
        P("fsdp", "tp"),
        P("tp", "fsdp"),
    )
    ctx, fsdp, tp = mesh.shape["ctx"], mesh.shape["fsdp"], mesh.shape["tp"]
    return jax.shard_map(
        local_fast if (fsdp, ctx, tp) == (4, 4, 2) else local,
        mesh=mesh,
        in_specs=placed,
        out_specs=(
            P("fsdp", "ctx", None),
            P("fsdp", "ctx", None),
            P(),
            P(),
            P("fsdp", None, "tp"),
            P(None, None, "tp"),
            P(None, "tp"),
            P("tp", "fsdp"),
            P(),
            P(),
            P("fsdp", "tp"),
            P("tp", "fsdp"),
        ),
        check_vma=False,
    )
```
